8 devices in a mesh: tp: 8 (over z, y, x, core).
Axes of the slice: x: 2, y: 2, z: 1, core: 2. Of those that a mesh axis runs over, the one named last changes fastest.
Arguments:
- tok_ids: int32 [2, 1024], replicated
- next_ids: int32 [2, 1024], replicated
- seq_lens: int32 [1024], replicated
- embed: bfloat16 [49280, 2048], P('tp')
- ln_gain: bfloat16 [2048], replicated
- w_in: bfloat16 [2048, 18688], P(None, 'tp')
- w_out: bfloat16 [10240, 2048], P('tp')
- final_gain: bfloat16 [2048], replicated
- k_cache: bfloat16 [1024, 1024, 128], P('tp')
- v_cache: bfloat16 [1024, 1024, 128], P('tp')
Outputs:
- output 1: float32 [2, 1024], replicated
- output 2: bfloat16 [1024, 1024, 128], P('tp')
- output 3: bfloat16 [1024, 1024, 128], P('tp')
All inputs are finite; a program needn't handle non-finite values.
Results may differ from the reference program's by a relative error of at most 0.001.
Values are sent between devices in bfloat16 or wider.
A program may use at most 1 GiB of HBM per device.

```python
import jax
import jax.numpy as jnp
from jax import lax

D = 2048
HEADS = 16
HEAD = 128
FF = 8192
VOCAB = 49280
GROUP = 8
BATCH_DEV = 128
CACHE_LEN = 1024
NUM_STEPS = 2

BATCH = BATCH_DEV * GROUP
QKV_WIDTH = (HEADS + 2) * HEAD
ATTN_WIDTH = HEADS * HEAD
QKV_DEV = QKV_WIDTH // GROUP
ATTN_DEV = ATTN_WIDTH // GROUP
FF_DEV = FF // GROUP
IN_DEV = QKV_DEV + 2 * FF_DEV
OUT_DEV = ATTN_DEV + FF_DEV
IN_WIDTH = IN_DEV * GROUP
OUT_WIDTH = OUT_DEV * GROUP
MAP_ROWS = min(BATCH, 64)
MAP_COUNT = BATCH // MAP_ROWS
NORM_EPS = 1e-6
ROPE_BASE = 10000.0


def setup_inputs(seed: int = 0) -> dict:
    key_list = jax.random.split(jax.random.key(seed), 11)
    tok_ids = jax.random.randint(key_list[0], (NUM_STEPS, BATCH), 0, VOCAB, dtype=jnp.int32)
    next_ids = jax.random.randint(key_list[1], (NUM_STEPS, BATCH), 0, VOCAB, dtype=jnp.int32)
    base_lens = jax.random.randint(key_list[2], (BATCH,), 0, CACHE_LEN - 1, dtype=jnp.int32)
    perm_order = jax.random.permutation(key_list[3], BATCH)
    seq_lens = base_lens.at[perm_order[0]].set(CACHE_LEN - 2).at[perm_order[1]].set(0)
    embed = jax.random.normal(key_list[4], (VOCAB, D), jnp.float32).astype(jnp.bfloat16)
    ln_gain = (1.0 + 0.3 * jax.random.normal(key_list[5], (D,), jnp.float32)).astype(jnp.bfloat16)
    w_in = (jax.random.normal(key_list[6], (D, IN_WIDTH), jnp.float32) * D ** -0.5).astype(jnp.bfloat16)
    row_scale = jnp.where(jnp.arange(OUT_WIDTH) % OUT_DEV < ATTN_DEV, 2.0 * ATTN_WIDTH ** -0.5, FF ** -0.5)
    w_out = (jax.random.normal(key_list[7], (OUT_WIDTH, D), jnp.float32) * row_scale[:, None]).astype(jnp.bfloat16)
    final_gain = (1.6 * (1.0 + 0.3 * jax.random.normal(key_list[8], (D,), jnp.float32))).astype(jnp.bfloat16)
    k_cache = jax.random.normal(key_list[9], (BATCH, CACHE_LEN, HEAD), jnp.float32).astype(jnp.bfloat16)
    v_cache = jax.random.normal(key_list[10], (BATCH, CACHE_LEN, HEAD), jnp.float32).astype(jnp.bfloat16)
    return {'tok_ids': tok_ids, 'next_ids': next_ids, 'seq_lens': seq_lens, 'embed': embed, 'ln_gain': ln_gain, 'w_in': w_in, 'w_out': w_out, 'final_gain': final_gain, 'k_cache': k_cache, 'v_cache': v_cache}


def layer_norm(values, gain_vec):
    centered = values.astype(jnp.float32)
    centered = centered - jnp.mean(centered, axis=-1, keepdims=True)
    variance = jnp.mean(jnp.square(centered), axis=-1, keepdims=True)
    scaled = centered * lax.rsqrt(variance + NORM_EPS) * gain_vec.astype(jnp.float32)
    return scaled.astype(jnp.bfloat16)


def rotary(vectors, positions):
    half_dim = vectors.shape[-1] // 2
    inv_freq = ROPE_BASE ** (-jnp.arange(half_dim, dtype=jnp.float32) / half_dim)
    angles = positions.astype(jnp.float32)[..., None] * inv_freq
    cosine = jnp.cos(angles)
    sine_val = jnp.sin(angles)
    first_half = vectors[..., :half_dim]
    second_half = vectors[..., half_dim:]
    return jnp.concatenate([first_half * cosine - second_half * sine_val, second_half * cosine + first_half * sine_val], axis=-1)


def block_steps(tok_blk, next_blk, len_blk, k_blk, v_blk, embed, ln_gain, w_in, w_out, final_gain):
    row_count = len_blk.shape[0]
    time_ids = jnp.arange(CACHE_LEN)
    step_logp = []
    for step_idx in range(NUM_STEPS):
        positions = len_blk + step_idx
        x_rows = embed[tok_blk[step_idx]]
        normed = layer_norm(x_rows, ln_gain)
        proj_out = jnp.dot(normed, w_in, preferred_element_type=jnp.float32).astype(jnp.bfloat16)
        proj_out = proj_out.reshape(row_count, GROUP, IN_DEV)
        qkv_vec = proj_out[:, :, :QKV_DEV].reshape(row_count, QKV_WIDTH)
        gate_proj = proj_out[:, :, QKV_DEV:QKV_DEV + FF_DEV].astype(jnp.float32)
        up_proj = proj_out[:, :, QKV_DEV + FF_DEV:].astype(jnp.float32)
        mlp_act = (jax.nn.silu(gate_proj) * up_proj).astype(jnp.bfloat16)
        queries = qkv_vec[:, :ATTN_WIDTH].reshape(row_count, HEADS, HEAD).astype(jnp.float32)
        q_rot = (rotary(queries, positions[:, None]) * HEAD ** -0.5).astype(jnp.bfloat16)
        k_new = rotary(qkv_vec[:, ATTN_WIDTH:ATTN_WIDTH + HEAD].astype(jnp.float32), positions).astype(jnp.bfloat16)
        v_new = qkv_vec[:, ATTN_WIDTH + HEAD:]
        write_mask = time_ids[None, :, None] == positions[:, None, None]
        k_blk = jnp.where(write_mask, k_new[:, None, :], k_blk)
        v_blk = jnp.where(write_mask, v_new[:, None, :], v_blk)
        scores = jnp.einsum('bhd,btd->bht', q_rot.astype(jnp.float32), k_blk.astype(jnp.float32))
        visible = time_ids[None, None, :] <= positions[:, None, None]
        attn_probs = jax.nn.softmax(jnp.where(visible, scores, -jnp.inf), axis=-1).astype(jnp.bfloat16)
        attn_out = jnp.einsum('bht,btd->bhd', attn_probs.astype(jnp.float32), v_blk.astype(jnp.float32)).astype(jnp.bfloat16)
        attn_grp = attn_out.reshape(row_count, GROUP, ATTN_DEV)
        combined = jnp.concatenate([attn_grp, mlp_act], axis=2).reshape(row_count, OUT_WIDTH)
        layer_out = jnp.dot(combined, w_out, preferred_element_type=jnp.float32).astype(jnp.bfloat16)
        resid_sum = x_rows.astype(jnp.float32) + layer_out.astype(jnp.float32)
        final_normed = layer_norm(resid_sum, final_gain)
        logits = jnp.dot(final_normed, embed.T, preferred_element_type=jnp.float32) * D ** -0.5
        picked = jnp.take_along_axis(logits, next_blk[step_idx][:, None], axis=1)[:, 0]
        step_logp.append(picked - jax.nn.logsumexp(logits, axis=1))
    return jnp.stack(step_logp), k_blk, v_blk


def reference(tok_ids, next_ids, seq_lens, embed, ln_gain, w_in, w_out, final_gain, k_cache, v_cache):
    tok_grp = tok_ids.reshape(NUM_STEPS, MAP_COUNT, MAP_ROWS).transpose(1, 0, 2)
    next_grp = next_ids.reshape(NUM_STEPS, MAP_COUNT, MAP_ROWS).transpose(1, 0, 2)
    len_grp = seq_lens.reshape(MAP_COUNT, MAP_ROWS)
    k_grp = k_cache.reshape(MAP_COUNT, MAP_ROWS, CACHE_LEN, HEAD)
    v_grp = v_cache.reshape(MAP_COUNT, MAP_ROWS, CACHE_LEN, HEAD)

    def run_group(group_in):
        return block_steps(group_in[0], group_in[1], group_in[2], group_in[3], group_in[4], embed, ln_gain, w_in, w_out, final_gain)

    logp_grp, k_done, v_done = lax.map(run_group, (tok_grp, next_grp, len_grp, k_grp, v_grp))
    log_probs = logp_grp.transpose(1, 0, 2).reshape(NUM_STEPS, BATCH)
    return log_probs, k_done.reshape(BATCH, CACHE_LEN, HEAD), v_done.reshape(BATCH, CACHE_LEN, HEAD)
```

```python
import functools

import jax
import jax.numpy as jnp
from jax import lax
from jax.experimental import pallas as pl
from jax.experimental.pallas import tpu as pltpu
from jax.sharding import PartitionSpec as P

ROPE_BASE = 10000.0
NORM_EPS = 1e-6
LOG2E = 1.4426950408889634


def layer_norm(values, gain_vec):
    centered = values.astype(jnp.float32)
    centered = centered - jnp.mean(centered, axis=-1, keepdims=True)
    variance = jnp.mean(jnp.square(centered), axis=-1, keepdims=True)
    scaled = centered * lax.rsqrt(variance + NORM_EPS) * gain_vec.astype(jnp.float32)
    return scaled.astype(jnp.bfloat16)


def attention_kernel(lens_ref, qkv_ref, cos_ref, sin_ref, k_ref, v_ref, o_ref, ko_ref, vo_ref, q_scr, o_scr, n_scr):
    num_steps, rows, _ = qkv_ref.shape
    cache_len, head = k_ref.shape[1], k_ref.shape[2]
    heads = o_ref.shape[2] // head
    block = pl.program_id(0)
    per_seq = num_steps * heads
    for s in range(num_steps):
        cos, sin = cos_ref[s], sin_ref[s]

        def rotate(lo):
            x = qkv_ref[s, :, lo:lo + head].astype(jnp.float32)
            return x * cos + pltpu.roll(x, head // 2, 1) * sin

        for h in range(heads):
            q_scr[pl.ds(s * heads + h, rows, stride=per_seq), :] = rotate(h * head) * head ** -0.5
        n_scr[0, s] = rotate(heads * head).astype(jnp.bfloat16).astype(jnp.float32)
        n_scr[1, s] = qkv_ref[s, :, (heads + 1) * head:].astype(jnp.float32)

    win_row = lax.broadcasted_iota(jnp.int32, (16, head), 0)
    col = lax.broadcasted_iota(jnp.int32, (per_seq, cache_len), 1)
    step_of = lax.broadcasted_iota(jnp.int32, (per_seq, cache_len), 0) // heads

    def one(b):
        length = lens_ref[block * rows + b]
        for src, dst, which in ((k_ref, ko_ref, 0), (v_ref, vo_ref, 1)):
            dst[b] = src[b]
            for s in range(num_steps):
                pos = length + s
                base = pl.multiple_of((pos // 16) * 16, 16)
                window = dst[b, pl.ds(base, 16), :].astype(jnp.float32)
                fresh = n_scr[which, s, pl.ds(b, 1), :]
                window = jnp.where(win_row == pos - base, fresh, window)
                dst[b, pl.ds(base, 16), :] = window.astype(jnp.bfloat16)
        q = q_scr[pl.ds(pl.multiple_of(b * per_seq, per_seq), per_seq), :].astype(jnp.bfloat16)
        scores = lax.dot_general(q, ko_ref[b], (((1,), (1,)), ((), ())), preferred_element_type=jnp.float32)
        scores = jnp.where(col <= step_of + length, scores, -jnp.inf)
        top = jnp.max(scores, axis=1, keepdims=True)
        weight = jnp.exp(scores - top)
        total = jnp.sum(weight, axis=1, keepdims=True)
        probs = (weight / total).astype(jnp.bfloat16)
        out = jnp.dot(probs, vo_ref[b], preferred_element_type=jnp.float32)
        o_scr[pl.ds(pl.multiple_of(b * per_seq, per_seq), per_seq), :] = out

    @pl.loop(0, rows // 2)
    def _(i):
        one(2 * i)
        one(2 * i + 1)

    for s in range(num_steps):
        for h in range(heads):
            o_ref[s, :, h * head:(h + 1) * head] = o_scr[pl.ds(s * heads + h, rows, stride=per_seq), :].astype(jnp.bfloat16)


def attention(lens, qkv, cos, sin, k_loc, v_loc):
    num_steps, batch, width = qkv.shape
    cache_len, head = k_loc.shape[1], k_loc.shape[2]
    attn_width = width - 2 * head
    heads = attn_width // head
    rows = 8
    row_spec = lambda last: pl.BlockSpec((num_steps, rows, last), lambda i, *_: (0, i, 0))
    cache_spec = pl.BlockSpec((rows, cache_len, head), lambda i, *_: (i, 0, 0))
    return pl.pallas_call(
        attention_kernel,
        grid_spec=pltpu.PrefetchScalarGridSpec(
            num_scalar_prefetch=1,
            grid=(batch // rows,),
            in_specs=[row_spec(width), row_spec(head), row_spec(head), cache_spec, cache_spec],
            out_specs=[row_spec(attn_width), cache_spec, cache_spec],
            scratch_shapes=[
                pltpu.VMEM((rows * num_steps * heads, head), jnp.float32),
                pltpu.VMEM((rows * num_steps * heads, head), jnp.float32),
                pltpu.VMEM((2, num_steps, rows, head), jnp.float32),
            ],
        ),
        out_shape=[
            jax.ShapeDtypeStruct((num_steps, batch, attn_width), jnp.bfloat16),
            jax.ShapeDtypeStruct(k_loc.shape, k_loc.dtype),
            jax.ShapeDtypeStruct(v_loc.shape, v_loc.dtype),
        ],
        compiler_params=pltpu.CompilerParams(vmem_limit_bytes=48 * 1024 * 1024),
        name="attention",
    )(lens, qkv, cos, sin, k_loc, v_loc)


def logits_kernel(scale, tile, ids_ref, z_ref, e_hbm, out_ref, e_buf, raw, e_sem):
    vocab = e_hbm.shape[0]
    tiles = vocab // tile
    shards, cols = z_ref.shape[0] // 256, 256
    copies = [pltpu.make_async_copy(e_hbm.at[pl.ds(t * tile, tile)], e_buf.at[pl.ds(t * tile, tile)], e_sem.at[t]) for t in range(tiles)]
    for c in copies:
        c.start()
    for c in copies:
        c.wait()
    row = lax.broadcasted_iota(jnp.int32, (8, cols), 0)

    @pl.loop(0, shards)
    def _(j):
        first = pl.multiple_of(j * cols, cols)
        ids = ids_ref[j]

        def product(t):
            e = e_buf[pl.ds(pl.multiple_of(t * tile, tile), tile), :]
            raw[lax.rem(t, 2)] = lax.dot_general(e, z_ref[pl.ds(first, cols), :], (((1,), (1,)), ((), ())), preferred_element_type=jnp.float32)

        def absorb(t, carry):
            top, total, target = carry
            local = ids - t * tile
            slot = lax.rem(t, 2)
            part = raw[slot].reshape(tile // 8, 8, cols)
            new_top = jnp.maximum(top, jnp.max(part, axis=0))
            total = total * jnp.exp2((top - new_top) * (scale * LOG2E))
            total = total + jnp.sum(jnp.exp2((part - new_top[None]) * (scale * LOG2E)), axis=0)
            rows = lax.broadcasted_iota(jnp.int32, part.shape, 0) * 8 + lax.broadcasted_iota(jnp.int32, part.shape, 1)
            target = target + jnp.sum(jnp.where(rows == local[None], part, 0.0), axis=0)
            return new_top, total, target

        product(0)
        start = (jnp.full((8, cols), -jnp.inf, jnp.float32), jnp.zeros((8, cols), jnp.float32), jnp.zeros((8, cols), jnp.float32))

        def body(t, carry):
            product(t)
            return absorb(t - 1, carry)

        carry = lax.fori_loop(1, tiles, body, start)
        top, total, target = absorb(tiles - 1, carry)
        best = jnp.max(top, axis=0, keepdims=True)
        total = jnp.sum(total * jnp.exp2((top - best) * (scale * LOG2E)), axis=0, keepdims=True)
        target = jnp.sum(target, axis=0, keepdims=True)
        out_ref[j, 0:1, :] = best * scale
        out_ref[j, 1:2, :] = total
        out_ref[j, 2:3, :] = target * scale


def logit_stats(ids, z, embed_loc):
    vocab, dim = embed_loc.shape
    tile = 560
    shards = z.shape[0] // 256
    return pl.pallas_call(
        functools.partial(logits_kernel, dim ** -0.5, tile),
        in_specs=[pl.BlockSpec(memory_space=pltpu.VMEM), pl.BlockSpec(memory_space=pltpu.VMEM), pl.BlockSpec(memory_space=pl.ANY)],
        out_specs=pl.BlockSpec(memory_space=pltpu.VMEM),
        out_shape=jax.ShapeDtypeStruct((shards, 8, 256), jnp.float32),
        scratch_shapes=[
            pltpu.VMEM((vocab, dim), jnp.bfloat16),
            pltpu.VMEM((2, tile, 256), jnp.float32),
            pltpu.SemaphoreType.DMA((vocab // tile,)),
        ],
        compiler_params=pltpu.CompilerParams(vmem_limit_bytes=56 * 1024 * 1024),
        name="logit_stats",
    )(ids, z, embed_loc)


def solution(mesh):
    group_size = mesh.shape['tp']

    def device_fn(tok_ids, next_ids, seq_lens, embed_loc, ln_gain, w_in_loc, w_out_loc, final_gain, k_loc, v_loc):
        num_steps, batch_size = tok_ids.shape
        batch_dev = batch_size // group_size
        rows_dev = num_steps * batch_dev
        vocab_dev, model_dim = embed_loc.shape
        head_dim = k_loc.shape[2]
        in_dev = w_in_loc.shape[1]
        out_dev = w_out_loc.shape[0]
        kv_dev = 2 * head_dim // group_size
        attn_dev = 2 * out_dev - in_dev + kv_dev
        ff_dev = out_dev - attn_dev
        qkv_dev = attn_dev + kv_dev
        dev_index = lax.axis_index('tp')
        vocab_start = dev_index * vocab_dev
        own_lens = lax.dynamic_slice_in_dim(seq_lens, dev_index * batch_dev, batch_dev)

        def by_device(ids):
            return ids.reshape(num_steps, group_size, batch_dev).transpose(1, 0, 2)

        local_ids = by_device(tok_ids).reshape(-1) - vocab_start
        tok_here = (local_ids >= 0) & (local_ids < vocab_dev)
        emb_rows = jnp.take(embed_loc, jnp.clip(local_ids, 0, vocab_dev - 1), axis=0)
        x_part = jnp.where(tok_here[:, None], emb_rows, jnp.zeros_like(emb_rows))
        x_own = lax.psum_scatter(x_part, 'tp', scatter_dimension=0, tiled=True)
        normed = lax.all_gather(layer_norm(x_own, ln_gain), 'tp', axis=0, tiled=True)
        proj_out = jnp.dot(normed, w_in_loc, preferred_element_type=jnp.float32).astype(jnp.bfloat16)
        gate_proj = proj_out[:, qkv_dev:qkv_dev + ff_dev].astype(jnp.float32)
        up_proj = proj_out[:, qkv_dev + ff_dev:].astype(jnp.float32)
        mlp_act = (jax.nn.silu(gate_proj) * up_proj).astype(jnp.bfloat16)
        qkv_own = lax.all_to_all(proj_out[:, :qkv_dev], 'tp', 0, 1, tiled=True).reshape(num_steps, batch_dev, -1)

        half = head_dim // 2
        inv_freq = ROPE_BASE ** (-jnp.arange(half, dtype=jnp.float32) / half)
        positions = own_lens[None, :] + jnp.arange(num_steps, dtype=jnp.int32)[:, None]
        angles = positions.astype(jnp.float32)[..., None] * inv_freq
        cos, sin = jnp.cos(angles), jnp.sin(angles)
        cos = jnp.concatenate([cos, cos], axis=-1)
        sin = jnp.concatenate([-sin, sin], axis=-1)
        attn_out, k_out, v_out = attention(own_lens, qkv_own, cos, sin, k_loc, v_loc)

        attn_cols = lax.all_to_all(attn_out.reshape(rows_dev, -1), 'tp', 1, 0, tiled=True)
        combined = jnp.concatenate([attn_cols, mlp_act], axis=1)
        part_out = jnp.dot(combined, w_out_loc, preferred_element_type=jnp.float32).astype(jnp.bfloat16)
        layer_out = lax.psum_scatter(part_out, 'tp', scatter_dimension=0, tiled=True)
        resid_sum = x_own.astype(jnp.float32) + layer_out.astype(jnp.float32)
        final_normed = lax.all_gather(layer_norm(resid_sum, final_gain), 'tp', axis=0, tiled=True)
        local_next = (by_device(next_ids).reshape(group_size, 1, rows_dev) - vocab_start)
        ids8 = jnp.broadcast_to(local_next, (group_size, 8, rows_dev)) - 0
        stats = logit_stats(ids8, final_normed, embed_loc)
        stats = lax.all_gather(stats[:, :3], 'tp', axis=0, tiled=False)
        row_max = jnp.max(stats[:, :, 0], axis=0)
        exp_sum = jnp.sum(stats[:, :, 1] * jnp.exp(stats[:, :, 0] - row_max[None]), axis=0)
        target = jnp.sum(stats[:, :, 2], axis=0)
        log_probs = target - row_max - jnp.log(exp_sum)
        log_probs = log_probs.reshape(group_size, num_steps, batch_dev).transpose(1, 0, 2).reshape(num_steps, batch_size)
        return log_probs, k_out, v_out

    cache_spec = P('tp', None, None)
    return jax.shard_map(device_fn, mesh=mesh, in_specs=(P(), P(), P(), P('tp', None), P(), P(None, 'tp'), P('tp', None), P(), cache_spec, cache_spec), out_specs=(P(), cache_spec, cache_spec), check_vma=False)
```

```python
import functools

import jax
import jax.numpy as jnp
from jax import lax
from jax.experimental import pallas as pl
from jax.experimental.pallas import tpu as pltpu
from jax.sharding import PartitionSpec as P

ROPE_BASE = 10000.0
NORM_EPS = 1e-6
LOG2E = 1.4426950408889634


def layer_norm(values, gain_vec):
    centered = values.astype(jnp.float32)
    centered = centered - jnp.mean(centered, axis=-1, keepdims=True)
    variance = jnp.mean(jnp.square(centered), axis=-1, keepdims=True)
    scaled = centered * lax.rsqrt(variance + NORM_EPS) * gain_vec.astype(jnp.float32)
    return scaled.astype(jnp.bfloat16)


def attention_kernel(lens_ref, qkv_ref, cos_ref, sin_ref, k_ref, v_ref, o_ref, ko_ref, vo_ref, q_scr, o_scr, n_scr):
    num_steps, rows, _ = qkv_ref.shape
    cache_len, head = k_ref.shape[1], k_ref.shape[2]
    pack = o_ref.shape[3] // head
    heads = o_ref.shape[0] * pack
    block = pl.program_id(0)
    per_seq = num_steps * heads
    for s in range(num_steps):
        cos, sin = cos_ref[s], sin_ref[s]

        def rotate(lo):
            x = qkv_ref[s, :, lo:lo + head].astype(jnp.float32)
            return x * cos + pltpu.roll(x, head // 2, 1) * sin

        for h in range(heads):
            q_scr[pl.ds(s * heads + h, rows, stride=per_seq), :] = rotate(h * head) * head ** -0.5
        n_scr[0, s] = rotate(heads * head).astype(jnp.bfloat16).astype(jnp.float32)
        n_scr[1, s] = qkv_ref[s, :, (heads + 1) * head:].astype(jnp.float32)

    win_row = lax.broadcasted_iota(jnp.int32, (16, head), 0)
    col = lax.broadcasted_iota(jnp.int32, (per_seq, cache_len), 1)
    step_of = lax.broadcasted_iota(jnp.int32, (per_seq, cache_len), 0) // heads

    def one(b):
        length = lens_ref[block * rows + b]
        for src, dst, which in ((k_ref, ko_ref, 0), (v_ref, vo_ref, 1)):
            dst[b] = src[b]
            for s in range(num_steps):
                pos = length + s
                base = pl.multiple_of((pos // 16) * 16, 16)
                window = dst[b, pl.ds(base, 16), :].astype(jnp.float32)
                fresh = n_scr[which, s, pl.ds(b, 1), :]
                window = jnp.where(win_row == pos - base, fresh, window)
                dst[b, pl.ds(base, 16), :] = window.astype(jnp.bfloat16)
        q = q_scr[pl.ds(pl.multiple_of(b * per_seq, per_seq), per_seq), :].astype(jnp.bfloat16)
        scores = lax.dot_general(q, ko_ref[b], (((1,), (1,)), ((), ())), preferred_element_type=jnp.float32)
        scores = jnp.where(col <= step_of + length, scores, -jnp.inf)
        top = jnp.max(scores, axis=1, keepdims=True)
        weight = jnp.exp(scores - top)
        total = jnp.sum(weight, axis=1, keepdims=True)
        probs = (weight / total).astype(jnp.bfloat16)
        out = jnp.dot(probs, vo_ref[b], preferred_element_type=jnp.float32)
        o_scr[pl.ds(pl.multiple_of(b * per_seq, per_seq), per_seq), :] = out

    @pl.loop(0, rows // 2)
    def _(i):
        one(2 * i)
        one(2 * i + 1)

    for s in range(num_steps):
        for h in range(heads):
            o_ref[h // pack, s, :, (h % pack) * head:(h % pack + 1) * head] = o_scr[pl.ds(s * heads + h, rows, stride=per_seq), :].astype(jnp.bfloat16)


def attention(lens, qkv, cos, sin, k_loc, v_loc, group):
    num_steps, batch, width = qkv.shape
    cache_len, head = k_loc.shape[1], k_loc.shape[2]
    attn_width = width - 2 * head
    heads = attn_width // head
    rows = 8
    row_spec = lambda last: pl.BlockSpec((num_steps, rows, last), lambda i, *_: (0, i, 0))
    cache_spec = pl.BlockSpec((rows, cache_len, head), lambda i, *_: (i, 0, 0))
    return pl.pallas_call(
        attention_kernel,
        grid_spec=pltpu.PrefetchScalarGridSpec(
            num_scalar_prefetch=1,
            grid=(batch // rows,),
            in_specs=[row_spec(width), row_spec(head), row_spec(head), cache_spec, cache_spec],
            out_specs=[pl.BlockSpec((group, num_steps, rows, attn_width // group), lambda i, *_: (0, 0, i, 0)), cache_spec, cache_spec],
            scratch_shapes=[
                pltpu.VMEM((rows * num_steps * heads, head), jnp.float32),
                pltpu.VMEM((rows * num_steps * heads, head), jnp.float32),
                pltpu.VMEM((2, num_steps, rows, head), jnp.float32),
            ],
        ),
        out_shape=[
            jax.ShapeDtypeStruct((group, num_steps, batch, attn_width // group), jnp.bfloat16),
            jax.ShapeDtypeStruct(k_loc.shape, k_loc.dtype),
            jax.ShapeDtypeStruct(v_loc.shape, v_loc.dtype),
        ],
        compiler_params=pltpu.CompilerParams(vmem_limit_bytes=48 * 1024 * 1024),
        name="attention",
    )(lens, qkv, cos, sin, k_loc, v_loc)


HALF = 128
UNIT = 2 * HALF
OWN, XN, YN, DIAG = (0, 0), (1, 0), (0, 1), (1, 1)
REDUCE_ORDER = (DIAG, XN, YN, OWN)
UNIT_HALVES = (((OWN, 0), (OWN, 1)), ((XN, 1), (YN, 0)), ((XN, 0), (YN, 1)), ((DIAG, 0), (DIAG, 1)))
MESH = pl.DeviceIdType.MESH


class Place:
    def __init__(self):
        me = lax.axis_index('tp')
        self.me = me
        self.core, self.x, self.y = me % 2, (me // 2) % 2, me // 4

    def at(self, chip, core):
        x = self.x if chip[0] == 0 else 1 - self.x
        y = self.y if chip[1] == 0 else 1 - self.y
        c = self.core if core == 0 else 1 - self.core
        return y * 4 + x * 2 + c


def everyone():
    return [(chip, core) for chip in (DIAG, XN, YN, OWN) for core in (1, 0) if (chip, core) != (OWN, 0)]


def greet(place):
    barrier = pltpu.get_barrier_semaphore()
    for chip, core in everyone():
        pl.semaphore_signal(barrier, inc=1, device_id=(place.at(chip, core),), device_id_type=MESH)
    pl.semaphore_wait(barrier, 7)


def push(src, dst, send, recv, target):
    copy = pltpu.make_async_remote_copy(src_ref=src, dst_ref=dst, send_sem=send, recv_sem=recv, device_id=(target,), device_id_type=MESH)
    copy.start()
    return copy


def reduce_rows(place, outgoing, own_block, rc, r1a, r1b, r2, csend, crecv, psend, precv, between=None):
    dim = rc.shape[2]
    partner = place.at(OWN, 1)
    to_x, to_y = place.at(XN, 0), place.at(YN, 0)
    first, second = pl.ds(0, HALF), pl.ds(HALF, HALF)
    exchange = []
    for i, chip in enumerate(REDUCE_ORDER):
        src = outgoing(i, place.at(chip, 1))
        exchange.append(push(src, rc.at[i], csend.at[i], crecv.at[i], partner))
    sends = []
    for i, chip in enumerate(REDUCE_ORDER):
        own_block(i, place.at(chip, 0), exchange[i])
        if chip == DIAG:
            sends.append(push(rc.at[i, first], r1a.at[0], psend.at[0], precv.at[0], to_x))
            sends.append(push(rc.at[i, second], r1b.at[0], psend.at[1], precv.at[1], to_y))
        elif chip == XN:
            sends.append(push(rc.at[i, first], r1a.at[1], psend.at[2], precv.at[2], to_x))
        elif chip == YN:
            sends.append(push(rc.at[i, second], r1b.at[1], psend.at[3], precv.at[3], to_y))
    for copy in exchange:
        copy.wait_send()
    for j, (slot, rows, landed, target) in enumerate(((2, 0, r1a, to_y), (1, HALF, r1b, to_x))):
        sends[j].wait_recv()

        @pl.loop(0, HALF // 16)
        def _(r):
            here = pl.ds(pl.multiple_of(rows + r * 16, 16), 16)
            there = pl.ds(pl.multiple_of(r * 16, 16), 16)
            total = rc[slot, here, :].astype(jnp.float32) + landed[0, there, :].astype(jnp.float32)
            rc[slot, here, :] = total.astype(jnp.bfloat16)

        sends.append(push(rc.at[slot, pl.ds(rows, HALF)], r2.at[j], psend.at[4 + j], precv.at[4 + j], target))
    for copy in sends[2:]:
        copy.wait_recv()
    for copy in sends:
        copy.wait_send()


def own_rows(rc, r1a, r1b, r2, half, r, rows):
    here = pl.ds(pl.multiple_of(half * HALF + r * rows, rows), rows)
    there = pl.ds(pl.multiple_of(r * rows, rows), rows)
    landed = r1b if half else r1a
    return rc[3, here, :].astype(jnp.float32) + landed[1, there, :].astype(jnp.float32) + r2[half, there, :].astype(jnp.float32)


def norm_rows(values, gain):
    centered = values - jnp.mean(values, axis=-1, keepdims=True)
    variance = jnp.mean(centered * centered, axis=-1, keepdims=True)
    return (centered * lax.rsqrt(variance + NORM_EPS) * gain).astype(jnp.bfloat16)


def gather_units(place, z, asend, arecv, work):
    partner = place.at(OWN, 1)
    to_x, to_y = place.at(XN, 0), place.at(YN, 0)
    part = lambda unit, pos: z.at[unit, pl.ds(pos * HALF, HALF)]
    sends = []

    def go(src, dst, slot, target):
        k = len(sends)
        sends.append(push(src, dst, asend.at[k], arecv.at[slot], target))
        return sends[-1]

    xb = go(part(0, 1), part(2, 0), 0, to_x)
    ya = go(part(0, 0), part(2, 1), 1, to_y)
    near = go(z.at[0], z.at[1], 2, partner)
    xa = go(part(0, 0), part(4, 0), 3, to_x)
    yb = go(part(0, 1), part(4, 1), 4, to_y)
    work(0)
    near.wait_recv()
    work(1)
    xb.wait_recv()
    db = go(part(2, 0), part(6, 1), 5, to_y)
    ya.wait_recv()
    da = go(part(2, 1), part(6, 0), 6, to_x)
    near2 = go(z.at[2], z.at[3], 7, partner)
    work(2)
    near2.wait_recv()
    work(3)
    xa.wait_recv()
    yb.wait_recv()
    near4 = go(z.at[4], z.at[5], 8, partner)
    work(4)
    near4.wait_recv()
    work(5)
    da.wait_recv()
    db.wait_recv()
    near6 = go(z.at[6], z.at[7], 9, partner)
    work(6)
    near6.wait_recv()
    work(7)
    for copy in sends:
        copy.wait_send()


def prologue_kernel(widths, part_ref, gain_ref, w_ref, x_ref, m_ref, qkv_ref, z, rc, r1a, r1b, r2, acc, qkv_out, csend, crecv, psend, precv, asend, arecv, qsend, qrecv):
    qkv_dev, ff_dev = widths
    dim = part_ref.shape[2]
    place = Place()
    greet(place)

    def own_block(i, block, copy):
        copy.wait_recv()

        @pl.loop(0, UNIT // 16)
        def _(r):
            here = pl.ds(pl.multiple_of(r * 16, 16), 16)
            rc[i, here, :] = (rc[i, here, :].astype(jnp.float32) + part_ref[block, here, :].astype(jnp.float32)).astype(jnp.bfloat16)

    reduce_rows(place, lambda i, block: part_ref.at[block], own_block, rc, r1a, r1b, r2, csend, crecv, psend, precv)
    gain = gain_ref[...].astype(jnp.float32)
    rows = 32
    for half in range(2):
        @pl.loop(0, HALF // rows)
        def _(r):
            here = pl.ds(pl.multiple_of(half * HALF + r * rows, rows), rows)
            x = own_rows(rc, r1a, r1b, r2, half, r, rows).astype(jnp.bfloat16)
            x_ref[here, :] = x
            z[0, here, :] = norm_rows(x.astype(jnp.float32), gain)

    out_sends = []

    def work(unit):
        pair, core = unit // 2, unit % 2
        tile = 512
        width = w_ref.shape[1]
        full = width // tile

        @pl.loop(0, full)
        def _(n):
            cols = pl.ds(pl.multiple_of(n * tile, tile), tile)
            acc[:, cols] = jnp.dot(z[unit], w_ref[:, cols], preferred_element_type=jnp.float32)

        acc[:, full * tile:] = jnp.dot(z[unit], w_ref[:, full * tile:], preferred_element_type=jnp.float32)
        for pos, (chip, half) in enumerate(UNIT_HALVES[pair]):
            block = place.at(chip, core)

            @pl.loop(0, HALF // 16)
            def _(r):
                here = pl.ds(pl.multiple_of(pos * HALF + r * 16, 16), 16)
                u = acc[here, :].astype(jnp.bfloat16)
                gate = u[:, qkv_dev:qkv_dev + ff_dev].astype(jnp.float32)
                up = u[:, qkv_dev + ff_dev:].astype(jnp.float32)
                act = (gate / (1.0 + jnp.exp(-gate)) * up).astype(jnp.bfloat16)
                m_ref[pl.ds(pl.multiple_of(block * UNIT + half * HALF + r * 16, 16), 16), :] = act
                qkv_out[unit, here, :] = u[:, :qkv_dev]

            src = qkv_out.at[unit, pl.ds(pos * HALF, HALF)]
            if unit == 0:
                qkv_ref[place.me, pl.ds(half * HALF, HALF), :] = qkv_out[unit, pl.ds(pos * HALF, HALF), :]
            else:
                k = len(out_sends)
                out_sends.append(push(src, qkv_ref.at[place.me, pl.ds(half * HALF, HALF)], qsend.at[k], qrecv.at[k], block))

    gather_units(place, z, asend, arecv, work)
    for copy in out_sends:
        copy.wait()


def prologue(part, gain, w_in, qkv_dev, ff_dev):
    group, rows, dim = part.shape
    vmem = pl.BlockSpec(memory_space=pltpu.VMEM)
    dma = pltpu.SemaphoreType.DMA
    return pl.pallas_call(
        functools.partial(prologue_kernel, (qkv_dev, ff_dev)),
        in_specs=[vmem] * 3,
        out_specs=[vmem] * 3,
        out_shape=[
            jax.ShapeDtypeStruct((rows, dim), jnp.bfloat16),
            jax.ShapeDtypeStruct((group * rows, ff_dev), jnp.bfloat16),
            jax.ShapeDtypeStruct((group, rows, qkv_dev), jnp.bfloat16),
        ],
        scratch_shapes=[
            pltpu.VMEM((group, rows, dim), jnp.bfloat16),
            pltpu.VMEM((4, rows, dim), jnp.bfloat16),
            pltpu.VMEM((2, HALF, dim), jnp.bfloat16),
            pltpu.VMEM((2, HALF, dim), jnp.bfloat16),
            pltpu.VMEM((2, HALF, dim), jnp.bfloat16),
            pltpu.VMEM((UNIT, w_in.shape[1]), jnp.float32),
            pltpu.VMEM((group, rows, qkv_dev), jnp.bfloat16),
            dma((4,)), dma((4,)), dma((6,)), dma((6,)), dma((10,)), dma((10,)), dma((14,)), dma((14,)),
        ],
        compiler_params=pltpu.CompilerParams(collective_id=0, has_side_effects=True, vmem_limit_bytes=60 * 1024 * 1024),
        name="prologue",
    )(part, gain, w_in)


def epilogue_kernel(scale, tile, attn_ref, m_ref, w_ref, x_ref, gain_ref, ids_ref, e_hbm, out_ref, e_buf, z, rc, r1a, r1b, r2, a_in, raw, stats, every, e_sem, csend, crecv, psend, precv, asend, arecv, qsend, qrecv, ssend, srecv):
    vocab = e_hbm.shape[0]
    tiles = vocab // tile
    cols = UNIT
    dim = z.shape[2]
    attn_dev = a_in.shape[2]
    loads = [pltpu.make_async_copy(e_hbm.at[pl.ds(t * tile, tile)], e_buf.at[pl.ds(t * tile, tile)], e_sem.at[t]) for t in range(tiles)]
    place = Place()
    greet(place)
    heads_in = {}
    for k, (chip, core) in enumerate(everyone()):
        target = place.at(chip, core)
        heads_in[(chip, core)] = push(attn_ref.at[target], a_in.at[place.me], qsend.at[k], qrecv.at[k], target)
    for c in loads:
        c.start()
    a_in[place.me] = attn_ref[place.me]

    def block_dot(block, n):
        lanes = pl.ds(pl.multiple_of(n * 512, 512), 512)
        mine = jnp.dot(a_in[block], w_ref[pl.ds(0, attn_dev), lanes], preferred_element_type=jnp.float32)
        rows = pl.ds(pl.multiple_of(block * UNIT, UNIT), UNIT)
        return mine + jnp.dot(m_ref[rows, :], w_ref[pl.ds(attn_dev, w_ref.shape[0] - attn_dev), lanes], preferred_element_type=jnp.float32)

    def outgoing(i, block):
        heads_in[(REDUCE_ORDER[i], 1)].wait_recv()

        @pl.loop(0, dim // 512)
        def _(n):
            lanes = pl.ds(pl.multiple_of(n * 512, 512), 512)
            z[2 * i, :, lanes] = block_dot(block, n).astype(jnp.bfloat16)

        return z.at[2 * i]

    def own_block(i, block, copy):
        if REDUCE_ORDER[i] != OWN:
            heads_in[(REDUCE_ORDER[i], 0)].wait_recv()
        copy.wait_recv()

        @pl.loop(0, dim // 512)
        def _(n):
            lanes = pl.ds(pl.multiple_of(n * 512, 512), 512)
            rc[i, :, lanes] = (block_dot(block, n) + rc[i, :, lanes].astype(jnp.float32)).astype(jnp.bfloat16)

    reduce_rows(place, outgoing, own_block, rc, r1a, r1b, r2, csend, crecv, psend, precv)
    gain = gain_ref[...].astype(jnp.float32)
    rows = 32
    for half in range(2):
        @pl.loop(0, HALF // rows)
        def _(r):
            here = pl.ds(pl.multiple_of(half * HALF + r * rows, rows), rows)
            o = own_rows(rc, r1a, r1b, r2, half, r, rows).astype(jnp.bfloat16).astype(jnp.float32)
            z[0, here, :] = norm_rows(x_ref[here, :].astype(jnp.float32) + o, gain)

    def work(unit):
        pair, core = unit // 2, unit % 2
        if unit == 0:
            for c in loads:
                c.wait()
        halves = [place.at(chip, core) * 2 + half for chip, half in UNIT_HALVES[pair]]
        ids = jnp.concatenate([ids_ref[h] for h in halves], axis=1)

        def product(t):
            e = e_buf[pl.ds(pl.multiple_of(t * tile, tile), tile), :]
            raw[lax.rem(t, 2)] = lax.dot_general(e, z[unit], (((1,), (1,)), ((), ())), preferred_element_type=jnp.float32)

        def absorb(t, carry):
            top, total, target = carry
            local = ids - t * tile
            part = raw[lax.rem(t, 2)].reshape(tile // 8, 8, cols)
            new_top = jnp.maximum(top, jnp.max(part, axis=0))
            total = total * jnp.exp2((top - new_top) * (scale * LOG2E))
            total = total + jnp.sum(jnp.exp2((part - new_top[None]) * (scale * LOG2E)), axis=0)
            index = lax.broadcasted_iota(jnp.int32, part.shape, 0) * 8 + lax.broadcasted_iota(jnp.int32, part.shape, 1)
            target = target + jnp.sum(jnp.where(index == local[None], part, 0.0), axis=0)
            return new_top, total, target

        product(0)
        start = (jnp.full((8, cols), -jnp.inf, jnp.float32), jnp.zeros((8, cols), jnp.float32), jnp.zeros((8, cols), jnp.float32))

        def body(t, carry):
            product(t)
            return absorb(t - 1, carry)

        top, total, target = absorb(tiles - 1, lax.fori_loop(1, tiles, body, start))
        best = jnp.max(top, axis=0, keepdims=True)
        total = jnp.sum(total * jnp.exp2((top - best) * (scale * LOG2E)), axis=0, keepdims=True)
        target = jnp.sum(target, axis=0, keepdims=True)
        for pos, h in enumerate(halves):
            lanes = slice(pos * HALF, (pos + 1) * HALF)
            stats[0, pl.ds(h, 1), :] = best[:, lanes] * scale
            stats[1, pl.ds(h, 1), :] = total[:, lanes]
            stats[2, pl.ds(h, 1), :] = target[:, lanes] * scale

    gather_units(place, z, asend, arecv, work)
    finals = []
    for k, (chip, core) in enumerate(everyone()):
        finals.append(push(stats, every.at[place.me], ssend.at[k], srecv.at[k], place.at(chip, core)))
    every[place.me] = stats[...]
    for copy in finals:
        copy.wait()
    for copy in heads_in.values():
        copy.wait_send()
    tops = every[:, 0]
    best = jnp.max(tops, axis=0)
    total = jnp.sum(every[:, 1] * jnp.exp(tops - best[None]), axis=0)
    out_ref[...] = jnp.sum(every[:, 2], axis=0) - best - jnp.log(total)


def epilogue(attn, m, w_out, x_own, gain, ids, embed_loc):
    group, rows, attn_dev = attn.shape
    vocab, dim = embed_loc.shape
    tile = 560
    vmem = pl.BlockSpec(memory_space=pltpu.VMEM)
    dma = pltpu.SemaphoreType.DMA
    halves = group * rows // HALF
    return pl.pallas_call(
        functools.partial(epilogue_kernel, dim ** -0.5, tile),
        in_specs=[vmem] * 6 + [pl.BlockSpec(memory_space=pl.ANY)],
        out_specs=vmem,
        out_shape=jax.ShapeDtypeStruct((halves, HALF), jnp.float32),
        scratch_shapes=[
            pltpu.VMEM((vocab, dim), jnp.bfloat16),
            pltpu.VMEM((group, rows, dim), jnp.bfloat16),
            pltpu.VMEM((4, rows, dim), jnp.bfloat16),
            pltpu.VMEM((2, HALF, dim), jnp.bfloat16),
            pltpu.VMEM((2, HALF, dim), jnp.bfloat16),
            pltpu.VMEM((2, HALF, dim), jnp.bfloat16),
            pltpu.VMEM((group, rows, attn_dev), jnp.bfloat16),
            pltpu.VMEM((2, tile, UNIT), jnp.float32),
            pltpu.VMEM((3, halves, HALF), jnp.float32),
            pltpu.VMEM((group, 3, halves, HALF), jnp.float32),
            dma((vocab // tile,)),
            dma((4,)), dma((4,)), dma((6,)), dma((6,)), dma((10,)), dma((10,)), dma((7,)), dma((7,)), dma((7,)), dma((7,)),
        ],
        compiler_params=pltpu.CompilerParams(collective_id=1, has_side_effects=True, vmem_limit_bytes=67043328),
        name="epilogue",
    )(attn, m, w_out, x_own, gain, ids, embed_loc)


def solution(mesh):
    group_size = mesh.shape['tp']

    def device_fn(tok_ids, next_ids, seq_lens, embed_loc, ln_gain, w_in_loc, w_out_loc, final_gain, k_loc, v_loc):
        num_steps, batch_size = tok_ids.shape
        batch_dev = batch_size // group_size
        rows_dev = num_steps * batch_dev
        vocab_dev, model_dim = embed_loc.shape
        head_dim = k_loc.shape[2]
        in_dev = w_in_loc.shape[1]
        out_dev = w_out_loc.shape[0]
        kv_dev = 2 * head_dim // group_size
        attn_dev = 2 * out_dev - in_dev + kv_dev
        ff_dev = out_dev - attn_dev
        qkv_dev = attn_dev + kv_dev
        dev_index = lax.axis_index('tp')
        vocab_start = dev_index * vocab_dev
        own_lens = lax.dynamic_slice_in_dim(seq_lens, dev_index * batch_dev, batch_dev)

        def by_device(ids):
            return ids.reshape(num_steps, group_size, batch_dev).transpose(1, 0, 2)

        local_ids = by_device(tok_ids).reshape(-1) - vocab_start
        tok_here = (local_ids >= 0) & (local_ids < vocab_dev)
        emb_rows = jnp.take(embed_loc, jnp.clip(local_ids, 0, vocab_dev - 1), axis=0)
        x_part = jnp.where(tok_here[:, None], emb_rows, jnp.zeros_like(emb_rows))
        x_own, mlp_act, qkv_own = prologue(x_part.reshape(group_size, rows_dev, model_dim), ln_gain[None], w_in_loc, qkv_dev, ff_dev)
        qkv_own = qkv_own.transpose(1, 0, 2).reshape(num_steps, batch_dev, -1)

        half = head_dim // 2
        inv_freq = ROPE_BASE ** (-jnp.arange(half, dtype=jnp.float32) / half)
        positions = own_lens[None, :] + jnp.arange(num_steps, dtype=jnp.int32)[:, None]
        angles = positions.astype(jnp.float32)[..., None] * inv_freq
        cos, sin = jnp.cos(angles), jnp.sin(angles)
        cos = jnp.concatenate([cos, cos], axis=-1)
        sin = jnp.concatenate([-sin, sin], axis=-1)
        attn_out, k_out, v_out = attention(own_lens, qkv_own, cos, sin, k_loc, v_loc, group_size)
        local_next = by_device(next_ids).reshape(2 * group_size, 1, batch_dev) - vocab_start
        ids8 = jnp.broadcast_to(local_next, (2 * group_size, 8, batch_dev))
        log_probs = epilogue(attn_out.reshape(group_size, rows_dev, attn_dev), mlp_act, w_out_loc, x_own, final_gain[None], ids8, embed_loc)
        log_probs = log_probs.reshape(group_size, num_steps, batch_dev).transpose(1, 0, 2).reshape(num_steps, batch_size)
        return log_probs, k_out, v_out

    cache_spec = P('tp', None, None)
    return jax.shard_map(device_fn, mesh=mesh, in_specs=(P(), P(), P(), P('tp', None), P(), P(None, 'tp'), P('tp', None), P(), cache_spec, cache_spec), out_specs=(P(), cache_spec, cache_spec), check_vma=False)
```

```python
import functools

import jax
import jax.numpy as jnp
from jax import lax
from jax.experimental import pallas as pl
from jax.experimental.pallas import tpu as pltpu
from jax.sharding import PartitionSpec as P

ROPE_BASE = 10000.0
NORM_EPS = 1e-6
LOG2E = 1.4426950408889634


def layer_norm(values, gain_vec):
    centered = values.astype(jnp.float32)
    centered = centered - jnp.mean(centered, axis=-1, keepdims=True)
    variance = jnp.mean(jnp.square(centered), axis=-1, keepdims=True)
    scaled = centered * lax.rsqrt(variance + NORM_EPS) * gain_vec.astype(jnp.float32)
    return scaled.astype(jnp.bfloat16)


def attention_kernel(lens_ref, qkv_ref, cos_ref, sin_ref, k_ref, v_ref, o_ref, ko_ref, vo_ref, q_scr, o_scr, n_scr):
    num_steps, rows, _ = qkv_ref.shape
    cache_len, head = k_ref.shape[1], k_ref.shape[2]
    pack = o_ref.shape[3] // head
    heads = o_ref.shape[0] * pack
    block = pl.program_id(0)
    per_seq = num_steps * heads
    for s in range(num_steps):
        cos, sin = cos_ref[s], sin_ref[s]

        def rotate(lo):
            x = qkv_ref[s, :, lo:lo + head].astype(jnp.float32)
            return x * cos + pltpu.roll(x, head // 2, 1) * sin

        for h in range(heads):
            q_scr[pl.ds(s * heads + h, rows, stride=per_seq), :] = rotate(h * head) * head ** -0.5
        n_scr[0, s] = rotate(heads * head).astype(jnp.bfloat16).astype(jnp.float32)
        n_scr[1, s] = qkv_ref[s, :, (heads + 1) * head:].astype(jnp.float32)

    win_row = lax.broadcasted_iota(jnp.int32, (16, head), 0)
    col = lax.broadcasted_iota(jnp.int32, (per_seq, cache_len), 1)
    step_of = lax.broadcasted_iota(jnp.int32, (per_seq, cache_len), 0) // heads

    def one(b):
        length = lens_ref[block * rows + b]
        for src, dst, which in ((k_ref, ko_ref, 0), (v_ref, vo_ref, 1)):
            dst[b] = src[b]
            for s in range(num_steps):
                pos = length + s
                base = pl.multiple_of((pos // 16) * 16, 16)
                window = dst[b, pl.ds(base, 16), :].astype(jnp.float32)
                fresh = n_scr[which, s, pl.ds(b, 1), :]
                window = jnp.where(win_row == pos - base, fresh, window)
                dst[b, pl.ds(base, 16), :] = window.astype(jnp.bfloat16)
        q = q_scr[pl.ds(pl.multiple_of(b * per_seq, per_seq), per_seq), :].astype(jnp.bfloat16)
        scores = lax.dot_general(q, ko_ref[b], (((1,), (1,)), ((), ())), preferred_element_type=jnp.float32)
        scores = jnp.where(col <= step_of + length, scores, -jnp.inf)
        top = jnp.max(scores, axis=1, keepdims=True)
        weight = jnp.exp(scores - top)
        total = jnp.sum(weight, axis=1, keepdims=True)
        probs = (weight / total).astype(jnp.bfloat16)
        out = jnp.dot(probs, vo_ref[b], preferred_element_type=jnp.float32)
        o_scr[pl.ds(pl.multiple_of(b * per_seq, per_seq), per_seq), :] = out

    @pl.loop(0, rows // 2)
    def _(i):
        one(2 * i)
        one(2 * i + 1)

    for s in range(num_steps):
        for h in range(heads):
            o_ref[h // pack, s, :, (h % pack) * head:(h % pack + 1) * head] = o_scr[pl.ds(s * heads + h, rows, stride=per_seq), :].astype(jnp.bfloat16)


def attention(lens, qkv, cos, sin, k_loc, v_loc, group):
    num_steps, batch, width = qkv.shape
    cache_len, head = k_loc.shape[1], k_loc.shape[2]
    attn_width = width - 2 * head
    heads = attn_width // head
    rows = 8
    row_spec = lambda last: pl.BlockSpec((num_steps, rows, last), lambda i, *_: (0, i, 0))
    cache_spec = pl.BlockSpec((rows, cache_len, head), lambda i, *_: (i, 0, 0))
    return pl.pallas_call(
        attention_kernel,
        grid_spec=pltpu.PrefetchScalarGridSpec(
            num_scalar_prefetch=1,
            grid=(batch // rows,),
            in_specs=[row_spec(width), row_spec(head), row_spec(head), cache_spec, cache_spec],
            out_specs=[pl.BlockSpec((group, num_steps, rows, attn_width // group), lambda i, *_: (0, 0, i, 0)), cache_spec, cache_spec],
            scratch_shapes=[
                pltpu.VMEM((rows * num_steps * heads, head), jnp.float32),
                pltpu.VMEM((rows * num_steps * heads, head), jnp.float32),
                pltpu.VMEM((2, num_steps, rows, head), jnp.float32),
            ],
        ),
        out_shape=[
            jax.ShapeDtypeStruct((group, num_steps, batch, attn_width // group), jnp.bfloat16),
            jax.ShapeDtypeStruct(k_loc.shape, k_loc.dtype),
            jax.ShapeDtypeStruct(v_loc.shape, v_loc.dtype),
        ],
        compiler_params=pltpu.CompilerParams(vmem_limit_bytes=48 * 1024 * 1024),
        name="attention",
    )(lens, qkv, cos, sin, k_loc, v_loc)


HALF = 128
UNIT = 2 * HALF
OWN, XN, YN, DIAG = (0, 0), (1, 0), (0, 1), (1, 1)
REDUCE_ORDER = (DIAG, XN, YN, OWN)
UNIT_HALVES = (((OWN, 0), (OWN, 1)), ((XN, 1), (YN, 0)), ((XN, 0), (YN, 1)), ((DIAG, 0), (DIAG, 1)))
MESH = pl.DeviceIdType.MESH


class Place:
    def __init__(self):
        me = lax.axis_index('tp')
        self.me = me
        self.core, self.x, self.y = me % 2, (me // 2) % 2, me // 4

    def at(self, chip, core):
        x = self.x if chip[0] == 0 else 1 - self.x
        y = self.y if chip[1] == 0 else 1 - self.y
        c = self.core if core == 0 else 1 - self.core
        return y * 4 + x * 2 + c


def everyone():
    return [(chip, core) for chip in (DIAG, XN, YN, OWN) for core in (1, 0) if (chip, core) != (OWN, 0)]


def greet(place):
    barrier = pltpu.get_barrier_semaphore()
    for chip, core in everyone():
        pl.semaphore_signal(barrier, inc=1, device_id=(place.at(chip, core),), device_id_type=MESH)
    pl.semaphore_wait(barrier, 7)


def push(src, dst, send, recv, target):
    copy = pltpu.make_async_remote_copy(src_ref=src, dst_ref=dst, send_sem=send, recv_sem=recv, device_id=(target,), device_id_type=MESH)
    copy.start()
    return copy


def reduce_rows(place, outgoing, own_block, rc, r1a, r1b, r2, csend, crecv, psend, precv, between=None):
    dim = rc.shape[2]
    partner = place.at(OWN, 1)
    to_x, to_y = place.at(XN, 0), place.at(YN, 0)
    first, second = pl.ds(0, HALF), pl.ds(HALF, HALF)
    exchange = []
    for i, chip in enumerate(REDUCE_ORDER):
        src = outgoing(i, place.at(chip, 1))
        exchange.append(push(src, rc.at[i], csend.at[i], crecv.at[i], partner))
    sends = []
    for i, chip in enumerate(REDUCE_ORDER):
        own_block(i, place.at(chip, 0), exchange[i])
        if chip == DIAG:
            sends.append(push(rc.at[i, first], r1a.at[0], psend.at[0], precv.at[0], to_x))
            sends.append(push(rc.at[i, second], r1b.at[0], psend.at[1], precv.at[1], to_y))
        elif chip == XN:
            sends.append(push(rc.at[i, first], r1a.at[1], psend.at[2], precv.at[2], to_x))
        elif chip == YN:
            sends.append(push(rc.at[i, second], r1b.at[1], psend.at[3], precv.at[3], to_y))
    for copy in exchange:
        copy.wait_send()
    for j, (slot, rows, landed, target) in enumerate(((2, 0, r1a, to_y), (1, HALF, r1b, to_x))):
        sends[j].wait_recv()

        @pl.loop(0, HALF // 16)
        def _(r):
            here = pl.ds(pl.multiple_of(rows + r * 16, 16), 16)
            there = pl.ds(pl.multiple_of(r * 16, 16), 16)
            total = rc[slot, here, :].astype(jnp.float32) + landed[0, there, :].astype(jnp.float32)
            rc[slot, here, :] = total.astype(jnp.bfloat16)

        sends.append(push(rc.at[slot, pl.ds(rows, HALF)], r2.at[j], psend.at[4 + j], precv.at[4 + j], target))
    for copy in sends[2:]:
        copy.wait_recv()
    for copy in sends:
        copy.wait_send()


def own_rows(rc, r1a, r1b, r2, half, r, rows):
    here = pl.ds(pl.multiple_of(half * HALF + r * rows, rows), rows)
    there = pl.ds(pl.multiple_of(r * rows, rows), rows)
    landed = r1b if half else r1a
    return rc[3, here, :].astype(jnp.float32) + landed[1, there, :].astype(jnp.float32) + r2[half, there, :].astype(jnp.float32)


def norm_rows(values, gain):
    centered = values - jnp.mean(values, axis=-1, keepdims=True)
    variance = jnp.mean(centered * centered, axis=-1, keepdims=True)
    return (centered * lax.rsqrt(variance + NORM_EPS) * gain).astype(jnp.bfloat16)


def gather_units(place, z, asend, arecv, work):
    partner = place.at(OWN, 1)
    to_x, to_y = place.at(XN, 0), place.at(YN, 0)
    part = lambda unit, pos: z.at[unit, pl.ds(pos * HALF, HALF)]
    sends = []

    def go(src, dst, slot, target):
        k = len(sends)
        sends.append(push(src, dst, asend.at[k], arecv.at[slot], target))
        return sends[-1]

    xb = go(part(0, 1), part(2, 0), 0, to_x)
    ya = go(part(0, 0), part(2, 1), 1, to_y)
    near = go(z.at[0], z.at[1], 2, partner)
    xa = go(part(0, 0), part(4, 0), 3, to_x)
    yb = go(part(0, 1), part(4, 1), 4, to_y)
    near.wait_recv()
    work(0)
    xb.wait_recv()
    db = go(part(2, 0), part(6, 1), 5, to_y)
    ya.wait_recv()
    da = go(part(2, 1), part(6, 0), 6, to_x)
    near2 = go(z.at[2], z.at[3], 7, partner)
    near2.wait_recv()
    work(1)
    xa.wait_recv()
    yb.wait_recv()
    near4 = go(z.at[4], z.at[5], 8, partner)
    near4.wait_recv()
    work(2)
    da.wait_recv()
    db.wait_recv()
    near6 = go(z.at[6], z.at[7], 9, partner)
    near6.wait_recv()
    work(3)
    for copy in sends:
        copy.wait_send()


def prologue_kernel(widths, part_ref, gain_ref, w_hbm, x_ref, m_ref, qkv_ref, z, rc, r1a, r1b, r2, w_buf, qkv_out, w_sem, csend, crecv, psend, precv, asend, arecv, qsend, qrecv):
    qkv_dev, ff_dev = widths
    dim = part_ref.shape[2]
    place = Place()
    greet(place)
    load = pltpu.make_async_copy(w_hbm, w_buf, w_sem)
    load.start()

    def own_block(i, block, copy):
        copy.wait_recv()

        @pl.loop(0, UNIT // 16)
        def _(r):
            here = pl.ds(pl.multiple_of(r * 16, 16), 16)
            rc[i, here, :] = (rc[i, here, :].astype(jnp.float32) + part_ref[block, here, :].astype(jnp.float32)).astype(jnp.bfloat16)

    reduce_rows(place, lambda i, block: part_ref.at[block], own_block, rc, r1a, r1b, r2, csend, crecv, psend, precv)
    gain = gain_ref[...].astype(jnp.float32)
    rows = 32
    for half in range(2):
        @pl.loop(0, HALF // rows)
        def _(r):
            here = pl.ds(pl.multiple_of(half * HALF + r * rows, rows), rows)
            x = own_rows(rc, r1a, r1b, r2, half, r, rows).astype(jnp.bfloat16)
            x_ref[here, :] = x
            z[0, here, :] = norm_rows(x.astype(jnp.float32), gain)

    out_sends = []

    def times(rows, first, count):
        return lax.dot_general(rows, w_buf[pl.ds(first, count), :], (((1,), (1,)), ((), ())), preferred_element_type=jnp.float32)

    def work(pair):
        if pair == 0:
            load.wait()
        rows = z[2 * pair:2 * pair + 2].reshape(2 * UNIT, dim)
        qkv_out[2 * pair:2 * pair + 2] = times(rows, 0, qkv_dev).astype(jnp.bfloat16).reshape(2, UNIT, qkv_dev)
        for core in range(2):
            for pos, (chip, half) in enumerate(UNIT_HALVES[pair]):
                unit = 2 * pair + core
                block = place.at(chip, core)
                src = qkv_out.at[unit, pl.ds(pos * HALF, HALF)]
                if unit == 0:
                    qkv_ref[place.me, pl.ds(half * HALF, HALF), :] = qkv_out[unit, pl.ds(pos * HALF, HALF), :]
                else:
                    k = len(out_sends)
                    out_sends.append(push(src, qkv_ref.at[place.me, pl.ds(half * HALF, HALF)], qsend.at[k], qrecv.at[k], block))
        tile = 256

        @pl.loop(0, ff_dev // tile)
        def _(n):
            at = pl.multiple_of(n * tile, tile)
            gate = times(rows, pl.multiple_of(qkv_dev + at, 16), tile).astype(jnp.bfloat16).astype(jnp.float32)
            up = times(rows, pl.multiple_of(qkv_dev + ff_dev + at, 16), tile).astype(jnp.bfloat16).astype(jnp.float32)
            act = (gate / (1.0 + jnp.exp(-gate)) * up).astype(jnp.bfloat16)
            for core in range(2):
                for pos, (chip, half) in enumerate(UNIT_HALVES[pair]):
                    first = place.at(chip, core) * UNIT + half * HALF
                    k = core * UNIT + pos * HALF
                    m_ref[pl.ds(pl.multiple_of(first, HALF), HALF), pl.ds(at, tile)] = act[k:k + HALF]

    gather_units(place, z, asend, arecv, work)
    for copy in out_sends:
        copy.wait()


def prologue(part, gain, w_in, qkv_dev, ff_dev):
    group, rows, dim = part.shape
    vmem = pl.BlockSpec(memory_space=pltpu.VMEM)
    dma = pltpu.SemaphoreType.DMA
    return pl.pallas_call(
        functools.partial(prologue_kernel, (qkv_dev, ff_dev)),
        in_specs=[vmem] * 2 + [pl.BlockSpec(memory_space=pl.ANY)],
        out_specs=[vmem] * 3,
        out_shape=[
            jax.ShapeDtypeStruct((rows, dim), jnp.bfloat16),
            jax.ShapeDtypeStruct((group * rows, ff_dev), jnp.bfloat16),
            jax.ShapeDtypeStruct((group, rows, qkv_dev), jnp.bfloat16),
        ],
        scratch_shapes=[
            pltpu.VMEM((group, rows, dim), jnp.bfloat16),
            pltpu.VMEM((4, rows, dim), jnp.bfloat16),
            pltpu.VMEM((2, HALF, dim), jnp.bfloat16),
            pltpu.VMEM((2, HALF, dim), jnp.bfloat16),
            pltpu.VMEM((2, HALF, dim), jnp.bfloat16),
            pltpu.VMEM(w_in.shape, jnp.bfloat16),
            pltpu.VMEM((group, rows, qkv_dev), jnp.bfloat16),
            dma,
            dma((4,)), dma((4,)), dma((6,)), dma((6,)), dma((10,)), dma((10,)), dma((14,)), dma((14,)),
        ],
        compiler_params=pltpu.CompilerParams(collective_id=0, has_side_effects=True, vmem_limit_bytes=60 * 1024 * 1024),
        name="prologue",
    )(part, gain, w_in)


def epilogue_kernel(scale, tile, attn_ref, m_ref, w_ref, x_ref, gain_ref, ids_ref, e_hbm, out_ref, e_buf, z, rc, r1a, r1b, r2, a_in, raw, stats, every, e_sem, csend, crecv, psend, precv, asend, arecv, qsend, qrecv, ssend, srecv):
    vocab = e_hbm.shape[0]
    tiles = vocab // tile
    cols = 2 * UNIT
    dim = z.shape[2]
    attn_dev = a_in.shape[2]
    loads = [pltpu.make_async_copy(e_hbm.at[pl.ds(t * tile, tile)], e_buf.at[pl.ds(t * tile, tile)], e_sem.at[t]) for t in range(tiles)]
    place = Place()
    greet(place)
    heads_in = {}
    for k, (chip, core) in enumerate(everyone()):
        target = place.at(chip, core)
        heads_in[(chip, core)] = push(attn_ref.at[target], a_in.at[place.me], qsend.at[k], qrecv.at[k], target)
    for c in loads:
        c.start()
    a_in[place.me] = attn_ref[place.me]

    def block_dot(block, n):
        lanes = pl.ds(pl.multiple_of(n * 512, 512), 512)
        mine = jnp.dot(a_in[block], w_ref[pl.ds(0, attn_dev), lanes], preferred_element_type=jnp.float32)
        rows = pl.ds(pl.multiple_of(block * UNIT, UNIT), UNIT)
        return mine + jnp.dot(m_ref[rows, :], w_ref[pl.ds(attn_dev, w_ref.shape[0] - attn_dev), lanes], preferred_element_type=jnp.float32)

    def outgoing(i, block):
        heads_in[(REDUCE_ORDER[i], 1)].wait_recv()

        @pl.loop(0, dim // 512)
        def _(n):
            lanes = pl.ds(pl.multiple_of(n * 512, 512), 512)
            z[2 * i, :, lanes] = block_dot(block, n).astype(jnp.bfloat16)

        return z.at[2 * i]

    def own_block(i, block, copy):
        if REDUCE_ORDER[i] != OWN:
            heads_in[(REDUCE_ORDER[i], 0)].wait_recv()
        copy.wait_recv()

        @pl.loop(0, dim // 512)
        def _(n):
            lanes = pl.ds(pl.multiple_of(n * 512, 512), 512)
            rc[i, :, lanes] = (block_dot(block, n) + rc[i, :, lanes].astype(jnp.float32)).astype(jnp.bfloat16)

    reduce_rows(place, outgoing, own_block, rc, r1a, r1b, r2, csend, crecv, psend, precv)
    gain = gain_ref[...].astype(jnp.float32)
    rows = 32
    for half in range(2):
        @pl.loop(0, HALF // rows)
        def _(r):
            here = pl.ds(pl.multiple_of(half * HALF + r * rows, rows), rows)
            o = own_rows(rc, r1a, r1b, r2, half, r, rows).astype(jnp.bfloat16).astype(jnp.float32)
            z[0, here, :] = norm_rows(x_ref[here, :].astype(jnp.float32) + o, gain)

    def work(pair):
        if pair == 0:
            for c in loads:
                c.wait()
        halves = [place.at(chip, core) * 2 + half for core in range(2) for chip, half in UNIT_HALVES[pair]]
        row = lax.broadcasted_iota(jnp.int32, (8, cols), 0)
        ids = jnp.concatenate([ids_ref[h] for h in halves], axis=1) - row
        rate = scale * LOG2E

        def product(t, slot):
            e = e_buf[pl.ds(pl.multiple_of(t * tile, 16), tile), :]
            rows = z[2 * pair:2 * pair + 2].reshape(cols, dim)
            raw[slot] = lax.dot_general(e, rows, (((1,), (1,)), ((), ())), preferred_element_type=jnp.float32)

        def absorb(t, slot, carry):
            top, total, target = carry
            local = ids - t * tile
            count = tile // 8
            tops = [top, None]
            for r in range(count):
                v = raw[slot, r * 8:r * 8 + 8, :]
                k = r % 2
                tops[k] = v if tops[k] is None else jnp.maximum(tops[k], v)
            new_top = jnp.maximum(tops[0], tops[1])
            sums = [total * jnp.exp2((top - new_top) * rate), None]
            for r in range(count):
                v = raw[slot, r * 8:r * 8 + 8, :]
                k = r % 2
                p = jnp.exp2((v - new_top) * rate)
                sums[k] = p if sums[k] is None else sums[k] + p
                target = target + jnp.where(local == r * 8, v, 0.0)
            return new_top, sums[0] + sums[1], target

        zero = jnp.zeros((8, cols), jnp.float32)
        product(0, 0)

        def body(i, carry):
            product(2 * i + 1, 1)
            carry = absorb(2 * i, 0, carry)
            product(2 * i + 2, 0)
            return absorb(2 * i + 1, 1, carry)

        carry = lax.fori_loop(0, (tiles - 1) // 2, body, (jnp.full((8, cols), -jnp.inf, jnp.float32), zero, zero))
        if tiles % 2 == 0:
            product(tiles - 1, 1)
            carry = absorb(tiles - 2, 0, carry)
        top, total, target = absorb(tiles - 1, (tiles - 1) % 2, carry)
        best = jnp.max(top, axis=0, keepdims=True)
        total = jnp.sum(total * jnp.exp2((top - best) * rate), axis=0, keepdims=True)
        target = jnp.sum(target, axis=0, keepdims=True)
        for pos, h in enumerate(halves):
            lanes = slice(pos * HALF, (pos + 1) * HALF)
            stats[0, pl.ds(h, 1), :] = best[:, lanes] * scale
            stats[1, pl.ds(h, 1), :] = total[:, lanes]
            stats[2, pl.ds(h, 1), :] = target[:, lanes] * scale

    gather_units(place, z, asend, arecv, work)
    finals = []
    for k, (chip, core) in enumerate(everyone()):
        finals.append(push(stats, every.at[place.me], ssend.at[k], srecv.at[k], place.at(chip, core)))
    every[place.me] = stats[...]
    for copy in finals:
        copy.wait()
    for copy in heads_in.values():
        copy.wait_send()
    tops = every[:, 0]
    best = jnp.max(tops, axis=0)
    total = jnp.sum(every[:, 1] * jnp.exp(tops - best[None]), axis=0)
    out_ref[...] = jnp.sum(every[:, 2], axis=0) - best - jnp.log(total)


def epilogue(attn, m, w_out, x_own, gain, ids, embed_loc):
    group, rows, attn_dev = attn.shape
    vocab, dim = embed_loc.shape
    tile = 560
    vmem = pl.BlockSpec(memory_space=pltpu.VMEM)
    dma = pltpu.SemaphoreType.DMA
    halves = group * rows // HALF
    return pl.pallas_call(
        functools.partial(epilogue_kernel, dim ** -0.5, tile),
        in_specs=[vmem] * 6 + [pl.BlockSpec(memory_space=pl.ANY)],
        out_specs=vmem,
        out_shape=jax.ShapeDtypeStruct((halves, HALF), jnp.float32),
        scratch_shapes=[
            pltpu.VMEM((vocab, dim), jnp.bfloat16),
            pltpu.VMEM((group, rows, dim), jnp.bfloat16),
            pltpu.VMEM((4, rows, dim), jnp.bfloat16),
            pltpu.VMEM((2, HALF, dim), jnp.bfloat16),
            pltpu.VMEM((2, HALF, dim), jnp.bfloat16),
            pltpu.VMEM((2, HALF, dim), jnp.bfloat16),
            pltpu.VMEM((group, rows, attn_dev), jnp.bfloat16),
            pltpu.VMEM((2, tile, 2 * UNIT), jnp.float32),
            pltpu.VMEM((3, halves, HALF), jnp.float32),
            pltpu.VMEM((group, 3, halves, HALF), jnp.float32),
            dma((vocab // tile,)),
            dma((4,)), dma((4,)), dma((6,)), dma((6,)), dma((10,)), dma((10,)), dma((7,)), dma((7,)), dma((7,)), dma((7,)),
        ],
        compiler_params=pltpu.CompilerParams(collective_id=1, has_side_effects=True, vmem_limit_bytes=67043328),
        name="epilogue",
    )(attn, m, w_out, x_own, gain, ids, embed_loc)


def solution(mesh):
    group_size = mesh.shape['tp']

    def device_fn(tok_ids, next_ids, seq_lens, embed_loc, ln_gain, w_in_loc, w_out_loc, final_gain, k_loc, v_loc):
        num_steps, batch_size = tok_ids.shape
        batch_dev = batch_size // group_size
        rows_dev = num_steps * batch_dev
        vocab_dev, model_dim = embed_loc.shape
        head_dim = k_loc.shape[2]
        in_dev = w_in_loc.shape[1]
        out_dev = w_out_loc.shape[0]
        kv_dev = 2 * head_dim // group_size
        attn_dev = 2 * out_dev - in_dev + kv_dev
        ff_dev = out_dev - attn_dev
        qkv_dev = attn_dev + kv_dev
        dev_index = lax.axis_index('tp')
        vocab_start = dev_index * vocab_dev
        own_lens = lax.dynamic_slice_in_dim(seq_lens, dev_index * batch_dev, batch_dev)

        def by_device(ids):
            return ids.reshape(num_steps, group_size, batch_dev).transpose(1, 0, 2)

        local_ids = by_device(tok_ids).reshape(-1) - vocab_start
        tok_here = (local_ids >= 0) & (local_ids < vocab_dev)
        emb_rows = jnp.take(embed_loc, jnp.clip(local_ids, 0, vocab_dev - 1), axis=0)
        x_part = jnp.where(tok_here[:, None], emb_rows, jnp.zeros_like(emb_rows))
        x_own, mlp_act, qkv_own = prologue(x_part.reshape(group_size, rows_dev, model_dim), ln_gain[None], w_in_loc.T, qkv_dev, ff_dev)
        qkv_own = qkv_own.transpose(1, 0, 2).reshape(num_steps, batch_dev, -1)

        half = head_dim // 2
        inv_freq = ROPE_BASE ** (-jnp.arange(half, dtype=jnp.float32) / half)
        positions = own_lens[None, :] + jnp.arange(num_steps, dtype=jnp.int32)[:, None]
        angles = positions.astype(jnp.float32)[..., None] * inv_freq
        cos, sin = jnp.cos(angles), jnp.sin(angles)
        cos = jnp.concatenate([cos, cos], axis=-1)
        sin = jnp.concatenate([-sin, sin], axis=-1)
        attn_out, k_out, v_out = attention(own_lens, qkv_own, cos, sin, k_loc, v_loc, group_size)
        local_next = by_device(next_ids).reshape(2 * group_size, 1, batch_dev) - vocab_start
        ids8 = jnp.broadcast_to(local_next, (2 * group_size, 8, batch_dev))
        log_probs = epilogue(attn_out.reshape(group_size, rows_dev, attn_dev), mlp_act, w_out_loc, x_own, final_gain[None], ids8, embed_loc)
        log_probs = log_probs.reshape(group_size, num_steps, batch_dev).transpose(1, 0, 2).reshape(num_steps, batch_size)
        return log_probs, k_out, v_out

    cache_spec = P('tp', None, None)
    return jax.shard_map(device_fn, mesh=mesh, in_specs=(P(), P(), P(), P('tp', None), P(), P(None, 'tp'), P('tp', None), P(), cache_spec, cache_spec), out_specs=(P(), cache_spec, cache_spec), check_vma=False)
```

```python
import functools

import jax
import jax.numpy as jnp
from jax import lax
from jax.experimental import pallas as pl
from jax.experimental.pallas import tpu as pltpu
from jax.sharding import PartitionSpec as P

ROPE_BASE = 10000.0
NORM_EPS = 1e-6
LOG2E = 1.4426950408889634


def layer_norm(values, gain_vec):
    centered = values.astype(jnp.float32)
    centered = centered - jnp.mean(centered, axis=-1, keepdims=True)
    variance = jnp.mean(jnp.square(centered), axis=-1, keepdims=True)
    scaled = centered * lax.rsqrt(variance + NORM_EPS) * gain_vec.astype(jnp.float32)
    return scaled.astype(jnp.bfloat16)


def attention_kernel(lens_ref, qkv_ref, cos_ref, sin_ref, k_ref, v_ref, o_ref, ko_ref, vo_ref, q_scr, o_scr, n_scr, s_scr, p_scr):
    num_steps, rows, _ = qkv_ref.shape
    cache_len, head = k_ref.shape[1], k_ref.shape[2]
    pack = o_ref.shape[3] // head
    heads = o_ref.shape[0] * pack
    block = pl.program_id(0)
    per_seq = num_steps * heads
    for s in range(num_steps):
        cos, sin = cos_ref[s], sin_ref[s]

        def rotate(lo):
            x = qkv_ref[s, :, lo:lo + head].astype(jnp.float32)
            return x * cos + pltpu.roll(x, head // 2, 1) * sin

        for h in range(heads):
            q_scr[pl.ds(s * heads + h, rows, stride=per_seq), :] = rotate(h * head) * head ** -0.5
        n_scr[0, s] = rotate(heads * head).astype(jnp.bfloat16).astype(jnp.float32)
        n_scr[1, s] = qkv_ref[s, :, (heads + 1) * head:].astype(jnp.float32)

    win_row = lax.broadcasted_iota(jnp.int32, (16, head), 0)
    col = lax.broadcasted_iota(jnp.int32, (per_seq, cache_len), 1) - lax.broadcasted_iota(jnp.int32, (per_seq, cache_len), 0) // heads
    depth = s_scr.shape[0]

    def insert(b):
        length = lens_ref[block * rows + b]
        for src, dst, which in ((k_ref, ko_ref, 0), (v_ref, vo_ref, 1)):
            dst[b] = src[b]
            for s in range(num_steps):
                pos = length + s
                base = pl.multiple_of((pos // 16) * 16, 16)
                window = dst[b, pl.ds(base, 16), :].astype(jnp.float32)
                fresh = n_scr[which, s, b:b + 1, :]
                window = jnp.where(win_row == pos - base, fresh, window)
                dst[b, pl.ds(base, 16), :] = window.astype(jnp.bfloat16)

    def score(b):
        q = q_scr[b * per_seq:(b + 1) * per_seq, :].astype(jnp.bfloat16)
        s_scr[b % depth] = lax.dot_general(q, ko_ref[b], (((1,), (1,)), ((), ())), preferred_element_type=jnp.float32)

    def soften(b):
        scores = jnp.where(col <= lens_ref[block * rows + b], s_scr[b % depth], -jnp.inf)
        top = jnp.max(scores, axis=1, keepdims=True)
        weight = jnp.exp(scores - top)
        total = jnp.sum(weight, axis=1, keepdims=True)
        p_scr[b % depth] = (weight * (1.0 / total)).astype(jnp.bfloat16)

    def mix(b):
        o_scr[b * per_seq:(b + 1) * per_seq, :] = jnp.dot(p_scr[b % depth], vo_ref[b], preferred_element_type=jnp.float32)

    for i in range(rows + 3):
        if i < rows:
            insert(i)
        if 0 <= i - 1 < rows:
            score(i - 1)
        if 0 <= i - 2 < rows:
            soften(i - 2)
        if 0 <= i - 3 < rows:
            mix(i - 3)

    for s in range(num_steps):
        for h in range(heads):
            o_ref[h // pack, s, :, (h % pack) * head:(h % pack + 1) * head] = o_scr[pl.ds(s * heads + h, rows, stride=per_seq), :].astype(jnp.bfloat16)


def attention(lens, qkv, cos, sin, k_loc, v_loc, group):
    num_steps, batch, width = qkv.shape
    cache_len, head = k_loc.shape[1], k_loc.shape[2]
    attn_width = width - 2 * head
    heads = attn_width // head
    rows = 8
    row_spec = lambda last: pl.BlockSpec((num_steps, rows, last), lambda i, *_: (0, i, 0))
    cache_spec = pl.BlockSpec((rows, cache_len, head), lambda i, *_: (i, 0, 0))
    return pl.pallas_call(
        attention_kernel,
        grid_spec=pltpu.PrefetchScalarGridSpec(
            num_scalar_prefetch=1,
            grid=(batch // rows,),
            in_specs=[row_spec(width), row_spec(head), row_spec(head), cache_spec, cache_spec],
            out_specs=[pl.BlockSpec((group, num_steps, rows, attn_width // group), lambda i, *_: (0, 0, i, 0)), cache_spec, cache_spec],
            scratch_shapes=[
                pltpu.VMEM((rows * num_steps * heads, head), jnp.float32),
                pltpu.VMEM((rows * num_steps * heads, head), jnp.float32),
                pltpu.VMEM((2, num_steps, rows, head), jnp.float32),
                pltpu.VMEM((4, num_steps * heads, cache_len), jnp.float32),
                pltpu.VMEM((4, num_steps * heads, cache_len), jnp.bfloat16),
            ],
        ),
        out_shape=[
            jax.ShapeDtypeStruct((group, num_steps, batch, attn_width // group), jnp.bfloat16),
            jax.ShapeDtypeStruct(k_loc.shape, k_loc.dtype),
            jax.ShapeDtypeStruct(v_loc.shape, v_loc.dtype),
        ],
        compiler_params=pltpu.CompilerParams(vmem_limit_bytes=48 * 1024 * 1024),
        name="attention",
    )(lens, qkv, cos, sin, k_loc, v_loc)


HALF = 128
UNIT = 2 * HALF
OWN, XN, YN, DIAG = (0, 0), (1, 0), (0, 1), (1, 1)
REDUCE_ORDER = (DIAG, XN, YN, OWN)
UNIT_HALVES = (((OWN, 0), (OWN, 1)), ((XN, 1), (YN, 0)), ((XN, 0), (YN, 1)), ((DIAG, 0), (DIAG, 1)))
MESH = pl.DeviceIdType.MESH


class Place:
    def __init__(self):
        me = lax.axis_index('tp')
        self.me = me
        self.core, self.x, self.y = me % 2, (me // 2) % 2, me // 4

    def at(self, chip, core):
        x = self.x if chip[0] == 0 else 1 - self.x
        y = self.y if chip[1] == 0 else 1 - self.y
        c = self.core if core == 0 else 1 - self.core
        return y * 4 + x * 2 + c


def everyone():
    return [(chip, core) for chip in (DIAG, XN, YN, OWN) for core in (1, 0) if (chip, core) != (OWN, 0)]


def greet(place):
    barrier = pltpu.get_barrier_semaphore()
    for chip, core in everyone():
        pl.semaphore_signal(barrier, inc=1, device_id=(place.at(chip, core),), device_id_type=MESH)
    pl.semaphore_wait(barrier, 7)


def push(src, dst, send, recv, target):
    copy = pltpu.make_async_remote_copy(src_ref=src, dst_ref=dst, send_sem=send, recv_sem=recv, device_id=(target,), device_id_type=MESH)
    copy.start()
    return copy


def reduce_rows(place, outgoing, own_block, rc, r1a, r1b, r2, csend, crecv, psend, precv, between=None):
    dim = rc.shape[2]
    partner = place.at(OWN, 1)
    to_x, to_y = place.at(XN, 0), place.at(YN, 0)
    first, second = pl.ds(0, HALF), pl.ds(HALF, HALF)
    exchange = []
    for i, chip in enumerate(REDUCE_ORDER):
        src = outgoing(i, place.at(chip, 1))
        exchange.append(push(src, rc.at[i], csend.at[i], crecv.at[i], partner))
    sends = []
    for i, chip in enumerate(REDUCE_ORDER):
        own_block(i, place.at(chip, 0), exchange[i])
        if chip == DIAG:
            sends.append(push(rc.at[i, first], r1a.at[0], psend.at[0], precv.at[0], to_x))
            sends.append(push(rc.at[i, second], r1b.at[0], psend.at[1], precv.at[1], to_y))
        elif chip == XN:
            sends.append(push(rc.at[i, first], r1a.at[1], psend.at[2], precv.at[2], to_x))
        elif chip == YN:
            sends.append(push(rc.at[i, second], r1b.at[1], psend.at[3], precv.at[3], to_y))
    for copy in exchange:
        copy.wait_send()
    for j, (slot, rows, landed, target) in enumerate(((2, 0, r1a, to_y), (1, HALF, r1b, to_x))):
        sends[j].wait_recv()

        @pl.loop(0, HALF // 16)
        def _(r):
            here = pl.ds(pl.multiple_of(rows + r * 16, 16), 16)
            there = pl.ds(pl.multiple_of(r * 16, 16), 16)
            total = rc[slot, here, :].astype(jnp.float32) + landed[0, there, :].astype(jnp.float32)
            rc[slot, here, :] = total.astype(jnp.bfloat16)

        sends.append(push(rc.at[slot, pl.ds(rows, HALF)], r2.at[j], psend.at[4 + j], precv.at[4 + j], target))
    for copy in sends[2:]:
        copy.wait_recv()
    for copy in sends:
        copy.wait_send()


def own_rows(rc, r1a, r1b, r2, half, r, rows):
    here = pl.ds(pl.multiple_of(half * HALF + r * rows, rows), rows)
    there = pl.ds(pl.multiple_of(r * rows, rows), rows)
    landed = r1b if half else r1a
    return rc[3, here, :].astype(jnp.float32) + landed[1, there, :].astype(jnp.float32) + r2[half, there, :].astype(jnp.float32)


def norm_rows(values, gain):
    centered = values - jnp.mean(values, axis=-1, keepdims=True)
    variance = jnp.mean(centered * centered, axis=-1, keepdims=True)
    return (centered * lax.rsqrt(variance + NORM_EPS) * gain).astype(jnp.bfloat16)


def gather_units(place, z, asend, arecv, work):
    partner = place.at(OWN, 1)
    to_x, to_y = place.at(XN, 0), place.at(YN, 0)
    part = lambda unit, pos: z.at[unit, pl.ds(pos * HALF, HALF)]
    sends = []

    def go(src, dst, slot, target):
        k = len(sends)
        sends.append(push(src, dst, asend.at[k], arecv.at[slot], target))
        return sends[-1]

    xb = go(part(0, 1), part(2, 0), 0, to_x)
    ya = go(part(0, 0), part(2, 1), 1, to_y)
    near = go(z.at[0], z.at[1], 2, partner)
    xa = go(part(0, 0), part(4, 0), 3, to_x)
    yb = go(part(0, 1), part(4, 1), 4, to_y)
    near.wait_recv()
    work(0)
    xb.wait_recv()
    db = go(part(2, 0), part(6, 1), 5, to_y)
    ya.wait_recv()
    da = go(part(2, 1), part(6, 0), 6, to_x)
    near2 = go(z.at[2], z.at[3], 7, partner)
    near2.wait_recv()
    work(1)
    xa.wait_recv()
    yb.wait_recv()
    near4 = go(z.at[4], z.at[5], 8, partner)
    near4.wait_recv()
    work(2)
    da.wait_recv()
    db.wait_recv()
    near6 = go(z.at[6], z.at[7], 9, partner)
    near6.wait_recv()
    work(3)
    for copy in sends:
        copy.wait_send()


def prologue_kernel(widths, part_ref, code_ref, gain_ref, w_hbm, x_ref, m_ref, qkv_ref, z, rc, r1a, r1b, r2, w_buf, qkv_out, w_sem, csend, crecv, psend, precv, asend, arecv, qsend, qrecv):
    qkv_dev, ff_dev = widths
    dim = part_ref.shape[2]
    place = Place()
    greet(place)
    load = pltpu.make_async_copy(w_hbm, w_buf, w_sem)
    load.start()

    def own_block(i, block, copy):
        copy.wait_recv()

        @pl.loop(0, UNIT // 32)
        def _(r):
            here = pl.ds(pl.multiple_of(r * 32, 32), 32)
            code = code_ref[pl.ds(pl.multiple_of(block * UNIT + r * 32, 32), 32), :]
            for c in range(dim // 128):
                lanes = slice(c * 128, (c + 1) * 128)
                theirs = jnp.where(code == 2, rc[i, here, lanes].astype(jnp.float32), 0.0)
                rc[i, here, lanes] = jnp.where(code == 1, part_ref[block, here, lanes].astype(jnp.float32), theirs).astype(jnp.bfloat16)

    reduce_rows(place, lambda i, block: part_ref.at[block], own_block, rc, r1a, r1b, r2, csend, crecv, psend, precv)
    gain = gain_ref[...].astype(jnp.float32)
    rows = 16
    for half in range(2):
        @pl.loop(0, HALF // rows // 4)
        def _(q):
            for g in range(4):
                r = q * 4 + g
                here = pl.ds(pl.multiple_of(half * HALF + r * rows, rows), rows)
                x = own_rows(rc, r1a, r1b, r2, half, r, rows).astype(jnp.bfloat16)
                x_ref[here, :] = x
                z[0, here, :] = norm_rows(x.astype(jnp.float32), gain)

    out_sends = []

    def times(rows, first, count):
        return lax.dot_general(rows, w_buf[pl.ds(first, count), :], (((1,), (1,)), ((), ())), preferred_element_type=jnp.float32)

    def work(pair):
        if pair == 0:
            load.wait()
        rows = z[2 * pair:2 * pair + 2].reshape(2 * UNIT, dim)
        qkv_out[2 * pair:2 * pair + 2] = times(rows, 0, qkv_dev).astype(jnp.bfloat16).reshape(2, UNIT, qkv_dev)
        for core in range(2):
            for pos, (chip, half) in enumerate(UNIT_HALVES[pair]):
                unit = 2 * pair + core
                block = place.at(chip, core)
                src = qkv_out.at[unit, pl.ds(pos * HALF, HALF)]
                if unit == 0:
                    qkv_ref[place.me, pl.ds(half * HALF, HALF), :] = qkv_out[unit, pl.ds(pos * HALF, HALF), :]
                else:
                    k = len(out_sends)
                    out_sends.append(push(src, qkv_ref.at[place.me, pl.ds(half * HALF, HALF)], qsend.at[k], qrecv.at[k], block))
        tile = 256

        @pl.loop(0, ff_dev // tile)
        def _(n):
            at = pl.multiple_of(n * tile, tile)
            gate = times(rows, pl.multiple_of(qkv_dev + at, 16), tile).astype(jnp.bfloat16).astype(jnp.float32)
            up = times(rows, pl.multiple_of(qkv_dev + ff_dev + at, 16), tile).astype(jnp.bfloat16).astype(jnp.float32)
            act = (gate / (1.0 + jnp.exp(-gate)) * up).astype(jnp.bfloat16)
            for core in range(2):
                for pos, (chip, half) in enumerate(UNIT_HALVES[pair]):
                    first = place.at(chip, core) * UNIT + half * HALF
                    k = core * UNIT + pos * HALF
                    m_ref[pl.ds(pl.multiple_of(first, HALF), HALF), pl.ds(at, tile)] = act[k:k + HALF]

    gather_units(place, z, asend, arecv, work)
    for copy in out_sends:
        copy.wait()


def prologue(part, code, gain, w_in, qkv_dev, ff_dev):
    group, rows, dim = part.shape
    vmem = pl.BlockSpec(memory_space=pltpu.VMEM)
    dma = pltpu.SemaphoreType.DMA
    return pl.pallas_call(
        functools.partial(prologue_kernel, (qkv_dev, ff_dev)),
        in_specs=[vmem] * 3 + [pl.BlockSpec(memory_space=pl.ANY)],
        out_specs=[vmem] * 3,
        out_shape=[
            jax.ShapeDtypeStruct((rows, dim), jnp.bfloat16),
            jax.ShapeDtypeStruct((group * rows, ff_dev), jnp.bfloat16),
            jax.ShapeDtypeStruct((group, rows, qkv_dev), jnp.bfloat16),
        ],
        scratch_shapes=[
            pltpu.VMEM((group, rows, dim), jnp.bfloat16),
            pltpu.VMEM((4, rows, dim), jnp.bfloat16),
            pltpu.VMEM((2, HALF, dim), jnp.bfloat16),
            pltpu.VMEM((2, HALF, dim), jnp.bfloat16),
            pltpu.VMEM((2, HALF, dim), jnp.bfloat16),
            pltpu.VMEM(w_in.shape, jnp.bfloat16),
            pltpu.VMEM((group, rows, qkv_dev), jnp.bfloat16),
            dma,
            dma((4,)), dma((4,)), dma((6,)), dma((6,)), dma((10,)), dma((10,)), dma((14,)), dma((14,)),
        ],
        compiler_params=pltpu.CompilerParams(collective_id=0, has_side_effects=True, vmem_limit_bytes=60 * 1024 * 1024),
        name="prologue",
    )(part, code, gain, w_in)


def epilogue_kernel(scale, tile, attn_ref, m_ref, w_ref, x_ref, gain_ref, ids_ref, e_hbm, out_ref, e_buf, z, rc, r1a, r1b, r2, a_in, raw, stats, every, e_sem, csend, crecv, psend, precv, asend, arecv, qsend, qrecv, ssend, srecv):
    vocab = e_hbm.shape[0]
    tiles = vocab // tile
    cols = 2 * UNIT
    dim = z.shape[2]
    attn_dev = a_in.shape[2]
    loads = [pltpu.make_async_copy(e_hbm.at[pl.ds(t * tile, tile)], e_buf.at[pl.ds(t * tile, tile)], e_sem.at[t]) for t in range(tiles)]
    place = Place()
    greet(place)
    heads_in = {}
    for k, (chip, core) in enumerate(everyone()):
        target = place.at(chip, core)
        heads_in[(chip, core)] = push(attn_ref.at[target], a_in.at[place.me], qsend.at[k], qrecv.at[k], target)
    for c in loads:
        c.start()
    a_in[place.me] = attn_ref[place.me]

    def block_dot(block, n):
        lanes = pl.ds(pl.multiple_of(n * 512, 512), 512)
        mine = jnp.dot(a_in[block], w_ref[pl.ds(0, attn_dev), lanes], preferred_element_type=jnp.float32)
        rows = pl.ds(pl.multiple_of(block * UNIT, UNIT), UNIT)
        return mine + jnp.dot(m_ref[rows, :], w_ref[pl.ds(attn_dev, w_ref.shape[0] - attn_dev), lanes], preferred_element_type=jnp.float32)

    def outgoing(i, block):
        heads_in[(REDUCE_ORDER[i], 1)].wait_recv()

        @pl.loop(0, dim // 512)
        def _(n):
            lanes = pl.ds(pl.multiple_of(n * 512, 512), 512)
            z[2 * i, :, lanes] = block_dot(block, n).astype(jnp.bfloat16)

        return z.at[2 * i]

    def own_block(i, block, copy):
        if REDUCE_ORDER[i] != OWN:
            heads_in[(REDUCE_ORDER[i], 0)].wait_recv()
        copy.wait_recv()

        @pl.loop(0, dim // 512)
        def _(n):
            lanes = pl.ds(pl.multiple_of(n * 512, 512), 512)
            rc[i, :, lanes] = (block_dot(block, n) + rc[i, :, lanes].astype(jnp.float32)).astype(jnp.bfloat16)

    reduce_rows(place, outgoing, own_block, rc, r1a, r1b, r2, csend, crecv, psend, precv)
    gain = gain_ref[...].astype(jnp.float32)
    rows = 16
    for half in range(2):
        @pl.loop(0, HALF // rows // 4)
        def _(q):
            for g in range(4):
                r = q * 4 + g
                here = pl.ds(pl.multiple_of(half * HALF + r * rows, rows), rows)
                o = own_rows(rc, r1a, r1b, r2, half, r, rows).astype(jnp.bfloat16).astype(jnp.float32)
                z[0, here, :] = norm_rows(x_ref[here, :].astype(jnp.float32) + o, gain)

    def work(pair):
        if pair == 0:
            for c in loads:
                c.wait()
        halves = [place.at(chip, core) * 2 + half for core in range(2) for chip, half in UNIT_HALVES[pair]]
        row = lax.broadcasted_iota(jnp.int32, (8, cols), 0)
        ids = jnp.concatenate([ids_ref[h] for h in halves], axis=1) - row
        rate = scale * LOG2E

        def product(t, slot):
            e = e_buf[pl.ds(pl.multiple_of(t * tile, 16), tile), :]
            rows = z[2 * pair:2 * pair + 2].reshape(cols, dim)
            raw[slot] = lax.dot_general(e, rows, (((1,), (1,)), ((), ())), preferred_element_type=jnp.float32)

        def absorb(t, slot, carry):
            top, total, target = carry
            local = ids - t * tile
            count = tile // 8
            tops = [top, None]
            for r in range(count):
                v = raw[slot, r * 8:r * 8 + 8, :]
                k = r % 2
                tops[k] = v if tops[k] is None else jnp.maximum(tops[k], v)
            new_top = jnp.maximum(tops[0], tops[1])
            sums = [total * jnp.exp2((top - new_top) * rate), None]
            for r in range(count):
                v = raw[slot, r * 8:r * 8 + 8, :]
                k = r % 2
                p = jnp.exp2((v - new_top) * rate)
                sums[k] = p if sums[k] is None else sums[k] + p
                target = target + jnp.where(local == r * 8, v, 0.0)
            return new_top, sums[0] + sums[1], target

        zero = jnp.zeros((8, cols), jnp.float32)
        product(0, 0)

        def body(i, carry):
            product(2 * i + 1, 1)
            carry = absorb(2 * i, 0, carry)
            product(2 * i + 2, 0)
            return absorb(2 * i + 1, 1, carry)

        carry = lax.fori_loop(0, (tiles - 1) // 2, body, (jnp.full((8, cols), -jnp.inf, jnp.float32), zero, zero))
        if tiles % 2 == 0:
            product(tiles - 1, 1)
            carry = absorb(tiles - 2, 0, carry)
        top, total, target = absorb(tiles - 1, (tiles - 1) % 2, carry)
        best = jnp.max(top, axis=0, keepdims=True)
        total = jnp.sum(total * jnp.exp2((top - best) * rate), axis=0, keepdims=True)
        target = jnp.sum(target, axis=0, keepdims=True)
        for pos, h in enumerate(halves):
            lanes = slice(pos * HALF, (pos + 1) * HALF)
            stats[0, pl.ds(h, 1), :] = best[:, lanes] * scale
            stats[1, pl.ds(h, 1), :] = total[:, lanes]
            stats[2, pl.ds(h, 1), :] = target[:, lanes] * scale

    gather_units(place, z, asend, arecv, work)
    finals = []
    for k, (chip, core) in enumerate(everyone()):
        finals.append(push(stats, every.at[place.me], ssend.at[k], srecv.at[k], place.at(chip, core)))
    every[place.me] = stats[...]
    for copy in finals:
        copy.wait()
    for copy in heads_in.values():
        copy.wait_send()
    tops = every[:, 0]
    best = jnp.max(tops, axis=0)
    total = jnp.sum(every[:, 1] * jnp.exp(tops - best[None]), axis=0)
    out_ref[...] = jnp.sum(every[:, 2], axis=0) - best - jnp.log(total)


def epilogue(attn, m, w_out, x_own, gain, ids, embed_loc):
    group, rows, attn_dev = attn.shape
    vocab, dim = embed_loc.shape
    tile = 560
    vmem = pl.BlockSpec(memory_space=pltpu.VMEM)
    dma = pltpu.SemaphoreType.DMA
    halves = group * rows // HALF
    return pl.pallas_call(
        functools.partial(epilogue_kernel, dim ** -0.5, tile),
        in_specs=[vmem] * 6 + [pl.BlockSpec(memory_space=pl.ANY)],
        out_specs=vmem,
        out_shape=jax.ShapeDtypeStruct((halves, HALF), jnp.float32),
        scratch_shapes=[
            pltpu.VMEM((vocab, dim), jnp.bfloat16),
            pltpu.VMEM((group, rows, dim), jnp.bfloat16),
            pltpu.VMEM((4, rows, dim), jnp.bfloat16),
            pltpu.VMEM((2, HALF, dim), jnp.bfloat16),
            pltpu.VMEM((2, HALF, dim), jnp.bfloat16),
            pltpu.VMEM((2, HALF, dim), jnp.bfloat16),
            pltpu.VMEM((group, rows, attn_dev), jnp.bfloat16),
            pltpu.VMEM((2, tile, 2 * UNIT), jnp.float32),
            pltpu.VMEM((3, halves, HALF), jnp.float32),
            pltpu.VMEM((group, 3, halves, HALF), jnp.float32),
            dma((vocab // tile,)),
            dma((4,)), dma((4,)), dma((6,)), dma((6,)), dma((10,)), dma((10,)), dma((7,)), dma((7,)), dma((7,)), dma((7,)),
        ],
        compiler_params=pltpu.CompilerParams(collective_id=1, has_side_effects=True, vmem_limit_bytes=67043328),
        name="epilogue",
    )(attn, m, w_out, x_own, gain, ids, embed_loc)


def solution(mesh):
    group_size = mesh.shape['tp']

    def device_fn(tok_ids, next_ids, seq_lens, embed_loc, ln_gain, w_in_loc, w_out_loc, final_gain, k_loc, v_loc):
        num_steps, batch_size = tok_ids.shape
        batch_dev = batch_size // group_size
        rows_dev = num_steps * batch_dev
        vocab_dev, model_dim = embed_loc.shape
        head_dim = k_loc.shape[2]
        in_dev = w_in_loc.shape[1]
        out_dev = w_out_loc.shape[0]
        kv_dev = 2 * head_dim // group_size
        attn_dev = 2 * out_dev - in_dev + kv_dev
        ff_dev = out_dev - attn_dev
        qkv_dev = attn_dev + kv_dev
        dev_index = lax.axis_index('tp')
        vocab_start = dev_index * vocab_dev
        own_lens = lax.dynamic_slice_in_dim(seq_lens, dev_index * batch_dev, batch_dev)

        def by_device(ids):
            return ids.reshape(num_steps, group_size, batch_dev).transpose(1, 0, 2)

        local_ids = by_device(tok_ids).reshape(-1) - vocab_start
        x_part = embed_loc.at[jnp.clip(local_ids, 0, vocab_dev - 1)].get(mode="promise_in_bounds")
        mate_ids = local_ids - (1 - 2 * (dev_index % 2)) * vocab_dev
        tok_mine = (local_ids >= 0) & (local_ids < vocab_dev)
        tok_mate = (mate_ids >= 0) & (mate_ids < vocab_dev)
        code = jnp.where(tok_mine, 1, jnp.where(tok_mate, 2, 0)).astype(jnp.int32)
        code = jnp.broadcast_to(code[:, None], (code.shape[0], 128))
        x_own, mlp_act, qkv_own = prologue(x_part.reshape(group_size, rows_dev, model_dim), code, ln_gain[None], w_in_loc.T, qkv_dev, ff_dev)
        qkv_own = qkv_own.transpose(1, 0, 2).reshape(num_steps, batch_dev, -1)

        half = head_dim // 2
        inv_freq = ROPE_BASE ** (-jnp.arange(half, dtype=jnp.float32) / half)
        positions = own_lens[None, :] + jnp.arange(num_steps, dtype=jnp.int32)[:, None]
        angles = positions.astype(jnp.float32)[..., None] * inv_freq
        cos, sin = jnp.cos(angles), jnp.sin(angles)
        cos = jnp.concatenate([cos, cos], axis=-1)
        sin = jnp.concatenate([-sin, sin], axis=-1)
        attn_out, k_out, v_out = attention(own_lens, qkv_own, cos, sin, k_loc, v_loc, group_size)
        local_next = by_device(next_ids).reshape(2 * group_size, 1, batch_dev) - vocab_start
        ids8 = jnp.broadcast_to(local_next, (2 * group_size, 8, batch_dev))
        log_probs = epilogue(attn_out.reshape(group_size, rows_dev, attn_dev), mlp_act, w_out_loc, x_own, final_gain[None], ids8, embed_loc)
        log_probs = log_probs.reshape(group_size, num_steps, batch_dev).transpose(1, 0, 2).reshape(num_steps, batch_size)
        return log_probs, k_out, v_out

    cache_spec = P('tp', None, None)
    return jax.shard_map(device_fn, mesh=mesh, in_specs=(P(), P(), P(), P('tp', None), P(), P(None, 'tp'), P('tp', None), P(), cache_spec, cache_spec), out_specs=(P(), cache_spec, cache_spec), check_vma=False)
```

```python
import functools

import jax
import jax.numpy as jnp
from jax import lax
from jax.experimental import pallas as pl
from jax.experimental.pallas import tpu as pltpu
from jax.sharding import PartitionSpec as P

ROPE_BASE = 10000.0
NORM_EPS = 1e-6
LOG2E = 1.4426950408889634


def layer_norm(values, gain_vec):
    centered = values.astype(jnp.float32)
    centered = centered - jnp.mean(centered, axis=-1, keepdims=True)
    variance = jnp.mean(jnp.square(centered), axis=-1, keepdims=True)
    scaled = centered * lax.rsqrt(variance + NORM_EPS) * gain_vec.astype(jnp.float32)
    return scaled.astype(jnp.bfloat16)


def attention_kernel(ahead, lens_ref, qkv_ref, cos_ref, sin_ref, k_hbm, v_hbm, o_ref, ko_hbm, vo_hbm, k_buf, v_buf, q_scr, o_scr, n_scr, s_scr, p_scr, read_sem, write_sem):
    num_steps, blocks, rows, _ = qkv_ref.shape
    slots, _, cache_len, head = k_buf.shape
    pack = o_ref.shape[4] // head
    heads = o_ref.shape[0] * pack
    per_seq = num_steps * heads
    win_row = lax.broadcasted_iota(jnp.int32, (16, head), 0)
    col = lax.broadcasted_iota(jnp.int32, (per_seq, cache_len), 1) - lax.broadcasted_iota(jnp.int32, (per_seq, cache_len), 0) // heads
    depth = s_scr.shape[0]

    def moves(block, slot, out):
        here = pl.ds(pl.multiple_of(block * rows, rows), rows)
        pairs = []
        for which, (hbm, hbm_out, buf) in enumerate(((k_hbm, ko_hbm, k_buf), (v_hbm, vo_hbm, v_buf))):
            if out:
                pairs.append(pltpu.make_async_copy(buf.at[slot], hbm_out.at[here], write_sem.at[which, slot]))
            else:
                pairs.append(pltpu.make_async_copy(hbm.at[here], buf.at[slot], read_sem.at[which, slot]))
        return pairs

    for block in range(ahead):
        for copy in moves(block, block, False):
            copy.start()

    @pl.loop(0, blocks)
    def _(block):
        slot = lax.rem(block, slots)

        @pl.when(block + ahead < blocks)
        def _():
            later = lax.rem(block + ahead, slots)

            @pl.when(block + ahead >= slots)
            def _():
                for copy in moves(block + ahead - slots, later, True):
                    copy.wait()

            for copy in moves(block + ahead, later, False):
                copy.start()

        for s in range(num_steps):
            cos, sin = cos_ref[s, block], sin_ref[s, block]

            def rotate(lo):
                x = qkv_ref[s, block, :, lo:lo + head].astype(jnp.float32)
                return x * cos + pltpu.roll(x, head // 2, 1) * sin

            for h in range(heads):
                q_scr[pl.ds(s * heads + h, rows, stride=per_seq), :] = rotate(h * head) * head ** -0.5
            n_scr[0, s] = rotate(heads * head).astype(jnp.bfloat16).astype(jnp.float32)
            n_scr[1, s] = qkv_ref[s, block, :, (heads + 1) * head:].astype(jnp.float32)

        for copy in moves(block, slot, False):
            copy.wait()

        def insert(b):
            length = lens_ref[block * rows + b]
            for dst, which in ((k_buf, 0), (v_buf, 1)):
                for s in range(num_steps):
                    pos = length + s
                    base = pl.multiple_of((pos // 16) * 16, 16)
                    window = dst[slot, b, pl.ds(base, 16), :].astype(jnp.float32)
                    fresh = n_scr[which, s, b:b + 1, :]
                    window = jnp.where(win_row == pos - base, fresh, window)
                    dst[slot, b, pl.ds(base, 16), :] = window.astype(jnp.bfloat16)

        def score(b):
            q = q_scr[b * per_seq:(b + 1) * per_seq, :].astype(jnp.bfloat16)
            s_scr[b % depth] = lax.dot_general(q, k_buf[slot, b], (((1,), (1,)), ((), ())), preferred_element_type=jnp.float32)

        def soften(b):
            scores = jnp.where(col <= lens_ref[block * rows + b], s_scr[b % depth], -jnp.inf)
            top = jnp.max(scores, axis=1, keepdims=True)
            weight = jnp.exp(scores - top)
            total = jnp.sum(weight, axis=1, keepdims=True)
            p_scr[b % depth] = (weight * (1.0 / total)).astype(jnp.bfloat16)

        def mix(b):
            o_scr[b * per_seq:(b + 1) * per_seq, :] = jnp.dot(p_scr[b % depth], v_buf[slot, b], preferred_element_type=jnp.float32)

        for i in range(rows):
            insert(i)
        for i in range(rows + 2):
            if i < rows:
                score(i)
            if 0 <= i - 1 < rows:
                soften(i - 1)
            if 0 <= i - 2 < rows:
                mix(i - 2)

        for copy in moves(block, slot, True):
            copy.start()
        for s in range(num_steps):
            for h in range(heads):
                o_ref[h // pack, s, block, :, (h % pack) * head:(h % pack + 1) * head] = o_scr[pl.ds(s * heads + h, rows, stride=per_seq), :].astype(jnp.bfloat16)

    for block in range(blocks - slots, blocks):
        for copy in moves(block, block % slots, True):
            copy.wait()


def attention(lens, qkv, cos, sin, k_loc, v_loc, group):
    num_steps, batch, width = qkv.shape
    cache_len, head = k_loc.shape[1], k_loc.shape[2]
    attn_width = width - 2 * head
    heads = attn_width // head
    rows, slots, ahead = 8, 5, 3
    blocks = batch // rows
    vmem, anywhere = pl.BlockSpec(memory_space=pltpu.VMEM), pl.BlockSpec(memory_space=pl.ANY)
    in_blocks = lambda a: a.reshape(num_steps, blocks, rows, a.shape[-1])
    out, k_out, v_out = pl.pallas_call(
        functools.partial(attention_kernel, ahead),
        in_specs=[pl.BlockSpec(memory_space=pltpu.SMEM), vmem, vmem, vmem, anywhere, anywhere],
        out_specs=[vmem, anywhere, anywhere],
        out_shape=[
            jax.ShapeDtypeStruct((group, num_steps, blocks, rows, attn_width // group), jnp.bfloat16),
            jax.ShapeDtypeStruct(k_loc.shape, k_loc.dtype),
            jax.ShapeDtypeStruct(v_loc.shape, v_loc.dtype),
        ],
        scratch_shapes=[
            pltpu.VMEM((slots, rows, cache_len, head), jnp.bfloat16),
            pltpu.VMEM((slots, rows, cache_len, head), jnp.bfloat16),
            pltpu.VMEM((rows * num_steps * heads, head), jnp.float32),
            pltpu.VMEM((rows * num_steps * heads, head), jnp.float32),
            pltpu.VMEM((2, num_steps, rows, head), jnp.float32),
            pltpu.VMEM((4, num_steps * heads, cache_len), jnp.float32),
            pltpu.VMEM((4, num_steps * heads, cache_len), jnp.bfloat16),
            pltpu.SemaphoreType.DMA((2, slots)),
            pltpu.SemaphoreType.DMA((2, slots)),
        ],
        compiler_params=pltpu.CompilerParams(vmem_limit_bytes=56 * 1024 * 1024),
        name="attention",
    )(lens, in_blocks(qkv), in_blocks(cos), in_blocks(sin), k_loc, v_loc)
    return out.reshape(group, num_steps, batch, attn_width // group), k_out, v_out


HALF = 128
UNIT = 2 * HALF
OWN, XN, YN, DIAG = (0, 0), (1, 0), (0, 1), (1, 1)
REDUCE_ORDER = (DIAG, XN, YN, OWN)
UNIT_HALVES = (((OWN, 0), (OWN, 1)), ((XN, 1), (YN, 0)), ((XN, 0), (YN, 1)), ((DIAG, 0), (DIAG, 1)))
MESH = pl.DeviceIdType.MESH


class Place:
    def __init__(self):
        me = lax.axis_index('tp')
        self.me = me
        self.core, self.x, self.y = me % 2, (me // 2) % 2, me // 4

    def at(self, chip, core):
        x = self.x if chip[0] == 0 else 1 - self.x
        y = self.y if chip[1] == 0 else 1 - self.y
        c = self.core if core == 0 else 1 - self.core
        return y * 4 + x * 2 + c


def everyone():
    return [(chip, core) for chip in (DIAG, XN, YN, OWN) for core in (1, 0) if (chip, core) != (OWN, 0)]


def greet(place):
    barrier = pltpu.get_barrier_semaphore()
    for chip, core in everyone():
        pl.semaphore_signal(barrier, inc=1, device_id=(place.at(chip, core),), device_id_type=MESH)
    pl.semaphore_wait(barrier, 7)


def push(src, dst, send, recv, target):
    copy = pltpu.make_async_remote_copy(src_ref=src, dst_ref=dst, send_sem=send, recv_sem=recv, device_id=(target,), device_id_type=MESH)
    copy.start()
    return copy


def reduce_rows(place, outgoing, own_block, rc, r1a, r1b, r2, csend, crecv, psend, precv, between=None):
    dim = rc.shape[2]
    partner = place.at(OWN, 1)
    to_x, to_y = place.at(XN, 0), place.at(YN, 0)
    first, second = pl.ds(0, HALF), pl.ds(HALF, HALF)
    exchange = []
    for i, chip in enumerate(REDUCE_ORDER):
        src = outgoing(i, place.at(chip, 1))
        exchange.append(push(src, rc.at[i], csend.at[i], crecv.at[i], partner))
    sends = []
    for i, chip in enumerate(REDUCE_ORDER):
        own_block(i, place.at(chip, 0), exchange[i])
        if chip == DIAG:
            sends.append(push(rc.at[i, first], r1a.at[0], psend.at[0], precv.at[0], to_x))
            sends.append(push(rc.at[i, second], r1b.at[0], psend.at[1], precv.at[1], to_y))
        elif chip == XN:
            sends.append(push(rc.at[i, first], r1a.at[1], psend.at[2], precv.at[2], to_x))
        elif chip == YN:
            sends.append(push(rc.at[i, second], r1b.at[1], psend.at[3], precv.at[3], to_y))
    for copy in exchange:
        copy.wait_send()
    for j, (slot, rows, landed, target) in enumerate(((2, 0, r1a, to_y), (1, HALF, r1b, to_x))):
        sends[j].wait_recv()

        @pl.loop(0, HALF // 16)
        def _(r):
            here = pl.ds(pl.multiple_of(rows + r * 16, 16), 16)
            there = pl.ds(pl.multiple_of(r * 16, 16), 16)
            total = rc[slot, here, :].astype(jnp.float32) + landed[0, there, :].astype(jnp.float32)
            rc[slot, here, :] = total.astype(jnp.bfloat16)

        sends.append(push(rc.at[slot, pl.ds(rows, HALF)], r2.at[j], psend.at[4 + j], precv.at[4 + j], target))
    for copy in sends[2:]:
        copy.wait_recv()
    for copy in sends:
        copy.wait_send()


def own_rows(rc, r1a, r1b, r2, half, r, rows):
    here = pl.ds(pl.multiple_of(half * HALF + r * rows, rows), rows)
    there = pl.ds(pl.multiple_of(r * rows, rows), rows)
    landed = r1b if half else r1a
    return rc[3, here, :].astype(jnp.float32) + landed[1, there, :].astype(jnp.float32) + r2[half, there, :].astype(jnp.float32)


def norm_rows(values, gain):
    centered = values - jnp.mean(values, axis=-1, keepdims=True)
    variance = jnp.mean(centered * centered, axis=-1, keepdims=True)
    return (centered * lax.rsqrt(variance + NORM_EPS) * gain).astype(jnp.bfloat16)


def gather_units(place, z, asend, arecv, work):
    partner = place.at(OWN, 1)
    to_x, to_y = place.at(XN, 0), place.at(YN, 0)
    part = lambda unit, pos: z.at[unit, pl.ds(pos * HALF, HALF)]
    sends = []

    def go(src, dst, slot, target):
        k = len(sends)
        sends.append(push(src, dst, asend.at[k], arecv.at[slot], target))
        return sends[-1]

    xb = go(part(0, 1), part(2, 0), 0, to_x)
    ya = go(part(0, 0), part(2, 1), 1, to_y)
    near = go(z.at[0], z.at[1], 2, partner)
    xa = go(part(0, 0), part(4, 0), 3, to_x)
    yb = go(part(0, 1), part(4, 1), 4, to_y)
    near.wait_recv()
    work(0)
    xb.wait_recv()
    db = go(part(2, 0), part(6, 1), 5, to_y)
    ya.wait_recv()
    da = go(part(2, 1), part(6, 0), 6, to_x)
    near2 = go(z.at[2], z.at[3], 7, partner)
    near2.wait_recv()
    work(1)
    xa.wait_recv()
    yb.wait_recv()
    near4 = go(z.at[4], z.at[5], 8, partner)
    near4.wait_recv()
    work(2)
    da.wait_recv()
    db.wait_recv()
    near6 = go(z.at[6], z.at[7], 9, partner)
    near6.wait_recv()
    work(3)
    for copy in sends:
        copy.wait_send()


def prologue_kernel(widths, part_ref, code_ref, gain_ref, w_hbm, x_ref, m_ref, qkv_ref, z, rc, r1a, r1b, r2, w_buf, qkv_out, w_sem, csend, crecv, psend, precv, asend, arecv, qsend, qrecv):
    qkv_dev, ff_dev = widths
    dim = part_ref.shape[2]
    place = Place()
    greet(place)
    load = pltpu.make_async_copy(w_hbm, w_buf, w_sem)
    load.start()

    def own_block(i, block, copy):
        copy.wait_recv()

        @pl.loop(0, UNIT // 32)
        def _(r):
            here = pl.ds(pl.multiple_of(r * 32, 32), 32)
            code = code_ref[pl.ds(pl.multiple_of(block * UNIT + r * 32, 32), 32), :]
            for c in range(dim // 128):
                lanes = slice(c * 128, (c + 1) * 128)
                theirs = jnp.where(code == 2, rc[i, here, lanes].astype(jnp.float32), 0.0)
                rc[i, here, lanes] = jnp.where(code == 1, part_ref[block, here, lanes].astype(jnp.float32), theirs).astype(jnp.bfloat16)

    reduce_rows(place, lambda i, block: part_ref.at[block], own_block, rc, r1a, r1b, r2, csend, crecv, psend, precv)
    gain = gain_ref[...].astype(jnp.float32)
    rows = 16
    for half in range(2):
        @pl.loop(0, HALF // rows // 4)
        def _(q):
            for g in range(4):
                r = q * 4 + g
                here = pl.ds(pl.multiple_of(half * HALF + r * rows, rows), rows)
                x = own_rows(rc, r1a, r1b, r2, half, r, rows).astype(jnp.bfloat16)
                x_ref[here, :] = x
                z[0, here, :] = norm_rows(x.astype(jnp.float32), gain)

    out_sends = []

    def times(rows, first, count):
        return lax.dot_general(rows, w_buf[pl.ds(first, count), :], (((1,), (1,)), ((), ())), preferred_element_type=jnp.float32)

    def work(pair):
        if pair == 0:
            load.wait()
        rows = z[2 * pair:2 * pair + 2].reshape(2 * UNIT, dim)
        qkv_out[2 * pair:2 * pair + 2] = times(rows, 0, qkv_dev).astype(jnp.bfloat16).reshape(2, UNIT, qkv_dev)
        for core in range(2):
            for pos, (chip, half) in enumerate(UNIT_HALVES[pair]):
                unit = 2 * pair + core
                block = place.at(chip, core)
                src = qkv_out.at[unit, pl.ds(pos * HALF, HALF)]
                if unit == 0:
                    qkv_ref[place.me, pl.ds(half * HALF, HALF), :] = qkv_out[unit, pl.ds(pos * HALF, HALF), :]
                else:
                    k = len(out_sends)
                    out_sends.append(push(src, qkv_ref.at[place.me, pl.ds(half * HALF, HALF)], qsend.at[k], qrecv.at[k], block))
        tile = 256

        @pl.loop(0, ff_dev // tile)
        def _(n):
            at = pl.multiple_of(n * tile, tile)
            gate = times(rows, pl.multiple_of(qkv_dev + at, 16), tile).astype(jnp.bfloat16).astype(jnp.float32)
            up = times(rows, pl.multiple_of(qkv_dev + ff_dev + at, 16), tile).astype(jnp.bfloat16).astype(jnp.float32)
            act = (gate / (1.0 + jnp.exp(-gate)) * up).astype(jnp.bfloat16)
            for core in range(2):
                for pos, (chip, half) in enumerate(UNIT_HALVES[pair]):
                    first = place.at(chip, core) * UNIT + half * HALF
                    k = core * UNIT + pos * HALF
                    m_ref[pl.ds(pl.multiple_of(first, HALF), HALF), pl.ds(at, tile)] = act[k:k + HALF]

    gather_units(place, z, asend, arecv, work)
    for copy in out_sends:
        copy.wait()


def prologue(part, code, gain, w_in, qkv_dev, ff_dev):
    group, rows, dim = part.shape
    vmem = pl.BlockSpec(memory_space=pltpu.VMEM)
    dma = pltpu.SemaphoreType.DMA
    return pl.pallas_call(
        functools.partial(prologue_kernel, (qkv_dev, ff_dev)),
        in_specs=[vmem] * 3 + [pl.BlockSpec(memory_space=pl.ANY)],
        out_specs=[vmem] * 3,
        out_shape=[
            jax.ShapeDtypeStruct((rows, dim), jnp.bfloat16),
            jax.ShapeDtypeStruct((group * rows, ff_dev), jnp.bfloat16),
            jax.ShapeDtypeStruct((group, rows, qkv_dev), jnp.bfloat16),
        ],
        scratch_shapes=[
            pltpu.VMEM((group, rows, dim), jnp.bfloat16),
            pltpu.VMEM((4, rows, dim), jnp.bfloat16),
            pltpu.VMEM((2, HALF, dim), jnp.bfloat16),
            pltpu.VMEM((2, HALF, dim), jnp.bfloat16),
            pltpu.VMEM((2, HALF, dim), jnp.bfloat16),
            pltpu.VMEM(w_in.shape, jnp.bfloat16),
            pltpu.VMEM((group, rows, qkv_dev), jnp.bfloat16),
            dma,
            dma((4,)), dma((4,)), dma((6,)), dma((6,)), dma((10,)), dma((10,)), dma((14,)), dma((14,)),
        ],
        compiler_params=pltpu.CompilerParams(collective_id=0, has_side_effects=True, vmem_limit_bytes=60 * 1024 * 1024),
        name="prologue",
    )(part, code, gain, w_in)


def epilogue_kernel(scale, tile, attn_ref, m_ref, w_ref, x_ref, gain_ref, ids_ref, e_hbm, out_ref, e_buf, z, rc, r1a, r1b, r2, a_in, raw, stats, every, e_sem, csend, crecv, psend, precv, asend, arecv, qsend, qrecv, ssend, srecv):
    vocab = e_hbm.shape[0]
    tiles = vocab // tile
    cols = 2 * UNIT
    dim = z.shape[2]
    attn_dev = a_in.shape[2]
    loads = [pltpu.make_async_copy(e_hbm.at[pl.ds(t * tile, tile)], e_buf.at[pl.ds(t * tile, tile)], e_sem.at[t]) for t in range(tiles)]
    place = Place()
    greet(place)
    heads_in = {}
    for k, (chip, core) in enumerate(everyone()):
        target = place.at(chip, core)
        heads_in[(chip, core)] = push(attn_ref.at[target], a_in.at[place.me], qsend.at[k], qrecv.at[k], target)
    for c in loads:
        c.start()
    a_in[place.me] = attn_ref[place.me]

    def block_dot(block, n):
        lanes = pl.ds(pl.multiple_of(n * 512, 512), 512)
        mine = jnp.dot(a_in[block], w_ref[pl.ds(0, attn_dev), lanes], preferred_element_type=jnp.float32)
        rows = pl.ds(pl.multiple_of(block * UNIT, UNIT), UNIT)
        return mine + jnp.dot(m_ref[rows, :], w_ref[pl.ds(attn_dev, w_ref.shape[0] - attn_dev), lanes], preferred_element_type=jnp.float32)

    def outgoing(i, block):
        heads_in[(REDUCE_ORDER[i], 1)].wait_recv()

        @pl.loop(0, dim // 512)
        def _(n):
            lanes = pl.ds(pl.multiple_of(n * 512, 512), 512)
            z[2 * i, :, lanes] = block_dot(block, n).astype(jnp.bfloat16)

        return z.at[2 * i]

    def own_block(i, block, copy):
        if REDUCE_ORDER[i] != OWN:
            heads_in[(REDUCE_ORDER[i], 0)].wait_recv()
        copy.wait_recv()

        @pl.loop(0, dim // 512)
        def _(n):
            lanes = pl.ds(pl.multiple_of(n * 512, 512), 512)
            rc[i, :, lanes] = (block_dot(block, n) + rc[i, :, lanes].astype(jnp.float32)).astype(jnp.bfloat16)

    reduce_rows(place, outgoing, own_block, rc, r1a, r1b, r2, csend, crecv, psend, precv)
    gain = gain_ref[...].astype(jnp.float32)
    rows = 16
    for half in range(2):
        @pl.loop(0, HALF // rows // 4)
        def _(q):
            for g in range(4):
                r = q * 4 + g
                here = pl.ds(pl.multiple_of(half * HALF + r * rows, rows), rows)
                o = own_rows(rc, r1a, r1b, r2, half, r, rows).astype(jnp.bfloat16).astype(jnp.float32)
                z[0, here, :] = norm_rows(x_ref[here, :].astype(jnp.float32) + o, gain)

    def work(pair):
        if pair == 0:
            for c in loads:
                c.wait()
        halves = [place.at(chip, core) * 2 + half for core in range(2) for chip, half in UNIT_HALVES[pair]]
        row = lax.broadcasted_iota(jnp.int32, (8, cols), 0)
        ids = jnp.concatenate([ids_ref[h] for h in halves], axis=1) - row
        rate = scale * LOG2E

        def product(t, slot):
            e = e_buf[pl.ds(pl.multiple_of(t * tile, 16), tile), :]
            rows = z[2 * pair:2 * pair + 2].reshape(cols, dim)
            raw[slot] = lax.dot_general(e, rows, (((1,), (1,)), ((), ())), preferred_element_type=jnp.float32)

        def absorb(t, slot, carry):
            top, total, target = carry
            local = ids - t * tile
            count = tile // 8
            tops = [top, None]
            for r in range(count):
                v = raw[slot, r * 8:r * 8 + 8, :]
                k = r % 2
                tops[k] = v if tops[k] is None else jnp.maximum(tops[k], v)
            new_top = jnp.maximum(tops[0], tops[1])
            sums = [total * jnp.exp2((top - new_top) * rate), None]
            for r in range(count):
                v = raw[slot, r * 8:r * 8 + 8, :]
                k = r % 2
                p = jnp.exp2((v - new_top) * rate)
                sums[k] = p if sums[k] is None else sums[k] + p
                target = target + jnp.where(local == r * 8, v, 0.0)
            return new_top, sums[0] + sums[1], target

        zero = jnp.zeros((8, cols), jnp.float32)
        product(0, 0)

        def body(i, carry):
            product(2 * i + 1, 1)
            carry = absorb(2 * i, 0, carry)
            product(2 * i + 2, 0)
            return absorb(2 * i + 1, 1, carry)

        carry = lax.fori_loop(0, (tiles - 1) // 2, body, (jnp.full((8, cols), -jnp.inf, jnp.float32), zero, zero))
        if tiles % 2 == 0:
            product(tiles - 1, 1)
            carry = absorb(tiles - 2, 0, carry)
        top, total, target = absorb(tiles - 1, (tiles - 1) % 2, carry)
        best = jnp.max(top, axis=0, keepdims=True)
        total = jnp.sum(total * jnp.exp2((top - best) * rate), axis=0, keepdims=True)
        target = jnp.sum(target, axis=0, keepdims=True)
        for pos, h in enumerate(halves):
            lanes = slice(pos * HALF, (pos + 1) * HALF)
            stats[0, pl.ds(h, 1), :] = best[:, lanes] * scale
            stats[1, pl.ds(h, 1), :] = total[:, lanes]
            stats[2, pl.ds(h, 1), :] = target[:, lanes] * scale

    gather_units(place, z, asend, arecv, work)
    finals = []
    for k, (chip, core) in enumerate(everyone()):
        finals.append(push(stats, every.at[place.me], ssend.at[k], srecv.at[k], place.at(chip, core)))
    every[place.me] = stats[...]
    for copy in finals:
        copy.wait()
    for copy in heads_in.values():
        copy.wait_send()
    tops = every[:, 0]
    best = jnp.max(tops, axis=0)
    total = jnp.sum(every[:, 1] * jnp.exp(tops - best[None]), axis=0)
    out_ref[...] = jnp.sum(every[:, 2], axis=0) - best - jnp.log(total)


def epilogue(attn, m, w_out, x_own, gain, ids, embed_loc):
    group, rows, attn_dev = attn.shape
    vocab, dim = embed_loc.shape
    tile = 560
    vmem = pl.BlockSpec(memory_space=pltpu.VMEM)
    dma = pltpu.SemaphoreType.DMA
    halves = group * rows // HALF
    return pl.pallas_call(
        functools.partial(epilogue_kernel, dim ** -0.5, tile),
        in_specs=[vmem] * 6 + [pl.BlockSpec(memory_space=pl.ANY)],
        out_specs=vmem,
        out_shape=jax.ShapeDtypeStruct((halves, HALF), jnp.float32),
        scratch_shapes=[
            pltpu.VMEM((vocab, dim), jnp.bfloat16),
            pltpu.VMEM((group, rows, dim), jnp.bfloat16),
            pltpu.VMEM((4, rows, dim), jnp.bfloat16),
            pltpu.VMEM((2, HALF, dim), jnp.bfloat16),
            pltpu.VMEM((2, HALF, dim), jnp.bfloat16),
            pltpu.VMEM((2, HALF, dim), jnp.bfloat16),
            pltpu.VMEM((group, rows, attn_dev), jnp.bfloat16),
            pltpu.VMEM((2, tile, 2 * UNIT), jnp.float32),
            pltpu.VMEM((3, halves, HALF), jnp.float32),
            pltpu.VMEM((group, 3, halves, HALF), jnp.float32),
            dma((vocab // tile,)),
            dma((4,)), dma((4,)), dma((6,)), dma((6,)), dma((10,)), dma((10,)), dma((7,)), dma((7,)), dma((7,)), dma((7,)),
        ],
        compiler_params=pltpu.CompilerParams(collective_id=1, has_side_effects=True, vmem_limit_bytes=67043328),
        name="epilogue",
    )(attn, m, w_out, x_own, gain, ids, embed_loc)


def solution(mesh):
    group_size = mesh.shape['tp']

    def device_fn(tok_ids, next_ids, seq_lens, embed_loc, ln_gain, w_in_loc, w_out_loc, final_gain, k_loc, v_loc):
        num_steps, batch_size = tok_ids.shape
        batch_dev = batch_size // group_size
        rows_dev = num_steps * batch_dev
        vocab_dev, model_dim = embed_loc.shape
        head_dim = k_loc.shape[2]
        in_dev = w_in_loc.shape[1]
        out_dev = w_out_loc.shape[0]
        kv_dev = 2 * head_dim // group_size
        attn_dev = 2 * out_dev - in_dev + kv_dev
        ff_dev = out_dev - attn_dev
        qkv_dev = attn_dev + kv_dev
        dev_index = lax.axis_index('tp')
        vocab_start = dev_index * vocab_dev
        own_lens = lax.dynamic_slice_in_dim(seq_lens, dev_index * batch_dev, batch_dev)

        def by_device(ids):
            return ids.reshape(num_steps, group_size, batch_dev).transpose(1, 0, 2)

        local_ids = by_device(tok_ids).reshape(-1) - vocab_start
        x_part = embed_loc.at[jnp.clip(local_ids, 0, vocab_dev - 1)].get(mode="promise_in_bounds")
        mate_ids = local_ids - (1 - 2 * (dev_index % 2)) * vocab_dev
        tok_mine = (local_ids >= 0) & (local_ids < vocab_dev)
        tok_mate = (mate_ids >= 0) & (mate_ids < vocab_dev)
        code = jnp.where(tok_mine, 1, jnp.where(tok_mate, 2, 0)).astype(jnp.int32)
        code = jnp.broadcast_to(code[:, None], (code.shape[0], 128))
        x_own, mlp_act, qkv_own = prologue(x_part.reshape(group_size, rows_dev, model_dim), code, ln_gain[None], w_in_loc.T, qkv_dev, ff_dev)
        qkv_own = qkv_own.transpose(1, 0, 2).reshape(num_steps, batch_dev, -1)

        half = head_dim // 2
        inv_freq = ROPE_BASE ** (-jnp.arange(half, dtype=jnp.float32) / half)
        positions = own_lens[None, :] + jnp.arange(num_steps, dtype=jnp.int32)[:, None]
        angles = positions.astype(jnp.float32)[..., None] * inv_freq
        cos, sin = jnp.cos(angles), jnp.sin(angles)
        cos = jnp.concatenate([cos, cos], axis=-1)
        sin = jnp.concatenate([-sin, sin], axis=-1)
        attn_out, k_out, v_out = attention(own_lens, qkv_own, cos, sin, k_loc, v_loc, group_size)
        local_next = by_device(next_ids).reshape(2 * group_size, 1, batch_dev) - vocab_start
        ids8 = jnp.broadcast_to(local_next, (2 * group_size, 8, batch_dev))
        log_probs = epilogue(attn_out.reshape(group_size, rows_dev, attn_dev), mlp_act, w_out_loc, x_own, final_gain[None], ids8, embed_loc)
        log_probs = log_probs.reshape(group_size, num_steps, batch_dev).transpose(1, 0, 2).reshape(num_steps, batch_size)
        return log_probs, k_out, v_out

    cache_spec = P('tp', None, None)
    return jax.shard_map(device_fn, mesh=mesh, in_specs=(P(), P(), P(), P('tp', None), P(), P(None, 'tp'), P('tp', None), P(), cache_spec, cache_spec), out_specs=(P(), cache_spec, cache_spec), check_vma=False)
```

```python
import functools

import jax
import jax.numpy as jnp
from jax import lax
from jax.experimental import pallas as pl
from jax.experimental.pallas import tpu as pltpu
from jax.sharding import PartitionSpec as P

ROPE_BASE = 10000.0
NORM_EPS = 1e-6
LOG2E = 1.4426950408889634


def layer_norm(values, gain_vec):
    centered = values.astype(jnp.float32)
    centered = centered - jnp.mean(centered, axis=-1, keepdims=True)
    variance = jnp.mean(jnp.square(centered), axis=-1, keepdims=True)
    scaled = centered * lax.rsqrt(variance + NORM_EPS) * gain_vec.astype(jnp.float32)
    return scaled.astype(jnp.bfloat16)


def attention_kernel(ahead, lens_ref, qkv_ref, cos_ref, sin_ref, k_hbm, v_hbm, o_ref, ko_hbm, vo_hbm, k_buf, v_buf, q_scr, o_scr, n_scr, s_scr, p_scr, read_sem, write_sem):
    num_steps, blocks, rows, _ = qkv_ref.shape
    slots, _, cache_len, head = k_buf.shape
    pack = o_ref.shape[4] // head
    heads = o_ref.shape[0] * pack
    per_seq = num_steps * heads
    win_row = lax.broadcasted_iota(jnp.int32, (16, head), 0)
    col = lax.broadcasted_iota(jnp.int32, (per_seq, cache_len), 1) - lax.broadcasted_iota(jnp.int32, (per_seq, cache_len), 0) // heads
    depth = s_scr.shape[0]

    def moves(block, slot, out):
        here = pl.ds(pl.multiple_of(block * rows, rows), rows)
        pairs = []
        for which, (hbm, hbm_out, buf) in enumerate(((k_hbm, ko_hbm, k_buf), (v_hbm, vo_hbm, v_buf))):
            if out:
                pairs.append(pltpu.make_async_copy(buf.at[slot], hbm_out.at[here], write_sem.at[which, slot]))
            else:
                pairs.append(pltpu.make_async_copy(hbm.at[here], buf.at[slot], read_sem.at[which, slot]))
        return pairs

    for block in range(ahead):
        for copy in moves(block, block, False):
            copy.start()

    @pl.loop(0, blocks)
    def _(block):
        slot = lax.rem(block, slots)

        @pl.when(block + ahead < blocks)
        def _():
            later = lax.rem(block + ahead, slots)

            @pl.when(block + ahead >= slots)
            def _():
                for copy in moves(block + ahead - slots, later, True):
                    copy.wait()

            for copy in moves(block + ahead, later, False):
                copy.start()

        for s in range(num_steps):
            cos, sin = cos_ref[s, block], sin_ref[s, block]

            def rotate(lo):
                x = qkv_ref[s, block, :, lo:lo + head].astype(jnp.float32)
                return x * cos + pltpu.roll(x, head // 2, 1) * sin

            for h in range(heads):
                q_scr[pl.ds(s * heads + h, rows, stride=per_seq), :] = rotate(h * head) * head ** -0.5
            n_scr[0, s] = rotate(heads * head).astype(jnp.bfloat16).astype(jnp.float32)
            n_scr[1, s] = qkv_ref[s, block, :, (heads + 1) * head:].astype(jnp.float32)

        for copy in moves(block, slot, False):
            copy.wait()

        def insert(b):
            length = lens_ref[block * rows + b]
            for dst, which in ((k_buf, 0), (v_buf, 1)):
                for s in range(num_steps):
                    pos = length + s
                    base = pl.multiple_of((pos // 16) * 16, 16)
                    window = dst[slot, b, pl.ds(base, 16), :].astype(jnp.float32)
                    fresh = n_scr[which, s, b:b + 1, :]
                    window = jnp.where(win_row == pos - base, fresh, window)
                    dst[slot, b, pl.ds(base, 16), :] = window.astype(jnp.bfloat16)

        def score(b):
            q = q_scr[b * per_seq:(b + 1) * per_seq, :].astype(jnp.bfloat16)
            s_scr[b % depth] = lax.dot_general(q, k_buf[slot, b], (((1,), (1,)), ((), ())), preferred_element_type=jnp.float32)

        def soften(b):
            scores = jnp.where(col <= lens_ref[block * rows + b], s_scr[b % depth], -jnp.inf)
            top = jnp.max(scores, axis=1, keepdims=True)
            weight = jnp.exp(scores - top)
            total = jnp.sum(weight, axis=1, keepdims=True)
            p_scr[b % depth] = (weight * (1.0 / total)).astype(jnp.bfloat16)

        def mix(b):
            o_scr[b * per_seq:(b + 1) * per_seq, :] = jnp.dot(p_scr[b % depth], v_buf[slot, b], preferred_element_type=jnp.float32)

        for i in range(rows):
            insert(i)
        for i in range(rows + 2):
            if i < rows:
                score(i)
            if 0 <= i - 1 < rows:
                soften(i - 1)
            if 0 <= i - 2 < rows:
                mix(i - 2)

        for copy in moves(block, slot, True):
            copy.start()
        for s in range(num_steps):
            for h in range(heads):
                o_ref[h // pack, s, block, :, (h % pack) * head:(h % pack + 1) * head] = o_scr[pl.ds(s * heads + h, rows, stride=per_seq), :].astype(jnp.bfloat16)

    for block in range(blocks - slots, blocks):
        for copy in moves(block, block % slots, True):
            copy.wait()


def attention(lens, qkv, cos, sin, k_loc, v_loc, group):
    num_steps, batch, width = qkv.shape
    cache_len, head = k_loc.shape[1], k_loc.shape[2]
    attn_width = width - 2 * head
    heads = attn_width // head
    rows, slots, ahead = 8, 5, 3
    blocks = batch // rows
    vmem, anywhere = pl.BlockSpec(memory_space=pltpu.VMEM), pl.BlockSpec(memory_space=pl.ANY)
    in_blocks = lambda a: a.reshape(num_steps, blocks, rows, a.shape[-1])
    out, k_out, v_out = pl.pallas_call(
        functools.partial(attention_kernel, ahead),
        in_specs=[pl.BlockSpec(memory_space=pltpu.SMEM), vmem, vmem, vmem, anywhere, anywhere],
        out_specs=[vmem, anywhere, anywhere],
        out_shape=[
            jax.ShapeDtypeStruct((group, num_steps, blocks, rows, attn_width // group), jnp.bfloat16),
            jax.ShapeDtypeStruct(k_loc.shape, k_loc.dtype),
            jax.ShapeDtypeStruct(v_loc.shape, v_loc.dtype),
        ],
        scratch_shapes=[
            pltpu.VMEM((slots, rows, cache_len, head), jnp.bfloat16),
            pltpu.VMEM((slots, rows, cache_len, head), jnp.bfloat16),
            pltpu.VMEM((rows * num_steps * heads, head), jnp.float32),
            pltpu.VMEM((rows * num_steps * heads, head), jnp.float32),
            pltpu.VMEM((2, num_steps, rows, head), jnp.float32),
            pltpu.VMEM((4, num_steps * heads, cache_len), jnp.float32),
            pltpu.VMEM((4, num_steps * heads, cache_len), jnp.bfloat16),
            pltpu.SemaphoreType.DMA((2, slots)),
            pltpu.SemaphoreType.DMA((2, slots)),
        ],
        compiler_params=pltpu.CompilerParams(vmem_limit_bytes=56 * 1024 * 1024),
        name="attention",
    )(lens, in_blocks(qkv), in_blocks(cos), in_blocks(sin), k_loc, v_loc)
    return out.reshape(group, num_steps, batch, attn_width // group), k_out, v_out


HALF = 128
UNIT = 2 * HALF
OWN, XN, YN, DIAG = (0, 0), (1, 0), (0, 1), (1, 1)
REDUCE_ORDER = (DIAG, XN, YN, OWN)
UNIT_HALVES = (((OWN, 0), (OWN, 1)), ((XN, 1), (YN, 0)), ((XN, 0), (YN, 1)), ((DIAG, 0), (DIAG, 1)))
MESH = pl.DeviceIdType.MESH


class Place:
    def __init__(self):
        me = lax.axis_index('tp')
        self.me = me
        self.core, self.x, self.y = me % 2, (me // 2) % 2, me // 4

    def at(self, chip, core):
        x = self.x if chip[0] == 0 else 1 - self.x
        y = self.y if chip[1] == 0 else 1 - self.y
        c = self.core if core == 0 else 1 - self.core
        return y * 4 + x * 2 + c


def everyone():
    return [(chip, core) for chip in (DIAG, XN, YN, OWN) for core in (1, 0) if (chip, core) != (OWN, 0)]


def greet(place):
    barrier = pltpu.get_barrier_semaphore()
    for chip, core in everyone():
        pl.semaphore_signal(barrier, inc=1, device_id=(place.at(chip, core),), device_id_type=MESH)
    pl.semaphore_wait(barrier, 7)


def push(src, dst, send, recv, target):
    copy = pltpu.make_async_remote_copy(src_ref=src, dst_ref=dst, send_sem=send, recv_sem=recv, device_id=(target,), device_id_type=MESH)
    copy.start()
    return copy


def reduce_rows(place, outgoing, own_block, rc, r1a, r1b, r2, csend, crecv, psend, precv, between=None):
    dim = rc.shape[2]
    partner = place.at(OWN, 1)
    to_x, to_y = place.at(XN, 0), place.at(YN, 0)
    first, second = pl.ds(0, HALF), pl.ds(HALF, HALF)
    exchange = []
    for i, chip in enumerate(REDUCE_ORDER):
        src = outgoing(i, place.at(chip, 1))
        exchange.append(push(src, rc.at[i], csend.at[i], crecv.at[i], partner))
    sends = []
    for i, chip in enumerate(REDUCE_ORDER):
        own_block(i, place.at(chip, 0), exchange[i])
        if chip == DIAG:
            sends.append(push(rc.at[i, first], r1a.at[0], psend.at[0], precv.at[0], to_x))
            sends.append(push(rc.at[i, second], r1b.at[0], psend.at[1], precv.at[1], to_y))
        elif chip == XN:
            sends.append(push(rc.at[i, first], r1a.at[1], psend.at[2], precv.at[2], to_x))
        elif chip == YN:
            sends.append(push(rc.at[i, second], r1b.at[1], psend.at[3], precv.at[3], to_y))
    for copy in exchange:
        copy.wait_send()
    for j, (slot, rows, landed, target) in enumerate(((2, 0, r1a, to_y), (1, HALF, r1b, to_x))):
        sends[j].wait_recv()

        @pl.loop(0, HALF // 16)
        def _(r):
            here = pl.ds(pl.multiple_of(rows + r * 16, 16), 16)
            there = pl.ds(pl.multiple_of(r * 16, 16), 16)
            total = rc[slot, here, :].astype(jnp.float32) + landed[0, there, :].astype(jnp.float32)
            rc[slot, here, :] = total.astype(jnp.bfloat16)

        sends.append(push(rc.at[slot, pl.ds(rows, HALF)], r2.at[j], psend.at[4 + j], precv.at[4 + j], target))
    for copy in sends[2:]:
        copy.wait_recv()
    for copy in sends:
        copy.wait_send()


def own_rows(rc, r1a, r1b, r2, half, r, rows):
    here = pl.ds(pl.multiple_of(half * HALF + r * rows, rows), rows)
    there = pl.ds(pl.multiple_of(r * rows, rows), rows)
    landed = r1b if half else r1a
    return rc[3, here, :].astype(jnp.float32) + landed[1, there, :].astype(jnp.float32) + r2[half, there, :].astype(jnp.float32)


def norm_rows(values, gain):
    centered = values - jnp.mean(values, axis=-1, keepdims=True)
    variance = jnp.mean(centered * centered, axis=-1, keepdims=True)
    return (centered * lax.rsqrt(variance + NORM_EPS) * gain).astype(jnp.bfloat16)


def gather_units(place, z, asend, arecv, work):
    partner = place.at(OWN, 1)
    to_x, to_y = place.at(XN, 0), place.at(YN, 0)
    part = lambda unit, pos: z.at[unit, pl.ds(pos * HALF, HALF)]
    sends = []

    def go(src, dst, slot, target):
        k = len(sends)
        sends.append(push(src, dst, asend.at[k], arecv.at[slot], target))
        return sends[-1]

    xb = go(part(0, 1), part(2, 0), 0, to_x)
    ya = go(part(0, 0), part(2, 1), 1, to_y)
    near = go(z.at[0], z.at[1], 2, partner)
    xa = go(part(0, 0), part(4, 0), 3, to_x)
    yb = go(part(0, 1), part(4, 1), 4, to_y)
    near.wait_recv()
    work(0)
    xb.wait_recv()
    db = go(part(2, 0), part(6, 1), 5, to_y)
    ya.wait_recv()
    da = go(part(2, 1), part(6, 0), 6, to_x)
    near2 = go(z.at[2], z.at[3], 7, partner)
    near2.wait_recv()
    work(1)
    xa.wait_recv()
    yb.wait_recv()
    near4 = go(z.at[4], z.at[5], 8, partner)
    near4.wait_recv()
    work(2)
    da.wait_recv()
    db.wait_recv()
    near6 = go(z.at[6], z.at[7], 9, partner)
    near6.wait_recv()
    work(3)
    for copy in sends:
        copy.wait_send()


def prologue_kernel(widths, part_ref, code_ref, gain_ref, w_hbm, x_ref, m_ref, qkv_ref, z, rc, r1a, r1b, r2, w_buf, qkv_out, w_sem, csend, crecv, psend, precv, asend, arecv, qsend, qrecv):
    qkv_dev, ff_dev = widths
    dim = part_ref.shape[2]
    place = Place()
    greet(place)
    load = pltpu.make_async_copy(w_hbm, w_buf, w_sem)
    load.start()

    def own_block(i, block, copy):
        copy.wait_recv()

        @pl.loop(0, UNIT // 32)
        def _(r):
            here = pl.ds(pl.multiple_of(r * 32, 32), 32)
            code = code_ref[pl.ds(pl.multiple_of(block * UNIT + r * 32, 32), 32), :]
            for c in range(dim // 128):
                lanes = slice(c * 128, (c + 1) * 128)
                theirs = jnp.where(code == 2, rc[i, here, lanes].astype(jnp.float32), 0.0)
                rc[i, here, lanes] = jnp.where(code == 1, part_ref[block, here, lanes].astype(jnp.float32), theirs).astype(jnp.bfloat16)

    reduce_rows(place, lambda i, block: part_ref.at[block], own_block, rc, r1a, r1b, r2, csend, crecv, psend, precv)
    gain = gain_ref[...].astype(jnp.float32)
    rows = 16
    for half in range(2):
        @pl.loop(0, HALF // rows // 4)
        def _(q):
            for g in range(4):
                r = q * 4 + g
                here = pl.ds(pl.multiple_of(half * HALF + r * rows, rows), rows)
                x = own_rows(rc, r1a, r1b, r2, half, r, rows).astype(jnp.bfloat16)
                x_ref[here, :] = x
                z[0, here, :] = norm_rows(x.astype(jnp.float32), gain)

    out_sends = []

    def times(rows, first, count):
        return lax.dot_general(rows, w_buf[pl.ds(first, count), :], (((1,), (1,)), ((), ())), preferred_element_type=jnp.float32)

    def work(pair):
        if pair == 0:
            load.wait()
        rows = z[2 * pair:2 * pair + 2].reshape(2 * UNIT, dim)
        qkv_out[2 * pair:2 * pair + 2] = times(rows, 0, qkv_dev).astype(jnp.bfloat16).reshape(2, UNIT, qkv_dev)
        for core in range(2):
            for pos, (chip, half) in enumerate(UNIT_HALVES[pair]):
                unit = 2 * pair + core
                block = place.at(chip, core)
                src = qkv_out.at[unit, pl.ds(pos * HALF, HALF)]
                if unit == 0:
                    qkv_ref[place.me, pl.ds(half * HALF, HALF), :] = qkv_out[unit, pl.ds(pos * HALF, HALF), :]
                else:
                    k = len(out_sends)
                    out_sends.append(push(src, qkv_ref.at[place.me, pl.ds(half * HALF, HALF)], qsend.at[k], qrecv.at[k], block))
        tile = 256

        @pl.loop(0, ff_dev // tile)
        def _(n):
            at = pl.multiple_of(n * tile, tile)
            gate = times(rows, pl.multiple_of(qkv_dev + at, 16), tile).astype(jnp.bfloat16).astype(jnp.float32)
            up = times(rows, pl.multiple_of(qkv_dev + ff_dev + at, 16), tile).astype(jnp.bfloat16).astype(jnp.float32)
            act = (gate / (1.0 + jnp.exp(-gate)) * up).astype(jnp.bfloat16)
            for core in range(2):
                for pos, (chip, half) in enumerate(UNIT_HALVES[pair]):
                    first = place.at(chip, core) * UNIT + half * HALF
                    k = core * UNIT + pos * HALF
                    m_ref[pl.ds(pl.multiple_of(first, HALF), HALF), pl.ds(at, tile)] = act[k:k + HALF]

    gather_units(place, z, asend, arecv, work)
    for copy in out_sends:
        copy.wait()


def prologue(part, code, gain, w_in, qkv_dev, ff_dev):
    group, rows, dim = part.shape
    vmem = pl.BlockSpec(memory_space=pltpu.VMEM)
    dma = pltpu.SemaphoreType.DMA
    return pl.pallas_call(
        functools.partial(prologue_kernel, (qkv_dev, ff_dev)),
        in_specs=[vmem] * 3 + [pl.BlockSpec(memory_space=pl.ANY)],
        out_specs=[vmem] * 3,
        out_shape=[
            jax.ShapeDtypeStruct((rows, dim), jnp.bfloat16),
            jax.ShapeDtypeStruct((group * rows, ff_dev), jnp.bfloat16),
            jax.ShapeDtypeStruct((group, rows, qkv_dev), jnp.bfloat16),
        ],
        scratch_shapes=[
            pltpu.VMEM((group, rows, dim), jnp.bfloat16),
            pltpu.VMEM((4, rows, dim), jnp.bfloat16),
            pltpu.VMEM((2, HALF, dim), jnp.bfloat16),
            pltpu.VMEM((2, HALF, dim), jnp.bfloat16),
            pltpu.VMEM((2, HALF, dim), jnp.bfloat16),
            pltpu.VMEM(w_in.shape, jnp.bfloat16),
            pltpu.VMEM((group, rows, qkv_dev), jnp.bfloat16),
            dma,
            dma((4,)), dma((4,)), dma((6,)), dma((6,)), dma((10,)), dma((10,)), dma((14,)), dma((14,)),
        ],
        compiler_params=pltpu.CompilerParams(collective_id=0, has_side_effects=True, vmem_limit_bytes=60 * 1024 * 1024),
        name="prologue",
    )(part, code, gain, w_in)


SLOTS = ((OWN, 0), (OWN, 1), (XN, 0), (XN, 1), (YN, 0), (YN, 1), (DIAG, 0), (DIAG, 1))
PIECE = HALF // 2


def epilogue_kernel(scale, tile, attn_ref, m_ref, w_ref, x_ref, gain_ref, ids_ref, e_hbm, out_ref, e_buf, z, rc, r1a, r1b, r2, a_in, raw, stats, every, e_sem, csend, crecv, psend, precv, asend, arecv, qsend, qrecv, ssend, srecv):
    vocab = e_hbm.shape[0]
    tiles = vocab // tile
    dim = z.shape[3]
    attn_dev = a_in.shape[2]
    loads = [pltpu.make_async_copy(e_hbm.at[pl.ds(t * tile, tile)], e_buf.at[pl.ds(t * tile, tile)], e_sem.at[t]) for t in range(tiles)]
    place = Place()
    greet(place)
    partner = place.at(OWN, 1)
    to_x, to_y = place.at(XN, 0), place.at(YN, 0)
    heads_in = {}
    for k, (chip, core) in enumerate(everyone()):
        target = place.at(chip, core)
        heads_in[(chip, core)] = push(attn_ref.at[target], a_in.at[place.me], qsend.at[k], qrecv.at[k], target)
    for c in loads:
        c.start()
    a_in[place.me] = attn_ref[place.me]

    def block_dot(block, n):
        lanes = pl.ds(pl.multiple_of(n * 512, 512), 512)
        mine = jnp.dot(a_in[block], w_ref[pl.ds(0, attn_dev), lanes], preferred_element_type=jnp.float32)
        rows = pl.ds(pl.multiple_of(block * UNIT, UNIT), UNIT)
        return mine + jnp.dot(m_ref[rows, :], w_ref[pl.ds(attn_dev, w_ref.shape[0] - attn_dev), lanes], preferred_element_type=jnp.float32)

    exchange = []
    for i, chip in enumerate(REDUCE_ORDER):
        heads_in[(chip, 1)].wait_recv()
        block = place.at(chip, 1)

        @pl.loop(0, dim // 512)
        def _(n):
            lanes = pl.ds(pl.multiple_of(n * 512, 512), 512)
            both = block_dot(block, n).astype(jnp.bfloat16)
            z[0, 2 * i, :, lanes] = both[:HALF]
            z[1, 2 * i, :, lanes] = both[HALF:]

        for h in range(2):
            exchange.append(push(z.at[h, 2 * i], rc.at[i, pl.ds(h * HALF, HALF)], csend.at[2 * i + h], crecv.at[2 * i + h], partner))

    partial = {}

    def first_send(sub, i):
        chip = REDUCE_ORDER[i]
        upper, lower = rc.at[i, pl.ds(sub * PIECE, PIECE)], rc.at[i, pl.ds(HALF + sub * PIECE, PIECE)]
        k = sub * 6
        if chip == DIAG:
            partial[sub, 0] = push(upper, r1a.at[sub, 0], psend.at[k], precv.at[k], to_x)
            partial[sub, 1] = push(lower, r1b.at[sub, 0], psend.at[k + 1], precv.at[k + 1], to_y)
        elif chip == XN:
            partial[sub, 2] = push(upper, r1a.at[sub, 1], psend.at[k + 2], precv.at[k + 2], to_x)
        elif chip == YN:
            partial[sub, 3] = push(lower, r1b.at[sub, 1], psend.at[k + 3], precv.at[k + 3], to_y)

    def second_send(sub):
        for q, (slot, rows, landed, target) in enumerate(((2, sub * PIECE, r1a, to_y), (1, HALF + sub * PIECE, r1b, to_x))):
            partial[sub, q].wait_recv()

            @pl.loop(0, PIECE // 16)
            def _(r):
                here = pl.ds(pl.multiple_of(rows + r * 16, 16), 16)
                there = pl.ds(pl.multiple_of(r * 16, 16), 16)
                total = rc[slot, here, :].astype(jnp.float32) + landed[sub, 0, there, :].astype(jnp.float32)
                rc[slot, here, :] = total.astype(jnp.bfloat16)

            k = sub * 6 + 4 + q
            partial[sub, 4 + q] = push(rc.at[slot, pl.ds(rows, PIECE)], r2.at[sub, q], psend.at[k], precv.at[k], target)

    gain = gain_ref[...].astype(jnp.float32)

    def finish_rows(sub):
        for k in range(2, 6):
            partial[sub, k].wait_recv()
        for half, landed in enumerate((r1a, r1b)):
            for g in range(PIECE // 16):
                there = pl.ds(g * 16, 16)
                here = pl.ds(half * HALF + sub * PIECE + g * 16, 16)
                o = rc[3, here, :].astype(jnp.float32) + landed[sub, 1, there, :].astype(jnp.float32) + r2[sub, half, there, :].astype(jnp.float32)
                o = o.astype(jnp.bfloat16).astype(jnp.float32)
                z[sub, 0, half * PIECE + g * 16:half * PIECE + g * 16 + 16, :] = norm_rows(x_ref[here, :].astype(jnp.float32) + o, gain)

    moved = {}

    def go(sub, k, src, dst, target):
        moved[sub, k] = push(src, dst, asend.at[sub * 10 + k], arecv.at[sub * 10 + k], target)

    def part(sub, slot, half):
        return z.at[sub, slot, pl.ds(half * PIECE, PIECE)]

    def gather_start(sub):
        go(sub, 0, part(sub, 0, 1), part(sub, 2, 1), to_x)
        go(sub, 1, part(sub, 0, 0), part(sub, 4, 0), to_y)
        go(sub, 2, z.at[sub, 0], z.at[sub, 1], partner)
        go(sub, 3, part(sub, 0, 0), part(sub, 2, 0), to_x)
        go(sub, 4, part(sub, 0, 1), part(sub, 4, 1), to_y)

    def gather_relay(sub):
        moved[sub, 0].wait_recv()
        go(sub, 5, part(sub, 2, 1), part(sub, 6, 1), to_y)
        moved[sub, 1].wait_recv()
        go(sub, 6, part(sub, 4, 0), part(sub, 6, 0), to_x)

    def gather_sides(sub):
        moved[sub, 3].wait_recv()
        go(sub, 7, z.at[sub, 2], z.at[sub, 3], partner)
        moved[sub, 4].wait_recv()
        go(sub, 8, z.at[sub, 4], z.at[sub, 5], partner)
        moved[sub, 7].wait_recv()
        moved[sub, 8].wait_recv()

    def gather_far(sub):
        moved[sub, 6].wait_recv()
        moved[sub, 5].wait_recv()
        go(sub, 9, z.at[sub, 6], z.at[sub, 7], partner)
        moved[sub, 9].wait_recv()

    def work(sub, first, count):
        cols = count * HALF
        places = [place.at(*SLOTS[first + k]) * 2 + sub for k in range(count)]
        row = lax.broadcasted_iota(jnp.int32, (8, cols), 0)
        ids = jnp.concatenate([ids_ref[h] for h in places], axis=1) - row
        rate = scale * LOG2E

        def product(t, slot):
            e = e_buf[pl.ds(pl.multiple_of(t * tile, 16), tile), :]
            rows = z[sub, first:first + count].reshape(cols, dim)
            raw[slot, :, :cols] = lax.dot_general(e, rows, (((1,), (1,)), ((), ())), preferred_element_type=jnp.float32)

        def absorb(t, slot, carry):
            top, total, target = carry
            local = ids - t * tile
            each = tile // 8
            tops = [top, None]
            for r in range(each):
                v = raw[slot, r * 8:r * 8 + 8, :cols]
                k = r % 2
                tops[k] = v if tops[k] is None else jnp.maximum(tops[k], v)
            new_top = jnp.maximum(tops[0], tops[1])
            sums = [total * jnp.exp2((top - new_top) * rate), None]
            for r in range(each):
                v = raw[slot, r * 8:r * 8 + 8, :cols]
                k = r % 2
                p = jnp.exp2((v - new_top) * rate)
                sums[k] = p if sums[k] is None else sums[k] + p
                target = target + jnp.where(local == r * 8, v, 0.0)
            return new_top, sums[0] + sums[1], target

        zero = jnp.zeros((8, cols), jnp.float32)
        product(0, 0)

        def body(i, carry):
            product(2 * i + 1, 1)
            carry = absorb(2 * i, 0, carry)
            product(2 * i + 2, 0)
            return absorb(2 * i + 1, 1, carry)

        carry = lax.fori_loop(0, (tiles - 1) // 2, body, (jnp.full((8, cols), -jnp.inf, jnp.float32), zero, zero))
        if tiles % 2 == 0:
            product(tiles - 1, 1)
            carry = absorb(tiles - 2, 0, carry)
        top, total, target = absorb(tiles - 1, (tiles - 1) % 2, carry)
        best = jnp.max(top, axis=0, keepdims=True)
        total = jnp.sum(total * jnp.exp2((top - best) * rate), axis=0, keepdims=True)
        target = jnp.sum(target, axis=0, keepdims=True)
        for pos, h in enumerate(places):
            lanes = slice(pos * HALF, (pos + 1) * HALF)
            stats[0, pl.ds(h, 1), :] = best[:, lanes] * scale
            stats[1, pl.ds(h, 1), :] = total[:, lanes]
            stats[2, pl.ds(h, 1), :] = target[:, lanes] * scale

    for i, chip in enumerate(REDUCE_ORDER):
        if chip != OWN:
            heads_in[(chip, 0)].wait_recv()
        exchange[2 * i].wait_recv()
        exchange[2 * i + 1].wait_recv()
        block = place.at(chip, 0)

        @pl.loop(0, dim // 512)
        def _(n):
            lanes = pl.ds(pl.multiple_of(n * 512, 512), 512)
            rc[i, :, lanes] = (block_dot(block, n) + rc[i, :, lanes].astype(jnp.float32)).astype(jnp.bfloat16)

        first_send(0, i)
    for copy in exchange:
        copy.wait_send()
    second_send(0)
    first_send(1, 0)
    finish_rows(0)
    gather_start(0)
    first_send(1, 1)
    first_send(1, 2)
    for c in loads:
        c.wait()
    moved[0, 2].wait_recv()
    work(0, 0, 2)
    gather_relay(0)
    second_send(1)
    gather_sides(0)
    work(0, 2, 4)
    finish_rows(1)
    gather_start(1)
    gather_far(0)
    work(0, 6, 2)
    gather_relay(1)
    moved[1, 2].wait_recv()
    work(1, 0, 2)
    gather_sides(1)
    work(1, 2, 4)
    gather_far(1)
    work(1, 6, 2)
    for copy in list(partial.values()) + list(moved.values()) + list(heads_in.values()):
        copy.wait_send()
    finals = []
    for k, (chip, core) in enumerate(everyone()):
        finals.append(push(stats, every.at[place.me], ssend.at[k], srecv.at[k], place.at(chip, core)))
    every[place.me] = stats[...]
    for copy in finals:
        copy.wait()
    tops = every[:, 0]
    best = jnp.max(tops, axis=0)
    total = jnp.sum(every[:, 1] * jnp.exp(tops - best[None]), axis=0)
    out_ref[...] = jnp.sum(every[:, 2], axis=0) - best - jnp.log(total)


def epilogue(attn, m, w_out, x_own, gain, ids, embed_loc):
    group, rows, attn_dev = attn.shape
    vocab, dim = embed_loc.shape
    tile = 560
    vmem = pl.BlockSpec(memory_space=pltpu.VMEM)
    dma = pltpu.SemaphoreType.DMA
    halves = group * rows // HALF
    return pl.pallas_call(
        functools.partial(epilogue_kernel, dim ** -0.5, tile),
        in_specs=[vmem] * 6 + [pl.BlockSpec(memory_space=pl.ANY)],
        out_specs=vmem,
        out_shape=jax.ShapeDtypeStruct((halves, HALF), jnp.float32),
        scratch_shapes=[
            pltpu.VMEM((vocab, dim), jnp.bfloat16),
            pltpu.VMEM((2, group, HALF, dim), jnp.bfloat16),
            pltpu.VMEM((4, rows, dim), jnp.bfloat16),
            pltpu.VMEM((2, 2, PIECE, dim), jnp.bfloat16),
            pltpu.VMEM((2, 2, PIECE, dim), jnp.bfloat16),
            pltpu.VMEM((2, 2, PIECE, dim), jnp.bfloat16),
            pltpu.VMEM((group, rows, attn_dev), jnp.bfloat16),
            pltpu.VMEM((2, tile, 2 * UNIT), jnp.float32),
            pltpu.VMEM((3, halves, HALF), jnp.float32),
            pltpu.VMEM((group, 3, halves, HALF), jnp.float32),
            dma((vocab // tile,)),
            dma((8,)), dma((8,)), dma((12,)), dma((12,)), dma((20,)), dma((20,)), dma((7,)), dma((7,)), dma((7,)), dma((7,)),
        ],
        compiler_params=pltpu.CompilerParams(collective_id=1, has_side_effects=True, vmem_limit_bytes=67043328),
        name="epilogue",
    )(attn, m, w_out, x_own, gain, ids, embed_loc)


def solution(mesh):
    group_size = mesh.shape['tp']

    def device_fn(tok_ids, next_ids, seq_lens, embed_loc, ln_gain, w_in_loc, w_out_loc, final_gain, k_loc, v_loc):
        num_steps, batch_size = tok_ids.shape
        batch_dev = batch_size // group_size
        rows_dev = num_steps * batch_dev
        vocab_dev, model_dim = embed_loc.shape
        head_dim = k_loc.shape[2]
        in_dev = w_in_loc.shape[1]
        out_dev = w_out_loc.shape[0]
        kv_dev = 2 * head_dim // group_size
        attn_dev = 2 * out_dev - in_dev + kv_dev
        ff_dev = out_dev - attn_dev
        qkv_dev = attn_dev + kv_dev
        dev_index = lax.axis_index('tp')
        vocab_start = dev_index * vocab_dev
        own_lens = lax.dynamic_slice_in_dim(seq_lens, dev_index * batch_dev, batch_dev)

        def by_device(ids):
            return ids.reshape(num_steps, group_size, batch_dev).transpose(1, 0, 2)

        local_ids = by_device(tok_ids).reshape(-1) - vocab_start
        x_part = embed_loc.at[jnp.clip(local_ids, 0, vocab_dev - 1)].get(mode="promise_in_bounds")
        mate_ids = local_ids - (1 - 2 * (dev_index % 2)) * vocab_dev
        tok_mine = (local_ids >= 0) & (local_ids < vocab_dev)
        tok_mate = (mate_ids >= 0) & (mate_ids < vocab_dev)
        code = jnp.where(tok_mine, 1, jnp.where(tok_mate, 2, 0)).astype(jnp.int32)
        code = jnp.broadcast_to(code[:, None], (code.shape[0], 128))
        x_own, mlp_act, qkv_own = prologue(x_part.reshape(group_size, rows_dev, model_dim), code, ln_gain[None], w_in_loc.T, qkv_dev, ff_dev)
        qkv_own = qkv_own.transpose(1, 0, 2).reshape(num_steps, batch_dev, -1)

        half = head_dim // 2
        inv_freq = ROPE_BASE ** (-jnp.arange(half, dtype=jnp.float32) / half)
        positions = own_lens[None, :] + jnp.arange(num_steps, dtype=jnp.int32)[:, None]
        angles = positions.astype(jnp.float32)[..., None] * inv_freq
        cos, sin = jnp.cos(angles), jnp.sin(angles)
        cos = jnp.concatenate([cos, cos], axis=-1)
        sin = jnp.concatenate([-sin, sin], axis=-1)
        attn_out, k_out, v_out = attention(own_lens, qkv_own, cos, sin, k_loc, v_loc, group_size)
        by_piece = by_device(next_ids).reshape(group_size, num_steps, 2, batch_dev // 2).transpose(0, 2, 1, 3)
        local_next = by_piece.reshape(2 * group_size, 1, batch_dev) - vocab_start
        ids8 = jnp.broadcast_to(local_next, (2 * group_size, 8, batch_dev))
        log_probs = epilogue(attn_out.reshape(group_size, rows_dev, attn_dev), mlp_act, w_out_loc, x_own, final_gain[None], ids8, embed_loc)
        log_probs = log_probs.reshape(group_size, 2, num_steps, batch_dev // 2).transpose(2, 0, 1, 3).reshape(num_steps, batch_size)
        return log_probs, k_out, v_out

    cache_spec = P('tp', None, None)
    return jax.shard_map(device_fn, mesh=mesh, in_specs=(P(), P(), P(), P('tp', None), P(), P(None, 'tp'), P('tp', None), P(), cache_spec, cache_spec), out_specs=(P(), cache_spec, cache_spec), check_vma=False)
```

```python
import functools

import jax
import jax.numpy as jnp
from jax import lax
from jax.experimental import pallas as pl
from jax.experimental.pallas import tpu as pltpu
from jax.sharding import PartitionSpec as P

ROPE_BASE = 10000.0
NORM_EPS = 1e-6
LOG2E = 1.4426950408889634
ROW_BY_ROW = (((1,), (1,)), ((), ()))
KEEP = True
LAST = -1
DOWN = 0


def layer_norm(values, gain_vec):
    centered = values.astype(jnp.float32)
    centered = centered - jnp.mean(centered, axis=LAST, keepdims=KEEP)
    variance = jnp.mean(jnp.square(centered), axis=LAST, keepdims=KEEP)
    scaled = centered * lax.rsqrt(variance + NORM_EPS) * gain_vec.astype(jnp.float32)
    return scaled.astype(jnp.bfloat16)


def attention_kernel(ahead, lens_ref, qkv_ref, cos_ref, sin_ref, k_hbm, v_hbm, o_ref, ko_hbm, vo_hbm, k_buf, v_buf, q_scr, o_scr, n_scr, s_scr, p_scr, read_sem, write_sem):
    num_steps, blocks, rows, _ = qkv_ref.shape
    slots, _, cache_len, head = k_buf.shape
    pack = o_ref.shape[4] // head
    heads = o_ref.shape[0] * pack
    per_seq = num_steps * heads
    win_row = lax.broadcasted_iota(jnp.int32, (16, head), 0)
    col = lax.broadcasted_iota(jnp.int32, (per_seq, cache_len), 1) - lax.broadcasted_iota(jnp.int32, (per_seq, cache_len), 0) // heads
    depth = s_scr.shape[0]

    def moves(block, slot, out):
        here = pl.ds(pl.multiple_of(block * rows, rows), rows)
        pairs = []
        for which, (hbm, hbm_out, buf) in enumerate(((k_hbm, ko_hbm, k_buf), (v_hbm, vo_hbm, v_buf))):
            if out:
                pairs.append(pltpu.make_async_copy(buf.at[slot], hbm_out.at[here], write_sem.at[which, slot]))
            else:
                pairs.append(pltpu.make_async_copy(hbm.at[here], buf.at[slot], read_sem.at[which, slot]))
        return pairs

    for block in range(ahead):
        for copy in moves(block, block, False):
            copy.start()

    @pl.loop(0, blocks)
    def _(block):
        slot = lax.rem(block, slots)

        @pl.when(block + ahead < blocks)
        def _():
            later = lax.rem(block + ahead, slots)

            @pl.when(block + ahead >= slots)
            def _():
                for copy in moves(block + ahead - slots, later, True):
                    copy.wait()

            for copy in moves(block + ahead, later, False):
                copy.start()

        for s in range(num_steps):
            cos, sin = cos_ref[s, block], sin_ref[s, block]

            def rotate(lo):
                x = qkv_ref[s, block, :, lo:lo + head].astype(jnp.float32)
                return x * cos + pltpu.roll(x, head // 2, 1) * sin

            for h in range(heads):
                q_scr[pl.ds(s * heads + h, rows, stride=per_seq), :] = rotate(h * head) * head ** -0.5
            n_scr[0, s] = rotate(heads * head).astype(jnp.bfloat16).astype(jnp.float32)
            n_scr[1, s] = qkv_ref[s, block, :, (heads + 1) * head:].astype(jnp.float32)

        for copy in moves(block, slot, False):
            copy.wait()

        def insert(b):
            length = lens_ref[block * rows + b]
            for dst, which in ((k_buf, 0), (v_buf, 1)):
                for s in range(num_steps):
                    pos = length + s
                    base = pl.multiple_of((pos // 16) * 16, 16)
                    window = dst[slot, b, pl.ds(base, 16), :].astype(jnp.float32)
                    fresh = n_scr[which, s, b:b + 1, :]
                    window = jnp.where(win_row == pos - base, fresh, window)
                    dst[slot, b, pl.ds(base, 16), :] = window.astype(jnp.bfloat16)

        def score(b):
            q = q_scr[b * per_seq:(b + 1) * per_seq, :].astype(jnp.bfloat16)
            s_scr[b % depth] = lax.dot_general(q, k_buf[slot, b], ROW_BY_ROW, preferred_element_type=jnp.float32)

        def soften(b):
            scores = jnp.where(col <= lens_ref[block * rows + b], s_scr[b % depth], -jnp.inf)
            top = jnp.max(scores, axis=1, keepdims=KEEP)
            weight = jnp.exp(scores - top)
            total = jnp.sum(weight, axis=1, keepdims=KEEP)
            p_scr[b % depth] = (weight * (1.0 / total)).astype(jnp.bfloat16)

        def mix(b):
            o_scr[b * per_seq:(b + 1) * per_seq, :] = jnp.dot(p_scr[b % depth], v_buf[slot, b], preferred_element_type=jnp.float32)

        for i in range(rows):
            insert(i)
        for i in range(rows + 2):
            if i < rows:
                score(i)
            if 0 <= i - 1 < rows:
                soften(i - 1)
            if 0 <= i - 2 < rows:
                mix(i - 2)

        for copy in moves(block, slot, True):
            copy.start()
        for s in range(num_steps):
            for h in range(heads):
                o_ref[h // pack, s, block, :, (h % pack) * head:(h % pack + 1) * head] = o_scr[pl.ds(s * heads + h, rows, stride=per_seq), :].astype(jnp.bfloat16)

    for block in range(blocks - slots, blocks):
        for copy in moves(block, block % slots, True):
            copy.wait()


def attention(lens, qkv, cos, sin, k_loc, v_loc, group):
    num_steps, batch, width = qkv.shape
    cache_len, head = k_loc.shape[1], k_loc.shape[2]
    attn_width = width - 2 * head
    heads = attn_width // head
    rows, slots, ahead = 8, 5, 3
    blocks = batch // rows
    vmem, anywhere = pl.BlockSpec(memory_space=pltpu.VMEM), pl.BlockSpec(memory_space=pl.ANY)
    in_blocks = lambda a: a.reshape(num_steps, blocks, rows, a.shape[-1])
    out, k_out, v_out = pl.pallas_call(
        functools.partial(attention_kernel, ahead),
        in_specs=[pl.BlockSpec(memory_space=pltpu.SMEM), vmem, vmem, vmem, anywhere, anywhere],
        out_specs=[vmem, anywhere, anywhere],
        out_shape=[
            jax.ShapeDtypeStruct((group, num_steps, blocks, rows, attn_width // group), jnp.bfloat16),
            jax.ShapeDtypeStruct(k_loc.shape, k_loc.dtype),
            jax.ShapeDtypeStruct(v_loc.shape, v_loc.dtype),
        ],
        scratch_shapes=[
            pltpu.VMEM((slots, rows, cache_len, head), jnp.bfloat16),
            pltpu.VMEM((slots, rows, cache_len, head), jnp.bfloat16),
            pltpu.VMEM((rows * num_steps * heads, head), jnp.float32),
            pltpu.VMEM((rows * num_steps * heads, head), jnp.float32),
            pltpu.VMEM((2, num_steps, rows, head), jnp.float32),
            pltpu.VMEM((4, num_steps * heads, cache_len), jnp.float32),
            pltpu.VMEM((4, num_steps * heads, cache_len), jnp.bfloat16),
            pltpu.SemaphoreType.DMA((2, slots)),
            pltpu.SemaphoreType.DMA((2, slots)),
        ],
        compiler_params=pltpu.CompilerParams(vmem_limit_bytes=56 * 1024 * 1024),
        name="attention",
    )(lens, in_blocks(qkv), in_blocks(cos), in_blocks(sin), k_loc, v_loc)
    return out.reshape(group, num_steps, batch, attn_width // group), k_out, v_out


HALF = 128
UNIT = 2 * HALF


def paired(*counts):
    return [pltpu.SemaphoreType.DMA((n,)) for n in counts for _ in ('send', 'recv')]


def eight(r):
    return slice(r * 8, r * 8 + 8)

OWN, XN, YN, DIAG = (0, 0), (1, 0), (0, 1), (1, 1)
REDUCE_ORDER = (DIAG, XN, YN, OWN)
UNIT_HALVES = (((OWN, 0), (OWN, 1)), ((XN, 1), (YN, 0)), ((XN, 0), (YN, 1)), ((DIAG, 0), (DIAG, 1)))
MESH = pl.DeviceIdType.MESH
ROWS = 16
PANEL = 512


def strip(first):
    return pl.ds(pl.multiple_of(first, ROWS), ROWS)


def panel(n):
    return pl.ds(pl.multiple_of(n * PANEL, PANEL), PANEL)


class Place:
    def __init__(self):
        me = lax.axis_index('tp')
        self.me = me
        self.core, self.x, self.y = me % 2, (me // 2) % 2, me // 4

    def at(self, chip, core):
        x_far, y_far = chip
        flip = lambda far, value: 1 - value if far else value
        return flip(y_far, self.y) * 4 + flip(x_far, self.x) * 2 + flip(core, self.core)


def everyone():
    return [(chip, core) for chip in (DIAG, XN, YN, OWN) for core in (1, 0) if (chip, core) != (OWN, 0)]


def greet(place):
    barrier = pltpu.get_barrier_semaphore()
    for chip, core in everyone():
        pl.semaphore_signal(barrier, inc=1, device_id=(place.at(chip, core),), device_id_type=MESH)
    pl.semaphore_wait(barrier, 7)


def push(src, dst, send, recv, target):
    copy = pltpu.make_async_remote_copy(src_ref=src, dst_ref=dst, send_sem=send, recv_sem=recv, device_id=(target,), device_id_type=MESH)
    copy.start()
    return copy


def reduce_rows(place, outgoing, own_block, rc, r1a, r1b, r2, csend, crecv, psend, precv):
    dim = rc.shape[2]
    partner = place.at(OWN, 1)
    to_x, to_y = place.at(XN, 0), place.at(YN, 0)
    first, second = pl.ds(0, HALF), pl.ds(HALF, HALF)
    exchange = []
    for i, chip in enumerate(REDUCE_ORDER):
        src = outgoing(i, place.at(chip, 1))
        exchange.append(push(src, rc.at[i], csend.at[i], crecv.at[i], partner))
    sends = []
    for i, chip in enumerate(REDUCE_ORDER):
        own_block(i, place.at(chip, 0), exchange[i])
        if chip == DIAG:
            sends.append(push(rc.at[i, first], r1a.at[0], psend.at[0], precv.at[0], to_x))
            sends.append(push(rc.at[i, second], r1b.at[0], psend.at[1], precv.at[1], to_y))
        elif chip == XN:
            sends.append(push(rc.at[i, first], r1a.at[1], psend.at[2], precv.at[2], to_x))
        elif chip == YN:
            sends.append(push(rc.at[i, second], r1b.at[1], psend.at[3], precv.at[3], to_y))
    for copy in exchange:
        copy.wait_send()
    for j, (slot, rows, landed, target) in enumerate(((2, 0, r1a, to_y), (1, HALF, r1b, to_x))):
        sends[j].wait_recv()

        @pl.loop(0, HALF // ROWS)
        def _(r):
            here = strip(rows + r * ROWS)
            there = strip(r * ROWS)
            total = rc[slot, here, :].astype(jnp.float32) + landed[0, there, :].astype(jnp.float32)
            rc[slot, here, :] = total.astype(jnp.bfloat16)

        sends.append(push(rc.at[slot, pl.ds(rows, HALF)], r2.at[j], psend.at[4 + j], precv.at[4 + j], target))
    for copy in sends[2:]:
        copy.wait_recv()
    for copy in sends:
        copy.wait_send()


def own_rows(rc, r1a, r1b, r2, half, r, rows):
    here = pl.ds(pl.multiple_of(half * HALF + r * rows, rows), rows)
    there = pl.ds(pl.multiple_of(r * rows, rows), rows)
    landed = r1b if half else r1a
    return rc[3, here, :].astype(jnp.float32) + landed[1, there, :].astype(jnp.float32) + r2[half, there, :].astype(jnp.float32)


def norm_rows(values, gain):
    centered = values - jnp.mean(values, axis=LAST, keepdims=KEEP)
    variance = jnp.mean(centered * centered, axis=LAST, keepdims=KEEP)
    return (centered * lax.rsqrt(variance + NORM_EPS) * gain).astype(jnp.bfloat16)


def gather_units(place, z, asend, arecv, work):
    partner = place.at(OWN, 1)
    to_x, to_y = place.at(XN, 0), place.at(YN, 0)
    part = lambda unit, pos: z.at[unit, pl.ds(pos * HALF, HALF)]
    sends = []

    def go(src, dst, slot, target):
        k = len(sends)
        sends.append(push(src, dst, asend.at[k], arecv.at[slot], target))
        return sends[-1]

    xb = go(part(0, 1), part(2, 0), 0, to_x)
    ya = go(part(0, 0), part(2, 1), 1, to_y)
    near = go(z.at[0], z.at[1], 2, partner)
    xa = go(part(0, 0), part(4, 0), 3, to_x)
    yb = go(part(0, 1), part(4, 1), 4, to_y)
    near.wait_recv()
    work(0)
    xb.wait_recv()
    db = go(part(2, 0), part(6, 1), 5, to_y)
    ya.wait_recv()
    da = go(part(2, 1), part(6, 0), 6, to_x)
    near2 = go(z.at[2], z.at[3], 7, partner)
    near2.wait_recv()
    work(1)
    xa.wait_recv()
    yb.wait_recv()
    near4 = go(z.at[4], z.at[5], 8, partner)
    near4.wait_recv()
    work(2)
    da.wait_recv()
    db.wait_recv()
    near6 = go(z.at[6], z.at[7], 9, partner)
    near6.wait_recv()
    work(3)
    for copy in sends:
        copy.wait_send()


def prologue_kernel(widths, part_ref, code_ref, gain_ref, w_hbm, x_ref, m_ref, qkv_ref, z, rc, r1a, r1b, r2, w_buf, qkv_out, w_sem, csend, crecv, psend, precv, asend, arecv, qsend, qrecv):
    qkv_dev, ff_dev = widths
    dim = part_ref.shape[2]
    place = Place()
    greet(place)
    load = pltpu.make_async_copy(w_hbm, w_buf, w_sem)
    load.start()

    def own_block(i, block, copy):
        copy.wait_recv()

        @pl.loop(0, UNIT // 32)
        def _(r):
            here = pl.ds(pl.multiple_of(r * 32, 32), 32)
            code = code_ref[pl.ds(pl.multiple_of(block * UNIT + r * 32, 32), 32), :]
            for c in range(dim // 128):
                lanes = slice(c * 128, (c + 1) * 128)
                theirs = jnp.where(code == 2, rc[i, here, lanes].astype(jnp.float32), 0.0)
                rc[i, here, lanes] = jnp.where(code == 1, part_ref[block, here, lanes].astype(jnp.float32), theirs).astype(jnp.bfloat16)

    reduce_rows(place, lambda i, block: part_ref.at[block], own_block, rc, r1a, r1b, r2, csend, crecv, psend, precv)
    gain = gain_ref[...].astype(jnp.float32)
    for half in range(2):
        @pl.loop(0, HALF // ROWS)
        def _(r):
            here = strip(half * HALF + r * ROWS)
            x = own_rows(rc, r1a, r1b, r2, half, r, ROWS).astype(jnp.bfloat16)
            x_ref[here, :] = x
            z[0, here, :] = norm_rows(x.astype(jnp.float32), gain)

    out_sends = []

    def times(rows, first, count):
        return lax.dot_general(rows, w_buf[pl.ds(first, count), :], ROW_BY_ROW, preferred_element_type=jnp.float32)

    def work(pair):
        if pair == 0:
            load.wait()
        rows = z[2 * pair:2 * pair + 2].reshape(2 * UNIT, dim)
        qkv_out[2 * pair:2 * pair + 2] = times(rows, 0, qkv_dev).astype(jnp.bfloat16).reshape(2, UNIT, qkv_dev)
        for core in range(2):
            for pos, (chip, half) in enumerate(UNIT_HALVES[pair]):
                unit = 2 * pair + core
                block = place.at(chip, core)
                src = qkv_out.at[unit, pl.ds(pos * HALF, HALF)]
                if unit == 0:
                    qkv_ref[place.me, pl.ds(half * HALF, HALF), :] = qkv_out[unit, pl.ds(pos * HALF, HALF), :]
                else:
                    k = len(out_sends)
                    out_sends.append(push(src, qkv_ref.at[place.me, pl.ds(half * HALF, HALF)], qsend.at[k], qrecv.at[k], block))
        tile = 256

        @pl.loop(0, ff_dev // tile)
        def _(n):
            at = pl.multiple_of(n * tile, tile)
            gate = times(rows, pl.multiple_of(qkv_dev + at, 16), tile).astype(jnp.bfloat16).astype(jnp.float32)
            up = times(rows, pl.multiple_of(qkv_dev + ff_dev + at, 16), tile).astype(jnp.bfloat16).astype(jnp.float32)
            act = (gate / (1.0 + jnp.exp(-gate)) * up).astype(jnp.bfloat16)
            for core in range(2):
                for pos, (chip, half) in enumerate(UNIT_HALVES[pair]):
                    first = place.at(chip, core) * UNIT + half * HALF
                    k = core * UNIT + pos * HALF
                    m_ref[pl.ds(pl.multiple_of(first, HALF), HALF), pl.ds(at, tile)] = act[k:k + HALF]

    gather_units(place, z, asend, arecv, work)
    for copy in out_sends:
        copy.wait()


def prologue(part, code, gain, w_in, qkv_dev, ff_dev):
    group, rows, dim = part.shape
    vmem = pl.BlockSpec(memory_space=pltpu.VMEM)
    dma = pltpu.SemaphoreType.DMA
    return pl.pallas_call(
        functools.partial(prologue_kernel, (qkv_dev, ff_dev)),
        in_specs=[vmem] * 3 + [pl.BlockSpec(memory_space=pl.ANY)],
        out_specs=[vmem] * 3,
        out_shape=[
            jax.ShapeDtypeStruct((rows, dim), jnp.bfloat16),
            jax.ShapeDtypeStruct((group * rows, ff_dev), jnp.bfloat16),
            jax.ShapeDtypeStruct((group, rows, qkv_dev), jnp.bfloat16),
        ],
        scratch_shapes=[
            pltpu.VMEM((group, rows, dim), jnp.bfloat16),
            pltpu.VMEM((4, rows, dim), jnp.bfloat16),
            *[pltpu.VMEM((2, HALF, dim), jnp.bfloat16) for _ in 'abc'],
            pltpu.VMEM(w_in.shape, jnp.bfloat16),
            pltpu.VMEM((group, rows, qkv_dev), jnp.bfloat16),
            dma,
            *paired(4, 6, 10, 14),
        ],
        compiler_params=pltpu.CompilerParams(collective_id=0, has_side_effects=True, vmem_limit_bytes=60 * 1024 * 1024),
        name="prologue",
    )(part, code, gain, w_in)


SLOTS = ((OWN, 0), (OWN, 1), (XN, 0), (XN, 1), (YN, 0), (YN, 1), (DIAG, 0), (DIAG, 1))
PIECE = HALF // 2
NEAR, SIDES, FAR = (0, 2), (2, 4), (6, 2)


def epilogue_kernel(scale, tile, attn_ref, m_ref, w_ref, x_ref, gain_ref, ids_ref, e_hbm, out_ref, e_buf, z, rc, r1a, r1b, r2, a_in, raw, stats, every, e_sem, csend, crecv, psend, precv, asend, arecv, qsend, qrecv, ssend, srecv):
    vocab = e_hbm.shape[0]
    tiles = vocab // tile
    dim = z.shape[3]
    attn_dev = a_in.shape[2]
    loads = [pltpu.make_async_copy(e_hbm.at[pl.ds(t * tile, tile)], e_buf.at[pl.ds(t * tile, tile)], e_sem.at[t]) for t in range(tiles)]
    place = Place()
    greet(place)
    partner = place.at(OWN, 1)
    to_x, to_y = place.at(XN, 0), place.at(YN, 0)
    heads_in = {}
    for k, (chip, core) in enumerate(everyone()):
        target = place.at(chip, core)
        heads_in[(chip, core)] = push(attn_ref.at[target], a_in.at[place.me], qsend.at[k], qrecv.at[k], target)
    for c in loads:
        c.start()
    a_in[place.me] = attn_ref[place.me]

    def block_dot(block, n):
        lanes = panel(n)
        mine = jnp.dot(a_in[block], w_ref[pl.ds(0, attn_dev), lanes], preferred_element_type=jnp.float32)
        rows = pl.ds(pl.multiple_of(block * UNIT, UNIT), UNIT)
        return mine + jnp.dot(m_ref[rows, :], w_ref[pl.ds(attn_dev, w_ref.shape[0] - attn_dev), lanes], preferred_element_type=jnp.float32)

    exchange = []
    for i, chip in enumerate(REDUCE_ORDER):
        heads_in[(chip, 1)].wait_recv()
        block = place.at(chip, 1)

        @pl.loop(0, dim // PANEL)
        def _(n):
            lanes = panel(n)
            both = block_dot(block, n).astype(jnp.bfloat16)
            z[0, 2 * i, :, lanes] = both[:HALF]
            z[1, 2 * i, :, lanes] = both[HALF:]

        for h in range(2):
            exchange.append(push(z.at[h, 2 * i], rc.at[i, pl.ds(h * HALF, HALF)], csend.at[2 * i + h], crecv.at[2 * i + h], partner))

    partial = {}

    def first_send(sub, i):
        chip = REDUCE_ORDER[i]
        upper, lower = rc.at[i, pl.ds(sub * PIECE, PIECE)], rc.at[i, pl.ds(HALF + sub * PIECE, PIECE)]
        k = sub * 6
        if chip == DIAG:
            partial[sub, 0] = push(upper, r1a.at[sub, 0], psend.at[k], precv.at[k], to_x)
            partial[sub, 1] = push(lower, r1b.at[sub, 0], psend.at[k + 1], precv.at[k + 1], to_y)
        elif chip == XN:
            partial[sub, 2] = push(upper, r1a.at[sub, 1], psend.at[k + 2], precv.at[k + 2], to_x)
        elif chip == YN:
            partial[sub, 3] = push(lower, r1b.at[sub, 1], psend.at[k + 3], precv.at[k + 3], to_y)

    def second_send(sub):
        for q, (slot, rows, landed, target) in enumerate(((2, sub * PIECE, r1a, to_y), (1, HALF + sub * PIECE, r1b, to_x))):
            partial[sub, q].wait_recv()

            @pl.loop(0, PIECE // ROWS)
            def _(r):
                here = strip(rows + r * ROWS)
                there = strip(r * ROWS)
                total = rc[slot, here, :].astype(jnp.float32) + landed[sub, 0, there, :].astype(jnp.float32)
                rc[slot, here, :] = total.astype(jnp.bfloat16)

            k = sub * 6 + 4 + q
            partial[sub, 4 + q] = push(rc.at[slot, pl.ds(rows, PIECE)], r2.at[sub, q], psend.at[k], precv.at[k], target)

    gain = gain_ref[...].astype(jnp.float32)

    def finish_rows(sub):
        for k in range(2, 6):
            partial[sub, k].wait_recv()
        for half, landed in enumerate((r1a, r1b)):
            @pl.loop(0, PIECE // ROWS)
            def _(r):
                there = strip(r * ROWS)
                here = strip(half * HALF + sub * PIECE + r * ROWS)
                o = rc[3, here, :].astype(jnp.float32) + landed[sub, 1, there, :].astype(jnp.float32) + r2[sub, half, there, :].astype(jnp.float32)
                o = o.astype(jnp.bfloat16).astype(jnp.float32)
                z[sub, 0, strip(half * PIECE + r * ROWS), :] = norm_rows(x_ref[here, :].astype(jnp.float32) + o, gain)

    moved = {}

    def go(sub, k, src, dst, target):
        moved[sub, k] = push(src, dst, asend.at[sub * 10 + k], arecv.at[sub * 10 + k], target)

    def part(sub, slot, half):
        return z.at[sub, slot, pl.ds(half * PIECE, PIECE)]

    def gather_start(sub):
        go(sub, 0, part(sub, 0, 1), part(sub, 2, 1), to_x)
        go(sub, 1, part(sub, 0, 0), part(sub, 4, 0), to_y)
        go(sub, 2, z.at[sub, 0], z.at[sub, 1], partner)
        go(sub, 3, part(sub, 0, 0), part(sub, 2, 0), to_x)
        go(sub, 4, part(sub, 0, 1), part(sub, 4, 1), to_y)

    def gather_relay(sub):
        moved[sub, 0].wait_recv()
        go(sub, 5, part(sub, 2, 1), part(sub, 6, 1), to_y)
        moved[sub, 1].wait_recv()
        go(sub, 6, part(sub, 4, 0), part(sub, 6, 0), to_x)

    def gather_sides(sub):
        for k, slot in ((3, 2), (4, 4)):
            moved[sub, k].wait_recv()
            go(sub, 4 + k, z.at[sub, slot], z.at[sub, slot + 1], partner)
        for k in (7, 8):
            moved[sub, k].wait_recv()

    def gather_far(sub):
        moved[sub, 6].wait_recv()
        moved[sub, 5].wait_recv()
        go(sub, 9, z.at[sub, 6], z.at[sub, 7], partner)
        moved[sub, 9].wait_recv()

    def work(sub, first, count):
        cols = count * HALF
        places = [place.at(*SLOTS[first + k]) * 2 + sub for k in range(count)]
        row = lax.broadcasted_iota(jnp.int32, (8, cols), 0)
        ids = jnp.concatenate([ids_ref[h] for h in places], axis=1) - row
        rate = scale * LOG2E

        def product(t, slot):
            e = e_buf[pl.ds(pl.multiple_of(t * tile, 16), tile), :]
            rows = z[sub, first:first + count].reshape(cols, dim)
            raw[slot, :, :cols] = lax.dot_general(e, rows, ROW_BY_ROW, preferred_element_type=jnp.float32)

        def absorb(t, slot, carry):
            top, total, target = carry
            local = ids - t * tile
            each = tile // 8
            tops = [top, None]
            for r in range(each):
                v = raw[slot, eight(r), :cols]
                k = r % 2
                tops[k] = v if tops[k] is None else jnp.maximum(tops[k], v)
            new_top = jnp.maximum(tops[0], tops[1])
            sums = [total * jnp.exp2((top - new_top) * rate), None]
            for r in range(each):
                v = raw[slot, eight(r), :cols]
                k = r % 2
                p = jnp.exp2((v - new_top) * rate)
                sums[k] = p if sums[k] is None else sums[k] + p
                target = target + jnp.where(local == r * 8, v, 0.0)
            return new_top, sums[0] + sums[1], target

        zero = jnp.zeros((8, cols), jnp.float32)
        product(0, 0)

        def body(i, carry):
            product(2 * i + 1, 1)
            carry = absorb(2 * i, 0, carry)
            product(2 * i + 2, 0)
            return absorb(2 * i + 1, 1, carry)

        carry = lax.fori_loop(0, (tiles - 1) // 2, body, (jnp.full((8, cols), -jnp.inf, jnp.float32), zero, zero))
        if tiles % 2 == 0:
            product(tiles - 1, 1)
            carry = absorb(tiles - 2, 0, carry)
        top, total, target = absorb(tiles - 1, (tiles - 1) % 2, carry)
        best = jnp.max(top, axis=DOWN, keepdims=KEEP)
        total = jnp.sum(total * jnp.exp2((top - best) * rate), axis=DOWN, keepdims=KEEP)
        target = jnp.sum(target, axis=DOWN, keepdims=KEEP)
        for pos, h in enumerate(places):
            lanes = slice(pos * HALF, (pos + 1) * HALF)
            for k, found in enumerate((best * scale, total, target * scale)):
                stats[k, pl.ds(h, 1), :] = found[:, lanes]

    for i, chip in enumerate(REDUCE_ORDER):
        if chip != OWN:
            heads_in[(chip, 0)].wait_recv()
        for copy in exchange[2 * i:2 * i + 2]:
            copy.wait_recv()
        block = place.at(chip, 0)

        @pl.loop(0, dim // PANEL)
        def _(n):
            lanes = panel(n)
            rc[i, :, lanes] = (block_dot(block, n) + rc[i, :, lanes].astype(jnp.float32)).astype(jnp.bfloat16)

        first_send(0, i)
    for copy in exchange:
        copy.wait_send()
    second_send(0)
    first_send(1, 0)
    finish_rows(0)
    gather_start(0)
    first_send(1, 1)
    first_send(1, 2)
    for c in loads:
        c.wait()
    moved[0, 2].wait_recv()
    work(0, *NEAR)
    gather_relay(0)
    second_send(1)
    gather_sides(0)
    work(0, *SIDES)
    finish_rows(1)
    gather_start(1)
    gather_far(0)
    work(0, *FAR)
    gather_relay(1)
    moved[1, 2].wait_recv()
    work(1, *NEAR)
    gather_sides(1)
    work(1, *SIDES)
    gather_far(1)
    work(1, *FAR)
    for copy in (*partial.values(), *moved.values(), *heads_in.values()):
        copy.wait_send()
    finals = []
    for k, (chip, core) in enumerate(everyone()):
        finals.append(push(stats, every.at[place.me], ssend.at[k], srecv.at[k], place.at(chip, core)))
    every[place.me] = stats[...]
    for copy in finals:
        copy.wait()
    tops = every[:, 0]
    best = jnp.max(tops, axis=DOWN)
    total = jnp.sum(every[:, 1] * jnp.exp(tops - best[None]), axis=DOWN)
    out_ref[...] = jnp.sum(every[:, 2], axis=DOWN) - best - jnp.log(total)


def epilogue(attn, m, w_out, x_own, gain, ids, embed_loc):
    group, rows, attn_dev = attn.shape
    vocab, dim = embed_loc.shape
    tile = 560
    vmem = pl.BlockSpec(memory_space=pltpu.VMEM)
    dma = pltpu.SemaphoreType.DMA
    halves = group * rows // HALF
    return pl.pallas_call(
        functools.partial(epilogue_kernel, dim ** -0.5, tile),
        in_specs=[vmem] * 6 + [pl.BlockSpec(memory_space=pl.ANY)],
        out_specs=vmem,
        out_shape=jax.ShapeDtypeStruct((halves, HALF), jnp.float32),
        scratch_shapes=[
            pltpu.VMEM((vocab, dim), jnp.bfloat16),
            pltpu.VMEM((2, group, HALF, dim), jnp.bfloat16),
            pltpu.VMEM((4, rows, dim), jnp.bfloat16),
            *[pltpu.VMEM((2, 2, PIECE, dim), jnp.bfloat16) for _ in 'abc'],
            pltpu.VMEM((group, rows, attn_dev), jnp.bfloat16),
            pltpu.VMEM((2, tile, 2 * UNIT), jnp.float32),
            pltpu.VMEM((3, halves, HALF), jnp.float32),
            pltpu.VMEM((group, 3, halves, HALF), jnp.float32),
            dma((vocab // tile,)),
            *paired(8, 12, 20, 7, 7),
        ],
        compiler_params=pltpu.CompilerParams(collective_id=1, has_side_effects=True, vmem_limit_bytes=67043328),
        name="epilogue",
    )(attn, m, w_out, x_own, gain, ids, embed_loc)


def solution(mesh):
    group_size = mesh.shape['tp']

    def device_fn(tok_ids, next_ids, seq_lens, embed_loc, ln_gain, w_in_loc, w_out_loc, final_gain, k_loc, v_loc):
        num_steps, batch_size = tok_ids.shape
        batch_dev = batch_size // group_size
        rows_dev = num_steps * batch_dev
        vocab_dev, model_dim = embed_loc.shape
        head_dim = k_loc.shape[2]
        in_dev = w_in_loc.shape[1]
        out_dev = w_out_loc.shape[0]
        kv_dev = 2 * head_dim // group_size
        attn_dev = 2 * out_dev - in_dev + kv_dev
        ff_dev = out_dev - attn_dev
        qkv_dev = attn_dev + kv_dev
        dev_index = lax.axis_index('tp')
        vocab_start = dev_index * vocab_dev
        own_lens = lax.dynamic_slice_in_dim(seq_lens, dev_index * batch_dev, batch_dev)

        def by_device(ids):
            return ids.reshape(num_steps, group_size, batch_dev).transpose(1, 0, 2)

        local_ids = by_device(tok_ids).reshape(-1) - vocab_start
        x_part = embed_loc.at[jnp.clip(local_ids, 0, vocab_dev - 1)].get(mode="promise_in_bounds")
        mate_ids = local_ids - (1 - 2 * (dev_index % 2)) * vocab_dev
        tok_mine = (local_ids >= 0) & (local_ids < vocab_dev)
        tok_mate = (mate_ids >= 0) & (mate_ids < vocab_dev)
        code = jnp.where(tok_mine, 1, jnp.where(tok_mate, 2, 0)).astype(jnp.int32)
        code = jnp.broadcast_to(code[:, None], (code.shape[0], 128))
        x_own, mlp_act, qkv_own = prologue(x_part.reshape(group_size, rows_dev, model_dim), code, ln_gain[None], w_in_loc.T, qkv_dev, ff_dev)
        qkv_own = qkv_own.transpose(1, 0, 2).reshape(num_steps, batch_dev, -1)

        half = head_dim // 2
        inv_freq = ROPE_BASE ** (-jnp.arange(half, dtype=jnp.float32) / half)
        positions = own_lens[None, :] + jnp.arange(num_steps, dtype=jnp.int32)[:, None]
        angles = positions.astype(jnp.float32)[..., None] * inv_freq
        cos, sin = jnp.cos(angles), jnp.sin(angles)
        cos = jnp.concatenate([cos, cos], axis=LAST)
        sin = jnp.concatenate([-sin, sin], axis=LAST)
        attn_out, k_out, v_out = attention(own_lens, qkv_own, cos, sin, k_loc, v_loc, group_size)
        by_piece = by_device(next_ids).reshape(group_size, num_steps, 2, batch_dev // 2).transpose(0, 2, 1, 3)
        local_next = by_piece.reshape(2 * group_size, 1, batch_dev) - vocab_start
        ids8 = jnp.broadcast_to(local_next, (2 * group_size, 8, batch_dev))
        log_probs = epilogue(attn_out.reshape(group_size, rows_dev, attn_dev), mlp_act, w_out_loc, x_own, final_gain[None], ids8, embed_loc)
        log_probs = log_probs.reshape(group_size, 2, num_steps, batch_dev // 2).transpose(2, 0, 1, 3).reshape(num_steps, batch_size)
        return log_probs, k_out, v_out

    cache_spec = P('tp', None, None)
    return jax.shard_map(device_fn, mesh=mesh, in_specs=(P(), P(), P(), P('tp', None), P(), P(None, 'tp'), P('tp', None), P(), cache_spec, cache_spec), out_specs=(P(), cache_spec, cache_spec), check_vma=False)
```
